32 devices in a mesh: dp: 16 (over z, y, core), mp: 2 (over x).
Axes of the slice: x: 2, y: 2, z: 4, core: 2. Of those that a mesh axis runs over, the one named last changes fastest.
Arguments:
- tokens: bfloat16 [8192, 768], P('dp'), may hold values from -6 to 6
- crop_ids: int32 [32, 256], P('dp'), may hold values from 0 to 7, never falling along the last dimension, each value on 1 to 64 neighbouring positions
- w_query: bfloat16 [768, 768], P(None, 'mp'), may hold values from -0.4375 to 0.4375
- w_key: bfloat16 [768, 768], P(None, 'mp'), may hold values from -0.21875 to 0.21875
- w_value: bfloat16 [768, 768], P(None, 'mp'), may hold values from -0.21875 to 0.21875
- bias_query: float32 [768], P('mp'), may hold values from -3 to 3
- bias_value: float32 [768], P('mp'), may hold values from -2 to 2
- w_out: bfloat16 [768, 768], P('mp'), may hold values from -0.875 to 0.875
- bias_out: float32 [768], replicated, may hold values from -2 to 2
- gain_attn: float32 [768], replicated, may hold values from 0.5 to 1.5
- shift_attn: float32 [768], replicated, may hold values from -2 to 2
- gain_mlp: float32 [768], replicated, may hold values from 0.5 to 1.5
- shift_mlp: float32 [768], replicated, may hold values from -2 to 2
- w_up: bfloat16 [768, 3072], P(None, 'mp'), may hold values from -0.21875 to 0.21875
- bias_up: float32 [3072], P('mp'), may hold values from -3 to 3
- w_down: bfloat16 [3072, 768], P('mp'), may hold values from -0.109375 to 0.109375
- bias_down: float32 [768], replicated, may hold values from -2 to 2
- cotangent: bfloat16 [8192, 768], P('dp'), may hold values from -6 to 6
Outputs:
- block_out: bfloat16 [8192, 768], P('dp')
- grad_tokens: float32 [8192, 768], P('dp')
- grad_w_query: float32 [768, 768], P('dp', 'mp')
- grad_w_key: float32 [768, 768], P('dp', 'mp')
- grad_w_value: float32 [768, 768], P('dp', 'mp')
- grad_bias_query: float32 [768], P('mp')
- grad_bias_value: float32 [768], P('mp')
- grad_w_out: float32 [768, 768], P('mp', 'dp')
- grad_bias_out: float32 [768], P('dp')
- grad_gain_attn: float32 [768], P('dp')
- grad_shift_attn: float32 [768], P('dp')
- grad_gain_mlp: float32 [768], P('dp')
- grad_shift_mlp: float32 [768], P('dp')
- grad_w_up: float32 [768, 3072], P('dp', 'mp')
- grad_bias_up: float32 [3072], P('mp')
- grad_w_down: float32 [3072, 768], P('mp', 'dp')
- grad_bias_down: float32 [768], P('dp')
The draws below stay inside these ranges and needn't reach their ends.
Inputs may be any that keep to these rules, and one draw needn't show every extreme that they name: `crop_ids`: within each sequence the crop ids never fall, every crop has 1 to 64 patches, and some crop has exactly 64.
All inputs are finite; a program needn't handle non-finite values.
Results may differ from the reference program's by a relative error of at most 0.012.
The reference program's roundings to bfloat16 on the way count: a program that leaves them out, or rounds other values in their place, can miss the bound.
Values sent between devices are 32-bit elements; how exact they have to be, the bound alone decides.
No kernel may reach another device: no remote copies, remote signals or barrier semaphores. Data moves between devices by JAX's collectives and lax.ppermute only.
A program may use at most 128 MiB of HBM per device.

```python
import math
import jax
import jax.numpy as jnp
import numpy as np
from jax import lax

D = 768
HEADS = 12
HEAD_DIM = 64
FF = 3072
LEN = 256
SEGS = 8
SEG_MOST = 64
SEQS = 32
TOKENS = 8192


def raised(array, own_key, source, target, parts, factor):
    def block_of(axis_at):
        return (jnp.arange(array.shape[axis_at]) // (array.shape[axis_at] // parts)).reshape((-1,) + (1,) * (array.ndim - 1 - axis_at))

    near = jax.random.permutation(own_key, parts)[block_of(target)]
    far = (block_of(target) + parts // 2) % parts
    return jnp.where((block_of(source) == near) | (block_of(source) == far), factor * array, array)


def steps_of(rng, extent, pieces, smallest, top_value):
    factor_of, own = 1.0, jax.random.fold_in(rng, 6)
    for dim, parts in pieces:
        steps = jnp.exp(jax.random.uniform(jax.random.fold_in(own, dim), (parts,), jnp.float32, smallest / len(pieces), top_value / len(pieces)))
        factor_of = factor_of * jnp.repeat(steps, extent[dim] // parts).reshape([-1 if axis == dim else 1 for axis in range(len(extent))])
    return factor_of


def length_profile(amount, total, reach, slope):
    loads = [(1 << 20) // math.isqrt(rank ** slope) + 1 for rank in range(2, amount + 1)]
    rest, given = total - reach - (amount - 1), [1] * (amount - 1)
    while rest > 0:
        candidates = [i for i in range(amount - 1) if given[i] < reach]
        whole, left = sum([loads[i] for i in candidates]), rest
        for i in candidates:
            more = min(reach - given[i], max(1, left * loads[i] // whole), rest)
            given[i] = given[i] + more
            rest = rest - more
    return np.array([reach] + given)


def uneven_parts(own_key, amount, total, limit, skew):
    if amount == 2:
        one = jax.random.randint(own_key, (), max(1, total - limit), min(limit, total - 1) + 1)
        return jnp.stack([one, total - one])
    tallies = jnp.asarray(length_profile(amount, total, limit, skew), jnp.int32)
    couples = (amount - 1) // 2
    giver, sink = tallies[1:1 + 2 * couples:2], tallies[2:2 + 2 * couples:2]
    margin = jnp.minimum(giver - 1, limit - sink)
    moved = jax.random.randint(jax.random.fold_in(own_key, 1), (couples,), 0, 1 << 20) % (margin + 1)
    tallies = tallies.at[1:1 + 2 * couples:2].set(giver - moved).at[2:2 + 2 * couples:2].set(sink + moved)
    return tallies[jax.random.permutation(jax.random.fold_in(own_key, 2), amount)]


def bell_draw(key, extent, deviation, limit, shards=(), dtype=jnp.bfloat16):
    entries = jax.random.normal(key, extent, jnp.float32) * deviation
    if len(shards) > 0:
        entries = steps_of(key, extent, shards, -0.22, 0.18) * entries
    return jnp.clip(entries, min=-limit, max=limit).astype(dtype)


def noise_with(rng, dims, scale, bound, shards, heavy, kind=jnp.bfloat16):
    values = scale * jax.random.normal(rng, dims, jnp.float32)
    if shards:
        values = values * steps_of(rng, dims, shards, -0.22, 0.18)
    return jnp.clip(raised(values, jax.random.fold_in(rng, 3), *heavy), -bound, bound).astype(kind)


def setup_inputs(seed: int = 0) -> dict:
    streams_of = jax.random.split(jax.random.key(seed), 19)
    return {
        "tokens": bell_draw(streams_of[0], (TOKENS, D), 1.0, 6.0, ((0, 16),)),
        "crop_ids": jax.vmap(lambda own: jnp.searchsorted(jnp.cumsum(uneven_parts(own, SEGS, LEN, SEG_MOST, 2)), jnp.arange(LEN), side="right"))(jax.random.split(streams_of[1], SEQS)).reshape((SEQS, LEN)).astype(jnp.int32),
        "w_query": bell_draw(streams_of[2], (D, D), (D // 4) ** -0.5, 0.4375, ((1, 2),)),
        "w_key": bell_draw(streams_of[3], (D, D), D ** -0.5, 0.21875, ((1, 2),)),
        "w_value": bell_draw(streams_of[4], (D, D), D ** -0.5, 0.21875, ((1, 2),)),
        "bias_query": bell_draw(streams_of[5], (D,), 0.5, 3.0, ((0, 2),), jnp.float32),
        "bias_value": bell_draw(streams_of[6], (D,), 0.3, 2.0, ((0, 2),), jnp.float32),
        "w_out": bell_draw(streams_of[7], (D, D), (D // 16) ** -0.5, 0.875, ((0, 2),)),
        "bias_out": bell_draw(streams_of[8], (D,), 0.3, 2.0, (), jnp.float32),
        "gain_attn": jnp.clip(1.0 + 0.1 * jax.random.normal(streams_of[9], (D,), jnp.float32), 0.5, 1.5),
        "shift_attn": bell_draw(streams_of[10], (D,), 0.3, 2.0, (), jnp.float32),
        "gain_mlp": jnp.clip(1.0 + 0.1 * jax.random.normal(streams_of[11], (D,), jnp.float32), 0.5, 1.5),
        "shift_mlp": bell_draw(streams_of[12], (D,), 0.3, 2.0, (), jnp.float32),
        "w_up": bell_draw(streams_of[13], (D, FF), D ** -0.5, 0.21875, ((1, 2),)),
        "bias_up": bell_draw(streams_of[14], (FF,), 0.5, 3.0, ((0, 2),), jnp.float32),
        "w_down": bell_draw(streams_of[15], (FF, D), FF ** -0.5, 0.109375, ((0, 2),)),
        "bias_down": bell_draw(streams_of[16], (D,), 0.3, 2.0, (), jnp.float32),
        "cotangent": noise_with(streams_of[17], (TOKENS, D), 1.0, 6.0, ((0, 16),), (0, 1, 16, 2.0)),
    }


@jax.custom_vjp
def low(v):
    return lax.optimization_barrier(v.astype(jnp.bfloat16)).astype(jnp.float32)

@jax.custom_vjp
def low_back(v):
    return v

def low_keep(v):
    return (low(v), None)

def low_pass(kept, grad):
    return (grad,)

def back_keep(v):
    return (v, None)

def back_low(kept, grad):
    return (low(grad),)
low.defvjp(low_keep, low_pass)
low_back.defvjp(back_keep, back_low)
EPS = 1e-06
HIGH = lax.Precision.HIGHEST

def layer_norm(values, gain, shift):
    mean = lax.optimization_barrier(jnp.mean(values, axis=-1, keepdims=True))
    centred = values - mean
    var = lax.optimization_barrier(jnp.mean(centred * centred, axis=-1, keepdims=True))
    return centred * lax.rsqrt(var + EPS) * gain + shift

def matmul(left, right):
    return jnp.dot(left, right, precision=HIGH)

def attend(query, key_rows, value_rows, crops):
    scores = low_back(jnp.einsum('qhd,khd->hqk', query, key_rows, precision=HIGH) * 0.125)
    same = crops[:, None] == crops[None, :]
    scores = jnp.where(same[None], scores, -1e+30)
    top = lax.optimization_barrier(jnp.max(scores, axis=-1, keepdims=True))
    expo = jnp.exp(scores - top)
    probs = low(expo / lax.optimization_barrier(jnp.sum(expo, axis=-1, keepdims=True)))
    return jnp.einsum('hqk,khd->qhd', probs, value_rows, precision=HIGH)

def block(params, inputs, crops):
    w_query, w_key, w_value, bias_query, bias_value, w_out, bias_out, gain_attn, shift_attn, gain_mlp, shift_mlp, w_up, bias_up, w_down, bias_down = params
    first = low(layer_norm(inputs, gain_attn, shift_attn))
    query = low(low_back(matmul(first, w_query) + bias_query))
    key_rows = low(low_back(matmul(first, w_key)))
    value_rows = low(low_back(matmul(first, w_value) + bias_value))
    groups = crops.shape[0]
    length = crops.shape[1]
    shape = (groups, length, HEADS, HEAD_DIM)
    mixed = jax.vmap(attend)(query.reshape(shape), key_rows.reshape(shape), value_rows.reshape(shape), crops)
    heads_out = low(low_back(mixed.reshape(groups * length, D)))
    hidden = inputs + low_back(matmul(heads_out, w_out)) + bias_out
    second = low(layer_norm(hidden, gain_mlp, shift_mlp))
    pre = low_back(matmul(second, w_up) + bias_up)
    active = low(jax.nn.gelu(pre, approximate=False))
    return hidden + low_back(matmul(active, w_down)) + bias_down

def reference(tokens, crop_ids, w_query, w_key, w_value, bias_query, bias_value, w_out, bias_out, gain_attn, shift_attn, gain_mlp, shift_mlp, w_up, bias_up, w_down, bias_down, cotangent):
    params = tuple((p.astype(jnp.float32) for p in (w_query, w_key, w_value, bias_query, bias_value, w_out, bias_out, gain_attn, shift_attn, gain_mlp, shift_mlp, w_up, bias_up, w_down, bias_down)))
    total_seqs = crop_ids.shape[0]
    group = 16 if total_seqs % 16 == 0 else 1
    count = total_seqs // group
    inputs = tokens.astype(jnp.float32).reshape(count, group * LEN, D)
    crops = crop_ids.reshape(count, group, LEN)
    grads_in = cotangent.astype(jnp.float32).reshape(count, group * LEN, D)
    start = tuple((jnp.zeros_like(p) for p in params))

    def step(totals, item):
        rows, crop_rows, grad_rows = item
        result, pull = jax.vjp(lambda pr, xs: block(pr, xs, crop_rows), params, rows)
        grad_params, grad_rows_in = pull(grad_rows)
        totals = tuple((a + b for a, b in zip(totals, grad_params)))
        return (totals, (result.astype(jnp.bfloat16), grad_rows_in))
    totals, (results, grad_inputs) = lax.scan(step, start, (inputs, crops, grads_in))
    block_out = results.reshape(TOKENS, D)
    grad_tokens = grad_inputs.reshape(TOKENS, D)
    g_wq, g_wk, g_wv, g_bq, g_bv, g_wo, g_bo, g_ga, g_sa, g_gm, g_sm, g_wu, g_bu, g_wd, g_bd = totals
    return (block_out, grad_tokens, g_wq, g_wk, g_wv, g_bq, g_bv, g_wo, g_bo, g_ga, g_sa, g_gm, g_sm, g_wu, g_bu, g_wd, g_bd)
```

```python
from functools import partial

import jax
import jax.numpy as jnp
from jax import lax
from jax.sharding import PartitionSpec as P

HEAD_DIM = 64
LEN = 256


EPS = 1e-06
NEGATIVE = -1e30


def norm_rows(values, gain, shift):
    mean = jnp.mean(values, axis=-1, keepdims=True)
    centred = values - mean
    var = jnp.mean(centred * centred, axis=-1, keepdims=True)
    scale = lax.rsqrt(var + EPS)
    unit = centred * scale
    return (unit * gain + shift, unit, scale)


def norm_back(grad_out, unit, scale, gain):
    grad_unit = grad_out * gain
    inner = jnp.mean(grad_unit * unit, axis=-1, keepdims=True)
    return scale * (grad_unit - jnp.mean(grad_unit, axis=-1, keepdims=True) - unit * inner)


def plain_dot(left, right):
    return jnp.dot(left, right, preferred_element_type=jnp.float32)


def right_trans(left, right):
    return lax.dot_general(
        left, right, (((1,), (1,)), ((), ())), preferred_element_type=jnp.float32
    )


def left_trans(left, right):
    return lax.dot_general(
        left, right, (((0,), (0,)), ((), ())), preferred_element_type=jnp.float32
    )


def scores_of(query, key_rows, crops):
    raw = jnp.einsum("qhd,khd->hqk", query, key_rows, preferred_element_type=jnp.float32) * 0.125
    same = crops[:, None] == crops[None, :]
    return jnp.where(same[None], raw, NEGATIVE)


def attend_block(item):
    query, key_rows, value_rows, crops = item
    scores = scores_of(query, key_rows, crops)
    top = jnp.max(scores, axis=-1, keepdims=True)
    expo = jnp.exp(scores - top)
    total = jnp.sum(expo, axis=-1, keepdims=True)
    probs = (expo / total).astype(jnp.bfloat16)
    mixed = jnp.einsum("hqk,khd->qhd", probs, value_rows, preferred_element_type=jnp.float32)
    return (mixed.astype(jnp.bfloat16), top + jnp.log(total))


def attend_back(item):
    query, key_rows, value_rows, crops, log_total, grad_mixed = item
    probs = jnp.exp(scores_of(query, key_rows, crops) - log_total)
    grad_value = jnp.einsum(
        "hqk,qhd->khd", probs.astype(jnp.bfloat16), grad_mixed, preferred_element_type=jnp.float32
    )
    grad_probs = jnp.einsum(
        "qhd,khd->hqk", grad_mixed, value_rows, preferred_element_type=jnp.float32
    )
    inner = jnp.sum(grad_probs * probs, axis=-1, keepdims=True)
    grad_scores = (probs * (grad_probs - inner)).astype(jnp.bfloat16)
    grad_query = (
        jnp.einsum("hqk,khd->qhd", grad_scores, key_rows, preferred_element_type=jnp.float32)
        * 0.125
    )
    grad_key = (
        jnp.einsum("hqk,qhd->khd", grad_scores, query, preferred_element_type=jnp.float32) * 0.125
    )
    return (
        grad_query.astype(jnp.bfloat16),
        grad_key.astype(jnp.bfloat16),
        grad_value.astype(jnp.bfloat16),
    )


def pair_swap(bit, count):
    return [(i, i ^ bit) for i in range(count)]


def relative_columns(width, count):
    rest = count // 4
    size = width // count
    here = lax.axis_index("dp")
    place = lax.broadcasted_iota(jnp.int32, (1, width), 1)
    block = place // size
    core = (here & 1) ^ (block // (2 * rest))
    side = ((here >> 1) & 1) ^ ((block // rest) & 1)
    far = ((here >> 2) + block) % rest
    source = (far * 4 + side * 2 + core) * size + place % size
    return (lax.broadcasted_iota(jnp.int32, (width, width), 0) == source).astype(jnp.bfloat16)


def scatter_sum(left, right, count):
    rest = count // 4
    quarter = left.shape[1] // 4
    parts = [left[:, i * quarter : (i + 1) * quarter] for i in range(4)]
    core = pair_swap(1, count)
    got_far = lax.ppermute(left_trans(parts[3], right), "dp", core)
    got_near = lax.ppermute(left_trans(parts[2], right), "dp", core)
    side = lax.ppermute(left_trans(parts[1], right) + got_far, "dp", pair_swap(2, count))
    total = left_trans(parts[0], right) + got_near + side
    size = quarter // rest
    slots = [total[i * size : (i + 1) * size] for i in range(rest)]
    up = [(i, i + 4) for i in range(count - 4)]
    down = [(i + 4, i) for i in range(count - 4)]
    for step in range(1, rest):
        top = rest - step
        ups = [(i, j) for i, j in up if i // 4 + top < rest]
        downs = [(i, j) for i, j in down if i // 4 - top >= 0]
        from_low = lax.ppermute(slots[top], "dp", ups)
        from_high = lax.ppermute(slots[step], "dp", downs)
        slots[top - 1] = slots[top - 1] + from_low
        slots[(step + 1) % rest] = slots[(step + 1) % rest] + from_high
    return slots[0]


def all_sum(values, count):
    bit = 1
    while bit < count:
        values = values + lax.ppermute(values, "dp", pair_swap(bit, count))
        bit *= 2
    return values


def swap(values):
    return lax.ppermute(values, "mp", [(0, 1), (1, 0)])


def body(
    tokens,
    crop_ids,
    w_query,
    w_key,
    w_value,
    bias_query,
    bias_value,
    w_out,
    bias_out,
    gain_attn,
    shift_attn,
    gain_mlp,
    shift_mlp,
    w_up,
    bias_up,
    w_down,
    bias_down,
    cotangent,
    count,
):
    rows = tokens.shape[0]
    local = w_query.shape[1]
    heads = local // HEAD_DIM
    seq_count = crop_ids.shape[0]
    pair = 2
    blocks = seq_count // pair
    block_rows = pair * LEN
    inputs = tokens.astype(jnp.float32)
    first, unit_one, scale_one = norm_rows(inputs, gain_attn, shift_attn)
    first = first.astype(jnp.bfloat16)
    query = (plain_dot(first, w_query) + bias_query).astype(jnp.bfloat16)
    key_rows = plain_dot(first, w_key).astype(jnp.bfloat16)
    value_rows = (plain_dot(first, w_value) + bias_value).astype(jnp.bfloat16)
    seq_base = lax.broadcasted_iota(jnp.int32, crop_ids.shape, 0) * LEN
    crop_keys = (crop_ids + seq_base).reshape(blocks, block_rows)

    def split(values):
        return values.reshape(blocks, block_rows, heads, HEAD_DIM)

    q_blocks = split(query)
    k_blocks = split(key_rows)
    v_blocks = split(value_rows)
    mixed, log_total = lax.map(attend_block, (q_blocks, k_blocks, v_blocks, crop_keys))
    heads_out = mixed.reshape(rows, local)
    mine = plain_dot(heads_out, w_out)
    attn = mine + swap(mine) + bias_out
    hidden = inputs + attn
    second, unit_two, scale_two = norm_rows(hidden, gain_mlp, shift_mlp)
    second = second.astype(jnp.bfloat16)
    pre = plain_dot(second, w_up) + bias_up
    active, gelu_pull = jax.vjp(partial(jax.nn.gelu, approximate=False), pre)
    active = active.astype(jnp.bfloat16)
    grad_out = cotangent.astype(jnp.float32)
    grad_bias_down = jnp.sum(grad_out, axis=0)
    grad_active = right_trans(cotangent, w_down)
    grad_pre = gelu_pull(grad_active)[0].astype(jnp.bfloat16)
    grad_bias_up = jnp.sum(grad_pre.astype(jnp.float32), axis=0)
    second_part = right_trans(grad_pre, w_up)
    grad_second = second_part + swap(second_part)
    mlp_part = plain_dot(active, w_down)
    mlp_part, second_part = lax.optimization_barrier((mlp_part, second_part))
    mlp_sum = mlp_part + swap(mlp_part)
    block_out = (hidden + mlp_sum + bias_down).astype(jnp.bfloat16)
    order = relative_columns(second.shape[1], count)

    def arranged(values):
        return plain_dot(values, order).astype(jnp.bfloat16)

    done_w_down = scatter_sum(arranged(cotangent), active, count).T
    done_w_up = scatter_sum(arranged(second), grad_pre, count)
    grad_gain_mlp = jnp.sum(grad_second * unit_two, axis=0)
    grad_shift_mlp = jnp.sum(grad_second, axis=0)
    grad_hidden = grad_out + norm_back(grad_second, unit_two, scale_two, gain_mlp)
    grad_bias_out = jnp.sum(grad_hidden, axis=0)
    hidden_low = grad_hidden.astype(jnp.bfloat16)
    grad_heads = right_trans(hidden_low, w_out).astype(jnp.bfloat16)
    grad_q, grad_k, grad_v = lax.map(
        attend_back, (q_blocks, k_blocks, v_blocks, crop_keys, log_total, split(grad_heads))
    )
    grad_q = grad_q.reshape(rows, local)
    grad_k = grad_k.reshape(rows, local)
    grad_v = grad_v.reshape(rows, local)
    grad_bias_query = jnp.sum(grad_q.astype(jnp.float32), axis=0)
    grad_bias_value = jnp.sum(grad_v.astype(jnp.float32), axis=0)
    partial_first = (
        right_trans(grad_q, w_query) + right_trans(grad_k, w_key) + right_trans(grad_v, w_value)
    )
    grad_first = partial_first + swap(partial_first)
    first_order = arranged(first)
    done_w_out = scatter_sum(arranged(hidden_low), heads_out, count).T
    grads = scatter_sum(first_order, jnp.concatenate([grad_q, grad_k, grad_v], axis=1), count)
    done_w_query = grads[:, :local]
    done_w_key = grads[:, local : 2 * local]
    done_w_value = grads[:, 2 * local :]
    grad_gain_attn = jnp.sum(grad_first * unit_one, axis=0)
    grad_shift_attn = jnp.sum(grad_first, axis=0)
    grad_tokens = grad_hidden + norm_back(grad_first, unit_one, scale_one, gain_attn)
    wide = [
        grad_gain_attn,
        grad_shift_attn,
        grad_bias_out,
        grad_gain_mlp,
        grad_shift_mlp,
        grad_bias_down,
        grad_bias_query,
        grad_bias_value,
        grad_bias_up,
    ]
    packed = all_sum(jnp.concatenate(wide).reshape(-1, 128), count).reshape(-1)
    width = grad_bias_out.shape[0]
    size = width // count
    here = lax.axis_index("dp") * size

    def own(i):
        return lax.dynamic_slice(packed, (i * width + here,), (size,))

    done_gain_attn, done_shift_attn, done_bias_out = own(0), own(1), own(2)
    done_gain_mlp, done_shift_mlp, done_bias_down = own(3), own(4), own(5)
    at = 6 * width
    done_bias_query = packed[at : at + local]
    done_bias_value = packed[at + local : at + 2 * local]
    done_bias_up = packed[at + 2 * local :]
    return (
        block_out,
        grad_tokens,
        done_w_query,
        done_w_key,
        done_w_value,
        done_bias_query,
        done_bias_value,
        done_w_out,
        done_bias_out,
        done_gain_attn,
        done_shift_attn,
        done_gain_mlp,
        done_shift_mlp,
        done_w_up,
        done_bias_up,
        done_w_down,
        done_bias_down,
    )


def solution(mesh):
    placed = (
        P("dp", None),
        P("dp", None),
        P(None, "mp"),
        P(None, "mp"),
        P(None, "mp"),
        P("mp"),
        P("mp"),
        P("mp", None),
        P(),
        P(),
        P(),
        P(),
        P(),
        P(None, "mp"),
        P("mp"),
        P("mp", None),
        P(),
        P("dp", None),
    )
    return jax.shard_map(
        partial(body, count=mesh.shape["dp"]),
        mesh=mesh,
        in_specs=placed,
        out_specs=(
            P("dp", None),
            P("dp", None),
            P("dp", "mp"),
            P("dp", "mp"),
            P("dp", "mp"),
            P("mp"),
            P("mp"),
            P("mp", "dp"),
            P("dp"),
            P("dp"),
            P("dp"),
            P("dp"),
            P("dp"),
            P("dp", "mp"),
            P("mp"),
            P("mp", "dp"),
            P("dp"),
        ),
        check_vma=False,
    )
```

```python
from functools import partial

import jax
import jax.numpy as jnp
from jax import lax
from jax.experimental import pallas as pl
from jax.experimental.pallas import tpu as pltpu
from jax.sharding import PartitionSpec as P

HEAD_DIM = 64
PAIR = 2 * HEAD_DIM
EPS = 1e-06
NEGATIVE = -1e30
LOW = jnp.bfloat16
HIGH = jnp.float32
VMEM = pl.BlockSpec(memory_space=pltpu.VMEM)


def plain_dot(left, right):
    return jnp.dot(left, right, preferred_element_type=HIGH)


def right_trans(left, right):
    return lax.dot_general(left, right, (((1,), (1,)), ((), ())), preferred_element_type=HIGH)


def left_trans(left, right):
    return lax.dot_general(left, right, (((0,), (0,)), ((), ())), preferred_element_type=HIGH)


def unit_rows(values):
    mean = jnp.mean(values, axis=-1, keepdims=True)
    centred = values - mean
    scale = lax.rsqrt(jnp.mean(centred * centred, axis=-1, keepdims=True) + EPS)
    return centred * scale, scale


def norm_back(grad_unit, unit, scale):
    inner = jnp.mean(grad_unit * unit, axis=-1, keepdims=True)
    return scale * (grad_unit - jnp.mean(grad_unit, axis=-1, keepdims=True) - unit * inner)


def half_masks():
    lane = lax.broadcasted_iota(jnp.int32, (1, PAIR), 1)
    first = lane < HEAD_DIM
    return first, (first.astype(HIGH).astype(LOW), (~first).astype(HIGH).astype(LOW))


def col_sum(values):
    return jnp.sum(values, axis=0, keepdims=True)


def front_kernel(*refs, length, seqs):
    sources, targets = refs[:9], refs[9:13]
    first_out, outs = refs[13], refs[14 : 14 + seqs]
    held, (q, k, v, lse), sems = refs[14 + seqs : -5], refs[-5:-1], refs[-1]
    copies = [pltpu.make_async_copy(a, b, sems.at[i]) for i, (a, b) in enumerate(zip(sources, held))]
    for copy in copies:
        copy.start()
    tokens, gain, shift, w_q, w_k, w_v, b_q, b_v, crops = held
    for copy in copies[:3]:
        copy.wait()
    unit, _ = unit_rows(tokens[...].astype(HIGH))
    first = (unit * row(gain) + row(shift)).astype(LOW)
    first_out[...] = first
    for copy in copies[3:]:
        copy.wait()
    q_all = ((plain_dot(first, w_q[...]) + row(b_q)).astype(LOW) * 0.125).astype(LOW)
    k_all = plain_dot(first, w_k[...]).astype(LOW)
    v_all = (plain_dot(first, w_v[...]) + row(b_v)).astype(LOW)
    q[...] = q_all
    k[...] = k_all
    v[...] = v_all
    stores = [
        pltpu.make_async_copy(a, b, sems.at[len(sources) + i])
        for i, (a, b) in enumerate(zip((q, k, v, lse), targets))
    ]
    for store in stores[:3]:
        store.start()
    low_half, masks = half_masks()
    for s, o in enumerate(outs):
        rows = slice(s * length, (s + 1) * length)
        same = same_crop(crops, s)
        for t in range(q_all.shape[1] // PAIR):
            at = slice(t * PAIR, (t + 1) * PAIR)
            q_pair, k_pair, v_pair = q_all[rows, at], k_all[rows, at], v_all[rows, at]
            got = []
            for half in range(2):
                scores = jnp.where(same, right_trans(q_pair * masks[half], k_pair), NEGATIVE)
                top = jnp.max(scores, axis=-1, keepdims=True)
                expo = jnp.exp(scores - top)
                total = jnp.sum(expo, axis=-1, keepdims=True)
                probs = (expo * (1.0 / total)).astype(LOW)
                got.append(plain_dot(probs, v_pair))
                h = 2 * t + half
                lse[rows, h : h + 1] = top + jnp.log(total)
            o[:, at] = jnp.where(low_half, got[0], got[1])
    stores[3].start()
    for store in stores:
        store.wait()


def turn_kernel(order, first, cotangent, a1_t, cot_t, sums):
    cot = cotangent[...]
    a1_t[...] = right_trans(order[...], first[...]).astype(LOW)
    cot_t[...] = right_trans(order[...], cot).astype(LOW)
    sums[...] = col_sum(cot.astype(HIGH))


def middle_kernel(*refs, blocks, seq, length, chained):
    place, tokens, o_own, o_other, w_out, b_out, gain, shift, w_up, b_up = refs[:10]
    w_down, cotangent, order = refs[10:13]
    pieces = refs[13:17]
    hidden, g_second, a2_t, active, g_pre, g_bias, w_low = refs[17 + 5 * chained :]
    rows = slice(seq * length, (seq + 1) * length)
    for b in range(4):
        size = pieces[b].shape[0]
        start = pl.multiple_of((place[0] ^ b) * size, size)
        w_low[pl.ds(start, size), :] = pieces[b][...].astype(LOW)
    attn = plain_dot(o_own[...].astype(LOW), w_out[...])
    attn = attn + plain_dot(o_other[...].astype(LOW), w_low[...])
    values = tokens[rows, :].astype(HIGH) + (attn + row(b_out))
    hidden[...] = values
    unit, _ = unit_rows(values)
    second = (unit * row(gain) + row(shift)).astype(LOW)
    cot = cotangent[rows, :]
    size = w_up.shape[1] // blocks
    total = None
    for b in range(blocks):
        at = slice(b * size, (b + 1) * size)
        pre = plain_dot(second, w_up[:, at]) + b_up[at].reshape(1, size)
        cdf = 0.5 * (1.0 + lax.erf(pre * 0.7071067811865476))
        active[rows, at] = (pre * cdf).astype(LOW)
        slope = cdf + pre * (0.3989422804014327 * jnp.exp(-0.5 * (pre * pre)))
        grad = (right_trans(cot, w_down[at, :]) * slope).astype(LOW)
        g_pre[rows, at] = grad
        bias = col_sum(grad.astype(HIGH))
        g_bias[:, at] = refs[21][:, at] + bias if chained else bias
        part = right_trans(grad, w_up[:, at])
        total = part if total is None else total + part
    g_second[rows, :] = total
    a2_t[:, rows] = right_trans(order[...], second).astype(LOW)


def back_kernel(*refs, seqs, length):
    tokens, crops, cotangent, own, other, gain, w_out, w_q, w_k, w_v = refs[:10]
    q, k, v, lse, order, g_bias, cot_sum = refs[10:17]
    hidden = refs[17 : 17 + seqs]
    g_hidden, g_first, gh_t, g_qkv, sums = refs[17 + seqs :]
    width, local = tokens.shape[1], q.shape[1]
    low_half, masks = half_masks()

    def put(s, r, at, value):
        sums[r : r + 1, at] = sums[r : r + 1, at] + value if s else value

    full = slice(0, width)
    for s in range(seqs):
        rows = slice(s * length, (s + 1) * length)
        unit, scale = unit_rows(hidden[s][...])
        grad = own[rows, :] + other[rows, :]
        put(s, 0, full, col_sum(grad * unit))
        put(s, 1, full, col_sum(grad))
        values = cotangent[rows, :].astype(HIGH) + norm_back(grad * row(gain), unit, scale)
        g_hidden[rows, :] = values
        put(s, 2, full, col_sum(values))
        low = values.astype(LOW)
        gh_t[:, rows] = right_trans(order[...], low).astype(LOW)
        g_o = right_trans(low, w_out[...]).astype(LOW)
        same = same_crop(crops, s)
        for t in range(local // PAIR):
            at = slice(t * PAIR, (t + 1) * PAIR)
            q_pair, k_pair, v_pair, o_pair = q[rows, at], k[rows, at], v[rows, at], g_o[:, at]
            got = []
            for half in range(2):
                h = 2 * t + half
                scores = right_trans(q_pair * masks[half], k_pair)
                probs = jnp.exp(jnp.where(same, scores, NEGATIVE) - lse[rows, h : h + 1])
                g_probs = right_trans(o_pair * masks[half], v_pair)
                inner = jnp.sum(g_probs * probs, axis=-1, keepdims=True)
                g_scores = (probs * (g_probs - inner)).astype(LOW)
                got.append(
                    (
                        plain_dot(g_scores, k_pair),
                        left_trans(g_scores, q_pair),
                        left_trans(probs.astype(LOW), o_pair),
                    )
                )
            g_q = (jnp.where(low_half, got[0][0], got[1][0]) * 0.125).astype(LOW)
            g_k = jnp.where(low_half, got[0][1], got[1][1]).astype(LOW)
            g_v = jnp.where(low_half, got[0][2], got[1][2]).astype(LOW)
            for i, part in enumerate((g_q, g_k, g_v)):
                g_qkv[rows, i * local + t * PAIR : i * local + (t + 1) * PAIR] = part
            put(s, 5, at, col_sum(g_q.astype(HIGH)))
            put(s, 5, slice(local + t * PAIR, local + (t + 1) * PAIR), col_sum(g_v.astype(HIGH)))
        part = right_trans(g_qkv[rows, :local], w_q[...])
        part = part + right_trans(g_qkv[rows, local : 2 * local], w_k[...])
        part = part + right_trans(g_qkv[rows, 2 * local :], w_v[...])
        g_first[rows, :] = part
        unit_one, _ = unit_rows(tokens[rows, :].astype(HIGH))
        put(s, 3, full, col_sum(part * unit_one))
        put(s, 4, full, col_sum(part))
    sums[6:7, :] = g_bias[:, :width]
    sums[7:8, :] = g_bias[:, width:]
    sums[8:9, :] = cot_sum[...]
    sums[9:, :] = jnp.zeros_like(sums[9:, :])


def last_kernel(tokens, gain, g_hidden, own, other, g_tokens):
    unit, scale = unit_rows(tokens[...].astype(HIGH))
    grad = own[...] + other[...]
    g_tokens[...] = g_hidden[...] + norm_back(grad * row(gain), unit, scale)


def out_kernel(*refs, seqs, length):
    bias, own, other = refs[:3]
    for s in range(seqs):
        rows = slice(s * length, (s + 1) * length)
        total = refs[3 + s][...] + (own[rows, :] + other[rows, :])
        refs[3 + seqs][rows, :] = (total + row(bias)).astype(LOW)


def dot_kernel(left, right, *refs, start, with_add):
    outs = refs[with_add:]
    for o, out in enumerate(outs):
        size = out.shape[0]
        at = slice(start + o * size, start + (o + 1) * size)
        step = min(512, right.shape[1])
        for n in range(0, right.shape[1], step):
            value = plain_dot(left[at, :], right[:, n : n + step])
            if with_add:
                part = refs[0].shape[0]
                if size > part:
                    got = [r[:, n : n + step] for r in refs[o * size // part : (o + 1) * size // part]]
                    value = value + jnp.concatenate(got)
                else:
                    low = o * size % part
                    value = value + refs[o * size // part][low : low + size, n : n + step]
            out[:, n : n + step] = value


def add_kernel(left, right, *outs):
    size = outs[0].shape[0]
    if left.shape[0] != size * len(outs):
        wide = outs[0].shape[1]
        for o, out in enumerate(outs):
            at = slice(o * wide, (o + 1) * wide)
            out[...] = left[:, at] + right[:, at]
        return
    for o, out in enumerate(outs):
        at = slice(o * size, (o + 1) * size)
        out[...] = left[at, :] + right[at, :]


def small_kernel(sums, other, out):
    out[...] = sums[...]
    out[3:5, :] = sums[3:5, :] + other[...]


def row(ref):
    return ref[...].reshape(1, ref.shape[0])


def same_crop(crops, seq):
    ids = crops[seq : seq + 1, :]
    marks = lax.broadcasted_iota(jnp.int32, (16, ids.shape[1]), 0) == ids
    marks = marks.astype(HIGH).astype(LOW)
    return left_trans(marks, marks) > 0.5


class Steps:
    def __init__(self):
        self.last = None

    def __call__(self, kernel, name, outs, args, scratch=(), limit=12, smem=0, tie=0, alias=None, whole=0, whole_out=0):
        args = list(args)
        if self.last is not None:
            args[tie], _ = lax.optimization_barrier((args[tie], self.last))
        result = pl.pallas_call(
            kernel,
            name=name,
            out_shape=[jax.ShapeDtypeStruct(s, d) for s, d in outs],
            in_specs=[pl.BlockSpec(memory_space=pltpu.SMEM)] * smem
            + [pl.BlockSpec(memory_space=pl.ANY)] * whole
            + [VMEM] * (len(args) - smem - whole),
            out_specs=[pl.BlockSpec(memory_space=pl.ANY)] * whole_out
            + [VMEM] * (len(outs) - whole_out),
            scratch_shapes=list(scratch),
            input_output_aliases=alias or {},
            compiler_params=pltpu.CompilerParams(vmem_limit_bytes=limit << 20),
            cost_estimate=pl.CostEstimate(flops=1000, bytes_accessed=1000, transcendentals=0),
        )(*args)
        self.last = result[0]
        return result


def pair_swap(bit, count):
    return [(i, i ^ bit) for i in range(count)]


def relative_rows(width, count, side_first):
    rest = count // 4
    size = width // count
    here = lax.axis_index("dp")
    place = lax.broadcasted_iota(jnp.int32, (width, 1), 0)
    block = place // size
    core = (here & 1) ^ (block // (2 * rest))
    inner = block % (2 * rest)
    side, far = (inner // rest, inner % rest) if side_first else (inner % 2, inner // 2)
    side = ((here >> 1) & 1) ^ side
    own = here >> 2
    if rest == 4:
        half = (own >= 2).astype(jnp.int32)
        mid = 1 + half
        edge = 3 * half
        far = jnp.where(far < 2, own ^ far, jnp.where(far == 2, 3 - mid, 3 - edge))
    else:
        far = own ^ far
    source = (far * 4 + side * 2 + core) * size + place % size
    return (lax.broadcasted_iota(jnp.int32, (width, width), 1) == source).astype(LOW)


def send(values, pairs):
    return lax.ppermute(values, "dp", pairs)


def swap(values):
    return lax.ppermute(values, "mp", [(0, 1), (1, 0)])


class Scatter:
    def __init__(self, steps, count, left, right, side_first, wide=1):
        self.steps, self.count, self.left, self.right = steps, count, left, right
        self.side_first, self.wide = side_first, wide
        self.columns = right.shape[1]
        self.half = left.shape[0] // 2

    def dot(self, start, added, sizes):
        outs = [((n, self.columns), HIGH) for n in sizes]
        kernel = partial(dot_kernel, start=start, with_add=len(added))
        return self.steps(kernel, "grad", outs, [self.left, self.right] + added)

    def add(self, left, right, pieces=1, wide=1):
        shape = (left.shape[0] // pieces, left.shape[1] // wide)
        return self.steps(add_kernel, "sum", [(shape, HIGH)] * (pieces * wide), [left, right])

    def start(self):
        parts = self.dot(self.half, [], [self.half // 2] * 2)
        self.far = [send(p, pair_swap(1, self.count)) for p in parts]

    def near(self):
        if self.side_first:
            self.keep, sent = self.dot(0, self.far, [self.half // 2] * 2)
            self.side = send(sent, pair_swap(2, self.count))
        elif self.count == 16:
            self.slots = self.dot(0, self.far, [self.half // 4] * 4)
            self.edges()
        else:
            self.keep = self.dot(0, self.far, [self.half])[0]

    def sides(self):
        if self.count == 16:
            self.slots = self.add(self.keep, self.side, 4)
            self.edges()
        else:
            self.keep = self.add(self.keep, self.side)[0]

    def edges(self):
        pairs = [(i, i ^ 4) for i in range(16) if i // 4 in (0, 3)]
        self.beyond = [send(self.slots[i], pairs) for i in (3, 2)]

    def mids(self, i):
        if self.count != 16:
            return
        pairs = [(i, i ^ 12) for i in range(16) if i // 4 in (1, 2)]
        total = self.add(self.slots[3 - i], self.beyond[i])[0]
        self.beyond[i] = send(total, pairs)

    def pairs(self):
        if self.count != 16:
            return
        total = self.add(self.slots[1], self.beyond[0])[0]
        self.near_sum = send(total, pair_swap(4, 16))

    def own(self):
        if self.count != 16:
            return
        self.keep = self.add(self.slots[0], self.beyond[1])[0]

    def finish(self):
        if self.count != 16:
            slots, bit = self.keep, self.count // 8
            while bit:
                part = slots.shape[0] // 2
                slots = slots[:part] + send(slots[part:], pair_swap(4 * bit, self.count))
                bit //= 2
            if not self.side_first:
                part = slots.shape[0] // 2
                slots = slots[:part] + send(slots[part:], pair_swap(2, self.count))
            wide = self.columns // self.wide
            return [slots[:, i * wide : (i + 1) * wide] for i in range(self.wide)]
        if self.side_first:
            return self.add(self.keep, self.near_sum, 1, self.wide)
        self.keep, sent = self.add(self.keep, self.near_sum, 2)
        self.side = send(sent, pair_swap(2, 16))
        return None

    def close(self):
        if self.count != 16:
            return self.finish()
        return self.add(self.keep, self.side, 1, self.wide)


def body(
    tokens,
    crop_ids,
    w_query,
    w_key,
    w_value,
    bias_query,
    bias_value,
    w_out,
    bias_out,
    gain_attn,
    shift_attn,
    gain_mlp,
    shift_mlp,
    w_up,
    bias_up,
    w_down,
    bias_down,
    cotangent,
    count,
):
    width = tokens.shape[1]
    local = w_query.shape[1]
    hidden_units = w_up.shape[1]
    seqs, length = crop_ids.shape
    rows = seqs * length
    here = lax.axis_index("dp")
    place = here & 3
    steps = Steps()

    piece = local // 4
    mine = lax.dynamic_slice(w_out, (place * piece, 0), (piece, width)).astype(HIGH)
    got = swap(mine)

    loaded = [
        tokens,
        gain_attn,
        shift_attn,
        w_query,
        w_key,
        w_value,
        bias_query,
        bias_value,
        crop_ids,
    ]
    kept = [((rows, local), LOW)] * 3 + [((rows, 128), HIGH)]
    front = steps(
        partial(front_kernel, length=length, seqs=seqs),
        "front",
        kept + [((rows, width), LOW)] + [((length, local), HIGH)] * seqs,
        loaded,
        scratch=[pltpu.VMEM(a.shape, a.dtype) for a in loaded]
        + [pltpu.VMEM(*k) for k in kept]
        + [pltpu.SemaphoreType.DMA((len(loaded) + len(kept),))],
        whole=len(loaded),
        whole_out=len(kept),
        limit=52,
    )
    query, key_rows, value_rows, log_total, first = front[:5]
    mixed = front[5:]
    mixed_other = [swap(o) for o in mixed]

    o_low = jnp.concatenate([o.astype(LOW) for o in mixed])
    side_order = relative_rows(width, count, True)
    far_order = relative_rows(width, count, False)
    beside = send(got, pair_swap(2, count))
    pieces = [got, send(got, pair_swap(1, count)), beside, send(beside, pair_swap(1, count))]
    a1_t, cot_t, cot_sum = steps(
        turn_kernel,
        "turn",
        [((width, rows), LOW)] * 2 + [((1, width), HIGH)],
        [side_order, first, cotangent],
    )

    shared = [
        ((rows, width), HIGH),
        ((width, rows), LOW),
        ((rows, hidden_units), LOW),
        ((rows, hidden_units), LOW),
        ((1, hidden_units), HIGH),
    ]
    hidden, carried = [], []
    for s in range(seqs):
        result = steps(
            partial(middle_kernel, blocks=3, seq=s, length=length, chained=s > 0),
            "middle",
            [((length, width), HIGH)] + shared,
            [
                place.reshape(1),
                tokens,
                mixed[s],
                mixed_other[s],
                w_out,
                bias_out,
                gain_mlp,
                shift_mlp,
                w_up,
                bias_up,
                w_down,
                cotangent,
                far_order,
            ]
            + pieces
            + carried,
            scratch=[pltpu.VMEM((local, width), LOW)],
            smem=1,
            tie=2,
            alias={17 + i: 1 + i for i in range(5)} if s else None,
        )
        hidden.append(result[0])
        carried = list(result[1:])
    second, a2_t, active, g_pre, bias_sum = carried
    second_other = swap(second)

    down = Scatter(steps, count, cot_t, active, True)
    up = Scatter(steps, count, a2_t, g_pre, False)
    down.start()
    up.start()
    mlp_part = steps(
        partial(dot_kernel, start=0, with_add=0), "mlp", [((rows, width), HIGH)], [active, w_down]
    )[0]
    mlp_other = swap(mlp_part)
    down.near()
    up.near()

    up.mids(0)
    down.sides()
    g_hidden, g_first, gh_t, g_qkv, sums = steps(
        partial(back_kernel, seqs=seqs, length=length),
        "back",
        [((rows, width), HIGH)] * 2
        + [((width, rows), LOW), ((rows, 3 * local), LOW), ((16, width), HIGH)],
        [
            tokens,
            crop_ids,
            cotangent,
            second,
            second_other,
            gain_mlp,
            w_out,
            w_query,
            w_key,
            w_value,
            query,
            key_rows,
            value_rows,
            log_total,
            far_order,
            bias_sum,
            cot_sum,
        ]
        + hidden,
        tie=3,
    )
    heads_grad = Scatter(steps, count, a1_t, g_qkv, True, 3)
    out_grad = Scatter(steps, count, gh_t, o_low, False)
    first_other = swap(g_first)
    finals = {}

    def keep(name, act):
        finals[name] = act()

    def write_out():
        return steps(
            partial(out_kernel, seqs=seqs, length=length),
            "out",
            [((rows, width), LOW)],
            [bias_down, mlp_part, mlp_other] + hidden,
            tie=1,
        )[0]

    turns = [
        [lambda: up.mids(1), up.pairs, lambda: down.mids(0), lambda: down.mids(1)],
        [heads_grad.start, out_grad.start],
        [heads_grad.near, out_grad.near, up.own, down.pairs],
        [up.finish, down.own, lambda: keep("out", write_out)],
        [lambda: out_grad.mids(0), lambda: out_grad.mids(1), out_grad.pairs, out_grad.own],
        [heads_grad.sides, lambda: keep("down", down.finish), out_grad.finish],
        [lambda: heads_grad.mids(0), lambda: heads_grad.mids(1)],
        [lambda: keep("up", up.close), heads_grad.pairs, heads_grad.own],
        [lambda: keep("wo", out_grad.close), lambda: keep("heads", heads_grad.finish)],
    ]
    small, bit = sums, 1
    for acts in turns:
        got = send(small, pair_swap(bit, count)) if bit < count else None
        for act in acts:
            act()
        if bit < count:
            small = steps(add_kernel, "small", [((16, width), HIGH)], [small, got])[0]
        bit *= 2
    while bit < count:
        got = send(small, pair_swap(bit, count))
        small = steps(add_kernel, "small", [((16, width), HIGH)], [small, got])[0]
        bit *= 2
    block_out, grads = finals["out"], finals["heads"]
    done_w_down, done_w_up, done_w_out = finals["down"][0].T, finals["up"][0], finals["wo"][0].T
    small_other = swap(small[3:5])
    grad_tokens = steps(
        last_kernel,
        "last",
        [((rows, width), HIGH)],
        [tokens, gain_attn, g_hidden, g_first, first_other],
        tie=3,
    )[0]
    packed = steps(small_kernel, "packed", [((16, width), HIGH)], [small, small_other])[0]
    size = width // count
    blocks = lax.dynamic_slice(packed, (0, here * size), (9, size))
    return (
        block_out,
        grad_tokens,
        grads[0],
        grads[1],
        grads[2],
        packed[5, :local],
        packed[5, local:],
        done_w_out,
        blocks[2],
        blocks[3],
        blocks[4],
        blocks[0],
        blocks[1],
        done_w_up,
        packed[6:8].reshape(-1),
        done_w_down,
        blocks[8],
    )


def solution(mesh):
    placed = (
        P("dp", None),
        P("dp", None),
        P(None, "mp"),
        P(None, "mp"),
        P(None, "mp"),
        P("mp"),
        P("mp"),
        P("mp", None),
        P(),
        P(),
        P(),
        P(),
        P(),
        P(None, "mp"),
        P("mp"),
        P("mp", None),
        P(),
        P("dp", None),
    )
    return jax.shard_map(
        partial(body, count=mesh.shape["dp"]),
        mesh=mesh,
        in_specs=placed,
        out_specs=(
            P("dp", None),
            P("dp", None),
            P("dp", "mp"),
            P("dp", "mp"),
            P("dp", "mp"),
            P("mp"),
            P("mp"),
            P("mp", "dp"),
            P("dp"),
            P("dp"),
            P("dp"),
            P("dp"),
            P("dp"),
            P("dp", "mp"),
            P("mp"),
            P("mp", "dp"),
            P("dp"),
        ),
        check_vma=False,
    )
```

```python
from functools import partial

import jax
import jax.numpy as jnp
from jax import lax
from jax.experimental import pallas as pl
from jax.experimental.pallas import tpu as pltpu
from jax.sharding import PartitionSpec as P

HEAD_DIM = 64
PAIR = 2 * HEAD_DIM
EPS = 1e-06
NEGATIVE = -1e30
LOW = jnp.bfloat16
HIGH = jnp.float32
VMEM = pl.BlockSpec(memory_space=pltpu.VMEM)
SMALL = 16
GAIN_ATTN, SHIFT_ATTN, BIAS_Q, BIAS_V, BIAS_OUT, GAIN_MLP, SHIFT_MLP, BIAS_DOWN, BIAS_UP = range(9)


def plain_dot(left, right):
    return jnp.dot(left, right, preferred_element_type=HIGH)


def right_trans(left, right):
    return lax.dot_general(left, right, (((1,), (1,)), ((), ())), preferred_element_type=HIGH)


def left_trans(left, right):
    return lax.dot_general(left, right, (((0,), (0,)), ((), ())), preferred_element_type=HIGH)


def unit_rows(values):
    mean = jnp.mean(values, axis=-1, keepdims=True)
    centred = values - mean
    scale = lax.rsqrt(jnp.mean(centred * centred, axis=-1, keepdims=True) + EPS)
    return centred * scale, scale


def norm_back(grad_unit, unit, scale):
    inner = jnp.mean(grad_unit * unit, axis=-1, keepdims=True)
    return scale * (grad_unit - jnp.mean(grad_unit, axis=-1, keepdims=True) - unit * inner)


def half_masks():
    lane = lax.broadcasted_iota(jnp.int32, (1, PAIR), 1)
    first = lane < HEAD_DIM
    return first, (first.astype(HIGH).astype(LOW), (~first).astype(HIGH).astype(LOW))


def col_sum(values):
    return jnp.sum(values, axis=0, keepdims=True)


def row(table, at, size):
    return table[at : at + 1, :size]


def same_crop(table, slot, length):
    ids = row(table, slot, length)
    marks = lax.broadcasted_iota(jnp.int32, (SMALL, length), 0).astype(HIGH) == ids
    marks = marks.astype(HIGH).astype(LOW)
    return left_trans(marks, marks) > 0.5


def copies_of(sources, targets, sems):
    copies = [pltpu.make_async_copy(a, b, sems.at[i]) for i, (a, b) in enumerate(zip(sources, targets))]
    for copy in copies:
        copy.start()
    return copies


def load_kernel(here, w_out, crops, *refs):
    count = (len(refs) - 5) // 2
    vectors, (piece, table), sems = refs[:count], refs[count : count + 2], refs[-1]
    held = refs[count + 2 : -1]
    size = piece.shape[0]
    start = pl.multiple_of((here[0] & 3) * size, size)
    sources = [w_out.at[pl.ds(start, size), :], crops, *vectors]
    copies = copies_of(sources, held, sems)
    copies[0].wait()
    piece[...] = held[0][...].astype(HIGH)
    for copy in copies[1:]:
        copy.wait()
    table[...] = jnp.zeros_like(table)
    at, width = 0, table.shape[1]
    for vector in held[2:]:
        for low in range(0, vector.shape[0], width):
            part = min(width, vector.shape[0] - low)
            table[at : at + 1, :part] = vector[low : low + part].reshape(1, part)
            at += 1
    seqs, length = held[1].shape
    table[at : at + seqs, :length] = held[1][...].astype(HIGH)


def front_kernel(*refs, length, seqs, crops):
    sources, table, held = refs[:4], refs[4], refs[5:9]
    first_out, q, k, v, lse = refs[9:14]
    outs, sems = refs[14:-1], refs[-1]
    copies = copies_of(sources, held, sems)
    tokens, w_q, w_k, w_v = held
    copies[0].wait()
    unit, _ = unit_rows(tokens[...].astype(HIGH))
    local, width = w_q.shape[1], tokens.shape[1]
    first = (unit * row(table, GAIN_ATTN, width) + row(table, SHIFT_ATTN, width)).astype(LOW)
    first_out[...] = first
    for copy in copies[1:]:
        copy.wait()
    q_all = plain_dot(first, w_q[...]) + row(table, BIAS_Q, local)
    q_all = (q_all.astype(LOW) * 0.125).astype(LOW)
    k_all = plain_dot(first, w_k[...]).astype(LOW)
    v_all = (plain_dot(first, w_v[...]) + row(table, BIAS_V, local)).astype(LOW)
    q[...] = q_all
    k[...] = k_all
    v[...] = v_all
    low_half, masks = half_masks()
    for s, o in enumerate(outs):
        rows = slice(s * length, (s + 1) * length)
        same = same_crop(table, crops + s, length)
        for t in range(local // PAIR):
            at = slice(t * PAIR, (t + 1) * PAIR)
            q_pair, k_pair, v_pair = q_all[rows, at], k_all[rows, at], v_all[rows, at]
            got = []
            for half in range(2):
                scores = jnp.where(same, right_trans(q_pair * masks[half], k_pair), NEGATIVE)
                top = jnp.max(scores, axis=-1, keepdims=True)
                expo = jnp.exp(scores - top)
                total = jnp.sum(expo, axis=-1, keepdims=True)
                probs = (expo * (1.0 / total)).astype(LOW)
                got.append(plain_dot(probs, v_pair))
                h = 2 * t + half
                lse[rows, h : h + 1] = top + jnp.log(total)
            o[:, at] = jnp.where(low_half, got[0], got[1])


def relative_rows(here, width, count, bits):
    size = width // count
    place = lax.broadcasted_iota(jnp.int32, (width, 1), 0)
    block = ((place.astype(HIGH) + 0.5) * (1.0 / size)).astype(jnp.int32)
    mask = jnp.zeros_like(block)
    for p, bit in enumerate(bits):
        mask = mask + (((block >> (len(bits) - 1 - p)) & 1) << bit)
    source = (mask ^ here) * size + (place - block * size)
    marks = lax.broadcasted_iota(jnp.int32, (width, width), 1) == source
    return marks.astype(HIGH).astype(LOW)


def turn_kernel(here, first, *refs, count, orders):
    sources, held = refs[:4], refs[4:8]
    order_b, sums, sems = refs[8], refs[9], refs[-1]
    seqs = (len(refs) - 11) // 3
    a1_a, a1_b, cot_a = (refs[10 + i * seqs : 10 + (i + 1) * seqs] for i in range(3))
    length = first.shape[0] // seqs
    copies = copies_of(sources, held, sems)
    width = first.shape[1]
    order_a = relative_rows(here[0], width, count, orders[0])
    order = relative_rows(here[0], width, count, orders[1])
    order_b[...] = order
    for s in range(seqs):
        part = first[s * length : (s + 1) * length, :]
        a1_a[s][...] = right_trans(order_a, part).astype(LOW)
        a1_b[s][...] = right_trans(order, part).astype(LOW)
    for copy in copies:
        copy.wait()
    cot = held[0][...]
    for s in range(seqs):
        part = cot[s * length : (s + 1) * length, :]
        cot_a[s][...] = right_trans(order_a, part).astype(LOW)
    sums[...] = col_sum(cot.astype(HIGH))


def middle_kernel(*refs, blocks, seq, length):
    here, tokens, o_own, o_other, w_out, table, w_up, w_down, cotangent, order = refs[:10]
    hidden, a2_t, active, g_pre, g_bias, g_second, w_low = refs[-7:]
    rows = slice(seq * length, (seq + 1) * length)
    if seq:
        bias_before, second_before, w_before = refs[10:13]
        g_second[: seq * length, :] = second_before[...]
        w_low[...] = w_before[...]
    else:
        for b, piece in enumerate(refs[10:14]):
            size = piece.shape[0]
            start = pl.multiple_of(((here[0] & 3) ^ b) * size, size)
            w_low[pl.ds(start, size), :] = piece[...].astype(LOW)
    attn = plain_dot(o_own[...].astype(LOW), w_out[...])
    attn = attn + plain_dot(o_other[...].astype(LOW), w_low[...])
    width = tokens.shape[1]
    values = tokens[rows, :].astype(HIGH) + (attn + row(table, BIAS_OUT, width))
    hidden[...] = values
    unit, _ = unit_rows(values)
    second = (unit * row(table, GAIN_MLP, width) + row(table, SHIFT_MLP, width)).astype(LOW)
    cot = cotangent[rows, :]
    size = w_up.shape[1] // blocks
    total = None
    for b in range(blocks):
        at = slice(b * size, (b + 1) * size)
        low = b * size % width
        at_row = BIAS_UP + b * size // width
        bias_up = table[at_row : at_row + 1, low : low + size]
        pre = plain_dot(second, w_up[:, at]) + bias_up
        cdf = 0.5 * (1.0 + lax.erf(pre * 0.7071067811865476))
        active[:, at] = (pre * cdf).astype(LOW)
        slope = cdf + pre * (0.3989422804014327 * jnp.exp(-0.5 * (pre * pre)))
        grad = (right_trans(cot, w_down[at, :]) * slope).astype(LOW)
        g_pre[:, at] = grad
        bias = col_sum(grad.astype(HIGH))
        g_bias[:, at] = bias_before[:, at] + bias if seq else bias
        part = right_trans(grad, w_up[:, at])
        total = part if total is None else total + part
    g_second[rows, :] = total
    a2_t[...] = right_trans(order[...], second).astype(LOW)


def turn_back_kernel(*refs, seqs, length):
    table, cotangent, own, other, order, g_bias, cot_sum = refs[:7]
    hidden = refs[7 : 7 + seqs]
    g_hidden, gh, sums = refs[7 + seqs : 10 + seqs]
    gh_t = refs[10 + seqs :]
    width = cotangent.shape[1]
    totals = [0.0, 0.0, 0.0]
    for s in range(seqs):
        rows = slice(s * length, (s + 1) * length)
        unit, scale = unit_rows(hidden[s][...])
        grad = own[rows, :] + other[rows, :]
        values = norm_back(grad * row(table, GAIN_MLP, width), unit, scale)
        values = cotangent[rows, :].astype(HIGH) + values
        g_hidden[rows, :] = values
        low = values.astype(LOW)
        gh[rows, :] = low
        gh_t[s][...] = right_trans(order[...], low).astype(LOW)
        parts = (col_sum(grad * unit), col_sum(grad), col_sum(values))
        totals = [a + b for a, b in zip(totals, parts)]
    for i, total in enumerate(totals):
        sums[i : i + 1, :] = total
    sums[3:6, :] = jnp.zeros((3, width), HIGH)
    sums[6:7, :] = g_bias[:, :width]
    sums[7:8, :] = g_bias[:, width:]
    sums[8:9, :] = cot_sum[...]
    sums[9:, :] = jnp.zeros_like(sums[9:, :])


def back_kernel(*refs, seqs, length, crops):
    tokens, table, gh, w_out, w_q, w_k, w_v, q, k, v, lse, _ = refs[:12]
    sums, g_first = refs[12:14]
    g_qk, g_val = (refs[14 + i * seqs : 14 + (i + 1) * seqs] for i in range(2))
    width, local = tokens.shape[1], q.shape[1]
    low_half, masks = half_masks()
    full = slice(0, width)
    before = refs[11]
    sums[:3, :] = before[:3, :]
    sums[6:, :] = before[6:, :]

    def put(s, r, at, value):
        sums[r : r + 1, at] = sums[r : r + 1, at] + value if s else value

    for s in range(seqs):
        rows = slice(s * length, (s + 1) * length)
        g_o = right_trans(gh[rows, :], w_out[...]).astype(LOW)
        same = same_crop(table, crops + s, length)
        for t in range(local // PAIR):
            at = slice(t * PAIR, (t + 1) * PAIR)
            q_pair, k_pair, v_pair, o_pair = q[rows, at], k[rows, at], v[rows, at], g_o[:, at]
            got = []
            for half in range(2):
                h = 2 * t + half
                scores = right_trans(q_pair * masks[half], k_pair)
                probs = jnp.exp(jnp.where(same, scores, NEGATIVE) - lse[rows, h : h + 1])
                g_probs = right_trans(o_pair * masks[half], v_pair)
                inner = jnp.sum(g_probs * probs, axis=-1, keepdims=True)
                g_scores = (probs * (g_probs - inner)).astype(LOW)
                got.append(
                    (
                        plain_dot(g_scores, k_pair),
                        left_trans(g_scores, q_pair),
                        left_trans(probs.astype(LOW), o_pair),
                    )
                )
            g_q = (jnp.where(low_half, got[0][0], got[1][0]) * 0.125).astype(LOW)
            g_k = jnp.where(low_half, got[0][1], got[1][1]).astype(LOW)
            g_v = jnp.where(low_half, got[0][2], got[1][2]).astype(LOW)
            beside = slice(local + t * PAIR, local + (t + 1) * PAIR)
            g_qk[s][:, at] = g_q
            g_qk[s][:, beside] = g_k
            g_val[s][:, at] = g_v
            put(s, 5, at, col_sum(g_q.astype(HIGH)))
            put(s, 5, beside, col_sum(g_v.astype(HIGH)))
        part = right_trans(g_qk[s][:, :local], w_q[...])
        part = part + right_trans(g_qk[s][:, local:], w_k[...])
        part = part + right_trans(g_val[s][...], w_v[...])
        g_first[rows, :] = part
        unit_one, _ = unit_rows(tokens[rows, :].astype(HIGH))
        put(s, 3, full, col_sum(part * unit_one))
        put(s, 4, full, col_sum(part))


def base_kernel(table, tokens, g_hidden, own, base, unit_out, scale_out, *, length):
    gain = row(table, GAIN_ATTN, tokens.shape[1])
    for s in range(tokens.shape[0] // length):
        rows = slice(s * length, (s + 1) * length)
        part = own[rows, :]
        unit, scale = unit_rows(tokens[rows, :].astype(HIGH))
        base[rows, :] = g_hidden[rows, :] + norm_back(part * gain, unit, scale)
        unit_out[rows, :] = unit
        scale_out[rows, :] = scale


def last_kernel(table, base, unit, scale, other, g_tokens, *, length):
    gain = row(table, GAIN_ATTN, base.shape[1])
    for s in range(base.shape[0] // length):
        rows = slice(s * length, (s + 1) * length)
        grad = norm_back(other[rows, :] * gain, unit[rows, :], scale[rows, :])
        g_tokens[rows, :] = base[rows, :] + grad


def out_kernel(*refs, seqs, length):
    table, own, other = refs[:3]
    for s in range(seqs):
        rows = slice(s * length, (s + 1) * length)
        total = refs[3 + s][...] + (own[rows, :] + other[rows, :])
        refs[3 + seqs][rows, :] = (total + row(table, BIAS_DOWN, total.shape[1])).astype(LOW)


def mlp_kernel(w_down, *refs):
    length = refs[0].shape[0]
    for s, active in enumerate(refs[:-1]):
        refs[-1][s * length : (s + 1) * length, :] = plain_dot(active[...], w_down[...])


def products(plan, refs, at):
    for lefts, rights, column in plan:
        wide = refs[rights[0]].shape[1]
        step = min(512, wide)
        for n in range(0, wide, step):
            value = None
            for left, right in zip(lefts, rights):
                part = plain_dot(refs[left][at, :], refs[right][:, n : n + step].astype(LOW))
                value = part if value is None else value + part
            yield slice(column + n, column + n + step), value


def far_kernel(*refs, plan, start, pieces, small):
    outs = refs[-pieces:]
    size = start // pieces
    for o, out in enumerate(outs):
        at = slice(start + o * size, start + (o + 1) * size)
        for columns, value in products(plan, refs, at):
            out[:size, columns] = value
    if small:
        outs[0][size:, :] = refs[-pieces - 1][...]


def near_kernel(*refs, plan, pieces, small):
    outs, got = refs[-2:], refs[-2 - pieces - small :]
    half = outs[0].shape[0]
    for o, out in enumerate(outs):
        at = slice(o * half, (o + 1) * half)
        size = 2 * half // pieces
        low = o * half % size
        for columns, value in products(plan, refs, at):
            out[:half, columns] = value + got[o * half // size][low : low + half, columns]
    if small:
        outs[1][half:, :] = got[pieces][...] + got[0][2 * half // pieces :, :]


def step_kernel(*refs, small, joined):
    count = 2 if joined else 1
    keeps, sents, gots = (refs[i * count : (i + 1) * count] for i in range(3))
    outs = refs[3 * count :]
    at = 0
    for i in range(count):
        half = outs[i].shape[0]
        got = gots[i]
        outs[i][...] = keeps[i][:half, :] + got[:half, :]
        outs[count][at : at + half, :] = keeps[i][half:, :] + got[half : 2 * half, :]
        at += half
        if small and not i:
            outs[count][at : at + SMALL, :] = sents[i][2 * half :, :] + got[2 * half :, :]
            at += SMALL


def end_kernel(*refs, wide, small):
    keeps, (sent, got), outs = refs[:2], refs[2:4], refs[4:]
    at = o = 0
    for keep in keeps:
        size, each = keep.shape[0], keep.shape[1] // wide
        for w in range(wide):
            columns = slice(w * each, (w + 1) * each)
            outs[o][...] = keep[:, columns] + got[at : at + size, columns]
            o += 1
        at += size
        if small and at == size:
            total = sent[at : at + SMALL, :] + got[at : at + SMALL, :]
            outs[-2][...] = total
            outs[-1][...] = total[3:5, :]
            at += SMALL


def gain_kernel(small, other, out):
    out[...] = small[...]
    out[3:5, :] = small[3:5, :] + other[...]


class Steps:
    def __init__(self):
        self.last = None

    def __call__(
        self, kernel, name, outs, args, scratch=(), limit=12, smem=0, whole=0, tie=0, alias=None, cost=0
    ):
        args = list(args)
        if self.last is not None:
            args[tie], _ = lax.optimization_barrier((args[tie], self.last))
        result = pl.pallas_call(
            kernel,
            name=name,
            out_shape=[jax.ShapeDtypeStruct(s, d) for s, d in outs],
            in_specs=[pl.BlockSpec(memory_space=pltpu.SMEM)] * smem
            + [pl.BlockSpec(memory_space=pl.ANY) if i in whole else VMEM for i in range(smem, len(args))]
            if whole
            else [pl.BlockSpec(memory_space=pltpu.SMEM)] * smem + [VMEM] * (len(args) - smem),
            out_specs=[VMEM] * len(outs),
            scratch_shapes=list(scratch),
            input_output_aliases=alias or {},
            compiler_params=pltpu.CompilerParams(vmem_limit_bytes=limit << 20),
            cost_estimate=pl.CostEstimate(flops=1000 + cost, bytes_accessed=1000, transcendentals=0),
        )(*args)
        self.last = result[0]
        return result


def send(values, bit, count):
    return lax.ppermute(values, "dp", [(i, i ^ (1 << bit)) for i in range(count)])


def swap(values):
    return lax.ppermute(values, "mp", [(0, 1), (1, 0)])


class Scatter:
    def __init__(self, steps, count, bits, plan, pieces=2, wide=1, small=None):
        self.steps, self.count, self.bits = steps, count, bits
        self.pieces, self.wide, self.small = pieces, wide, small
        self.plan, self.arrays, self.columns = [], [], 0
        for lefts, rights in plan:
            at, each = len(self.arrays), len(lefts)
            self.arrays += lefts + rights
            places = list(range(at, at + each)), list(range(at + each, at + 2 * each))
            self.plan.append((*places, self.columns))
            self.columns += rights[0].shape[1]
        self.rows = plan[0][0][0].shape[0] // 2
        self.extra = SMALL if small is not None else 0
        self.at = 1

    def shapes(self, *sizes):
        return [((n, self.columns), HIGH) for n in sizes]

    def far(self):
        size = self.rows // self.pieces
        kernel = partial(
            far_kernel,
            plan=self.plan,
            start=self.rows,
            pieces=self.pieces,
            small=bool(self.extra),
        )
        held = self.arrays + ([self.small] if self.extra else [])
        outs = self.shapes(size + self.extra, *[size] * (self.pieces - 1))
        outs = self.steps(kernel, "far", outs, held)
        self.got = [send(o, self.bits[0], self.count) for o in outs]

    def near(self):
        kernel = partial(
            near_kernel,
            plan=self.plan,
            pieces=self.pieces,
            small=bool(self.extra),
        )
        held = self.arrays + self.got + ([self.small] if self.extra else [])
        self.rows //= 2
        outs = self.shapes(self.rows, self.rows + self.extra)
        self.keep, self.sent = self.steps(kernel, "near", outs, held)
        self.got = send(self.sent, self.bits[1], self.count)

    def step(self):
        self.at += 1
        self.rows //= 2
        outs = self.shapes(self.rows, self.rows + self.extra)
        kernel = partial(step_kernel, small=bool(self.extra), joined=False)
        self.keep, self.sent = self.steps(kernel, "sum", outs, [self.keep, self.sent, self.got])
        self.got = send(self.sent, self.bits[self.at], self.count)


def join(one, two):
    for part in (one, two):
        part.at += 1
        part.rows //= 2
    outs = one.shapes(one.rows) + two.shapes(two.rows) + one.shapes(one.rows + two.rows + one.extra)
    kernel = partial(step_kernel, small=bool(one.extra), joined=True)
    held = [one.keep, two.keep, one.sent, two.sent, one.got, two.got]
    one.keep, two.keep, sent = one.steps(kernel, "sums", outs, held)
    got = send(sent, one.bits[one.at], one.count)
    while one.at + 1 < len(one.bits):
        one.at += 1
        half = one.rows // 2
        starts = (0, one.rows + one.extra)
        keeps, sents = [], []
        for part, start in zip((one, two), starts):
            total = part.keep + got[start : start + part.rows]
            keeps.append(total[:half])
            sents.append(total[half:])
        if one.extra:
            at = slice(one.rows, one.rows + one.extra)
            sents.insert(1, sent[at] + got[at])
        one.keep, two.keep = keeps
        one.rows = two.rows = half
        sent = jnp.concatenate(sents)
        got = send(sent, one.bits[one.at], one.count)
    return sent, got


def finish(one, two, sent, got):
    outs = []
    for part in (one, two):
        outs += [((part.rows, part.columns // part.wide), HIGH)] * part.wide
    if one.extra:
        outs += [((SMALL, one.columns), HIGH), ((2, one.columns), HIGH)]
    kernel = partial(end_kernel, wide=one.wide, small=bool(one.extra))
    return one.steps(kernel, "end", outs, [one.keep, two.keep, sent, got])


def body(
    tokens,
    crop_ids,
    w_query,
    w_key,
    w_value,
    bias_query,
    bias_value,
    w_out,
    bias_out,
    gain_attn,
    shift_attn,
    gain_mlp,
    shift_mlp,
    w_up,
    bias_up,
    w_down,
    bias_down,
    cotangent,
    count,
):
    width = tokens.shape[1]
    local = w_query.shape[1]
    hidden_units = w_up.shape[1]
    seqs, length = crop_ids.shape
    rows = seqs * length
    here = lax.axis_index("dp")
    scalar = here.reshape(1)
    bits = list(range(count.bit_length() - 1))
    orders = (bits, [0, 2, 1] + bits[3:])
    steps = Steps()
    piece = local // 4
    lines = [gain_attn, shift_attn, bias_query, bias_value, bias_out, gain_mlp, shift_mlp]
    lines += [bias_down, bias_up]
    crops = BIAS_UP + hidden_units // width
    held = [((piece, width), LOW), (crop_ids.shape, jnp.int32)] + [(v.shape, HIGH) for v in lines]
    mine, table = steps(
        load_kernel,
        "load",
        [((piece, width), HIGH), ((crops + seqs, width), HIGH)],
        [scalar, w_out, crop_ids] + lines,
        scratch=[pltpu.VMEM(*h) for h in held] + [pltpu.SemaphoreType.DMA((len(held),))],
        smem=1,
        whole=range(1, 3 + len(lines)),
        limit=63,
    )
    got = swap(mine)

    def like(*arrays):
        return [(a.shape, a.dtype) for a in arrays]

    front = steps(
        partial(front_kernel, length=length, seqs=seqs, crops=crops),
        "front",
        like(tokens, w_query, w_key, w_value)
        + [((rows, width), LOW)]
        + [((rows, local), LOW)] * 3
        + [((rows, 128), HIGH)]
        + [((length, local), HIGH)] * seqs,
        [tokens, w_query, w_key, w_value, table],
        scratch=[pltpu.SemaphoreType.DMA((4,))],
        whole=range(4),
        limit=58,
    )
    tokens, w_query, w_key, w_value, first, query, key_rows, value_rows, log_total = front[:9]
    mixed = list(front[9:])
    mixed_other = [swap(o) for o in mixed]

    got, _ = lax.optimization_barrier((got, first))
    beside = send(got, 1, count)
    pieces = [got, send(got, 0, count), beside, send(beside, 0, count)]
    turned = steps(
        partial(turn_kernel, count=count, orders=orders),
        "turn",
        like(cotangent, w_up, w_down, w_out)
        + [((width, width), LOW), ((1, width), HIGH)]
        + [((width, length), LOW)] * (3 * seqs),
        [scalar, first, cotangent, w_up, w_down, w_out],
        scratch=[pltpu.SemaphoreType.DMA((4,))],
        whole=range(2, 6),
        smem=1,
        tie=1,
        limit=44,
    )

    cotangent, w_up, w_down, w_out, order_b, cot_sum = turned[:6]
    a1_a, a1_b, cot_a = (list(turned[6 + i * seqs : 6 + (i + 1) * seqs]) for i in range(3))
    hidden, a2_b, active, g_pre, carried = [], [], [], [], []
    for s in range(seqs):
        result = steps(
            partial(middle_kernel, blocks=4, seq=s, length=length),
            "middle",
            [
                ((length, width), HIGH),
                ((width, length), LOW),
                ((length, hidden_units), LOW),
                ((length, hidden_units), LOW),
                ((1, hidden_units), HIGH),
                (((s + 1) * length, width), HIGH),
                ((local, width), LOW),
            ],
            [
                scalar,
                tokens,
                mixed[s],
                mixed_other[s],
                w_out,
                table,
                w_up,
                w_down,
                cotangent,
                order_b,
            ]
            + (carried if s else pieces),
            smem=1,
            tie=2,
        )
        for held, value in zip((hidden, a2_b, active, g_pre), result):
            held.append(value)
        carried = list(result[4:])
    bias_sum, second, _ = carried
    second_other = swap(second)

    down = Scatter(steps, count, orders[0], [(cot_a, active)])
    up = Scatter(steps, count, orders[1], [(a2_b, g_pre)])
    down.far()
    up.far()
    mlp_part = steps(mlp_kernel, "mlp", [((rows, width), HIGH)], [w_down] + active, tie=1)[0]
    mlp_other = swap(mlp_part)
    down.near()
    up.near()
    g_hidden, gh, sums, *gh_b = steps(
        partial(turn_back_kernel, seqs=seqs, length=length),
        "turn_back",
        [((rows, width), HIGH), ((rows, width), LOW), ((SMALL, width), HIGH)]
        + [((width, length), LOW)] * seqs,
        [table, cotangent, second, second_other, order_b, bias_sum, cot_sum] + hidden,
        tie=2,
        cost=9 * 10**9,
    )
    down.step()
    up.step()
    sums, g_first, *result = steps(
        partial(back_kernel, seqs=seqs, length=length, crops=crops),
        "back",
        [((SMALL, width), HIGH), ((rows, width), HIGH)]
        + [((length, 2 * local), LOW)] * seqs
        + [((length, local), LOW)] * seqs,
        [tokens, table, gh, w_out, w_query, w_key, w_value, query, key_rows, value_rows]
        + [log_total, sums],
        tie=2,
    )
    g_qk, g_val = (result[i * seqs : (i + 1) * seqs] for i in range(2))
    first_other = swap(g_first)
    mlp_sent = join(down, up)
    heads = Scatter(steps, count, orders[0], [(a1_a, g_qk)], wide=2, small=sums)
    others = Scatter(steps, count, orders[1], [(a1_b, g_val), (gh_b, mixed)], wide=2)
    heads.far()
    others.far()
    heads.near()
    others.near()
    block_out = steps(
        partial(out_kernel, seqs=seqs, length=length),
        "out",
        [((rows, width), LOW)],
        [table, mlp_part, mlp_other] + hidden,
        tie=1,
    )[0]
    heads.step()
    others.step()
    w_down_t, done_w_up = finish(down, up, *mlp_sent)
    head_sent = join(heads, others)
    base, unit, scale = steps(
        partial(base_kernel, length=length),
        "base",
        [((rows, width), HIGH)] * 2 + [((rows, 1), HIGH)],
        [table, tokens, g_hidden, g_first],
        tie=2,
    )
    grad_w_q, grad_w_k, grad_w_v, w_out_t, total, gains = finish(heads, others, *head_sent)
    gain_other = swap(gains)
    packed = steps(gain_kernel, "gains", [((SMALL, width), HIGH)], [total, gain_other])[0]
    size = width // count
    own = lax.dynamic_slice(packed, (0, here * size), (9, size))
    done = [
        w_out_t.T,
        own[2],
        own[3],
        own[4],
        own[0],
        own[1],
        w_down_t.T,
        own[8],
        packed[5, :local],
        packed[5, local:],
        packed[6:8].reshape(-1),
    ]
    first_other, *done = lax.optimization_barrier((first_other, *done))
    grad_tokens = steps(
        partial(last_kernel, length=length),
        "last",
        [((rows, width), HIGH)],
        [table, base, unit, scale, first_other],
        tie=1,
    )[0]
    return (
        block_out,
        grad_tokens,
        grad_w_q,
        grad_w_k,
        grad_w_v,
        done[8],
        done[9],
        *done[:6],
        done_w_up,
        done[10],
        *done[6:8],
    )


def solution(mesh):
    placed = (
        P("dp", None),
        P("dp", None),
        P(None, "mp"),
        P(None, "mp"),
        P(None, "mp"),
        P("mp"),
        P("mp"),
        P("mp", None),
        P(),
        P(),
        P(),
        P(),
        P(),
        P(None, "mp"),
        P("mp"),
        P("mp", None),
        P(),
        P("dp", None),
    )
    return jax.shard_map(
        partial(body, count=mesh.shape["dp"]),
        mesh=mesh,
        in_specs=placed,
        out_specs=(
            P("dp", None),
            P("dp", None),
            P("dp", "mp"),
            P("dp", "mp"),
            P("dp", "mp"),
            P("mp"),
            P("mp"),
            P("mp", "dp"),
            P("dp"),
            P("dp"),
            P("dp"),
            P("dp"),
            P("dp"),
            P("dp", "mp"),
            P("mp"),
            P("mp", "dp"),
            P("dp"),
        ),
        check_vma=False,
    )
```

```python
from functools import partial

import jax
import jax.numpy as jnp
from jax import lax
from jax.experimental import pallas as pl
from jax.experimental.pallas import tpu as pltpu
from jax.sharding import PartitionSpec as P

HEAD_DIM = 64
PAIR = 2 * HEAD_DIM
EPS = 1e-06
NEGATIVE = -1e30
LOW = jnp.bfloat16
HIGH = jnp.float32
VMEM = pl.BlockSpec(memory_space=pltpu.VMEM)
SMALL = 16
GAIN_ATTN, SHIFT_ATTN, BIAS_Q, BIAS_V, BIAS_OUT, GAIN_MLP, SHIFT_MLP, BIAS_DOWN, BIAS_UP = range(9)


def plain_dot(left, right):
    return jnp.dot(left, right, preferred_element_type=HIGH)


def right_trans(left, right):
    return lax.dot_general(left, right, (((1,), (1,)), ((), ())), preferred_element_type=HIGH)


def left_trans(left, right):
    return lax.dot_general(left, right, (((0,), (0,)), ((), ())), preferred_element_type=HIGH)


def unit_rows(values):
    mean = jnp.mean(values, axis=-1, keepdims=True)
    centred = values - mean
    scale = lax.rsqrt(jnp.mean(centred * centred, axis=-1, keepdims=True) + EPS)
    return centred * scale, scale


def norm_back(grad_unit, unit, scale):
    inner = jnp.mean(grad_unit * unit, axis=-1, keepdims=True)
    return scale * (grad_unit - jnp.mean(grad_unit, axis=-1, keepdims=True) - unit * inner)


def half_masks():
    lane = lax.broadcasted_iota(jnp.int32, (1, PAIR), 1)
    first = lane < HEAD_DIM
    return first, (first.astype(HIGH).astype(LOW), (~first).astype(HIGH).astype(LOW))


def col_sum(values):
    return jnp.sum(values, axis=0, keepdims=True)


def row(table, at, size):
    return table[at : at + 1, :size]


def same_crop(table, slot, length):
    ids = row(table, slot, length)
    marks = lax.broadcasted_iota(jnp.int32, (SMALL, length), 0).astype(HIGH) == ids
    marks = marks.astype(HIGH).astype(LOW)
    return left_trans(marks, marks) > 0.5


def copies_of(sources, targets, sems):
    copies = [pltpu.make_async_copy(a, b, sems.at[i]) for i, (a, b) in enumerate(zip(sources, targets))]
    for copy in copies:
        copy.start()
    return copies


def load_kernel(here, w_out, crops, *refs):
    count = (len(refs) - 5) // 2
    vectors, (piece, table), sems = refs[:count], refs[count : count + 2], refs[-1]
    held = refs[count + 2 : -1]
    size = piece.shape[0]
    start = pl.multiple_of((here[0] & 3) * size, size)
    sources = [w_out.at[pl.ds(start, size), :], crops, *vectors]
    copies = copies_of(sources, held, sems)
    copies[0].wait()
    piece[...] = held[0][...].astype(HIGH)
    for copy in copies[1:]:
        copy.wait()
    table[...] = jnp.zeros_like(table)
    at, width = 0, table.shape[1]
    for vector in held[2:]:
        for low in range(0, vector.shape[0], width):
            part = min(width, vector.shape[0] - low)
            table[at : at + 1, :part] = vector[low : low + part].reshape(1, part)
            at += 1
    seqs, length = held[1].shape
    table[at : at + seqs, :length] = held[1][...].astype(HIGH)


def front_kernel(*refs, length, seqs, crops):
    sources, table, held = refs[:4], refs[4], refs[5:9]
    first_out, q, k, v, lse = refs[9:14]
    outs, sems = refs[14:-1], refs[-1]
    copies = copies_of(sources, held, sems)
    tokens, w_q, w_k, w_v = held
    copies[0].wait()
    unit, _ = unit_rows(tokens[...].astype(HIGH))
    local, width = w_q.shape[1], tokens.shape[1]
    first = (unit * row(table, GAIN_ATTN, width) + row(table, SHIFT_ATTN, width)).astype(LOW)
    first_out[...] = first
    for copy in copies[1:]:
        copy.wait()
    q_all = plain_dot(first, w_q[...]) + row(table, BIAS_Q, local)
    q_all = (q_all.astype(LOW) * 0.125).astype(LOW)
    k_all = plain_dot(first, w_k[...]).astype(LOW)
    v_all = (plain_dot(first, w_v[...]) + row(table, BIAS_V, local)).astype(LOW)
    q[...] = q_all
    k[...] = k_all
    v[...] = v_all
    low_half, masks = half_masks()
    for s, o in enumerate(outs):
        rows = slice(s * length, (s + 1) * length)
        same = same_crop(table, crops + s, length)
        for t in range(local // PAIR):
            at = slice(t * PAIR, (t + 1) * PAIR)
            q_pair, k_pair, v_pair = q_all[rows, at], k_all[rows, at], v_all[rows, at]
            got = []
            for half in range(2):
                scores = jnp.where(same, right_trans(q_pair * masks[half], k_pair), NEGATIVE)
                top = jnp.max(scores, axis=-1, keepdims=True)
                expo = jnp.exp(scores - top)
                total = jnp.sum(expo, axis=-1, keepdims=True)
                probs = (expo * (1.0 / total)).astype(LOW)
                got.append(plain_dot(probs, v_pair))
                h = 2 * t + half
                lse[rows, h : h + 1] = top + jnp.log(total)
            o[:, at] = jnp.where(low_half, got[0], got[1])


def relative_rows(here, width, count, bits):
    size = width // count
    place = lax.broadcasted_iota(jnp.int32, (width, 1), 0)
    block = ((place.astype(HIGH) + 0.5) * (1.0 / size)).astype(jnp.int32)
    mask = jnp.zeros_like(block)
    for p, bit in enumerate(bits):
        mask = mask + (((block >> (len(bits) - 1 - p)) & 1) << bit)
    source = (mask ^ here) * size + (place - block * size)
    marks = lax.broadcasted_iota(jnp.int32, (width, width), 1) == source
    return marks.astype(HIGH).astype(LOW)


def turn_kernel(here, first, *refs, count, orders):
    sources, held = refs[:4], refs[4:8]
    order_b, sums, sems = refs[8], refs[9], refs[-1]
    seqs = (len(refs) - 11) // 3
    a1_a, a1_b, cot_a = (refs[10 + i * seqs : 10 + (i + 1) * seqs] for i in range(3))
    length = first.shape[0] // seqs
    copies = copies_of(sources, held, sems)
    width = first.shape[1]
    order_a = relative_rows(here[0], width, count, orders[0])
    order = relative_rows(here[0], width, count, orders[1])
    order_b[...] = order
    for s in range(seqs):
        part = first[s * length : (s + 1) * length, :]
        a1_a[s][...] = right_trans(order_a, part).astype(LOW)
        a1_b[s][...] = right_trans(order, part).astype(LOW)
    for copy in copies:
        copy.wait()
    cot = held[0][...]
    for s in range(seqs):
        part = cot[s * length : (s + 1) * length, :]
        cot_a[s][...] = right_trans(order_a, part).astype(LOW)
    sums[...] = col_sum(cot.astype(HIGH))


def middle_kernel(*refs, blocks, seq, length):
    here, tokens, o_own, o_other, w_out, table, w_up, w_down, cotangent, order = refs[:10]
    hidden, a2_t, active, g_pre, g_bias, g_second, w_low = refs[-7:]
    rows = slice(seq * length, (seq + 1) * length)
    if seq:
        bias_before, second_before, w_before = refs[10:13]
        g_second[: seq * length, :] = second_before[...]
        w_low[...] = w_before[...]
    else:
        for b, piece in enumerate(refs[10:14]):
            size = piece.shape[0]
            start = pl.multiple_of(((here[0] & 3) ^ b) * size, size)
            w_low[pl.ds(start, size), :] = piece[...].astype(LOW)
    attn = plain_dot(o_own[...].astype(LOW), w_out[...])
    attn = attn + plain_dot(o_other[...].astype(LOW), w_low[...])
    width = tokens.shape[1]
    values = tokens[rows, :].astype(HIGH) + (attn + row(table, BIAS_OUT, width))
    hidden[...] = values
    unit, _ = unit_rows(values)
    second = (unit * row(table, GAIN_MLP, width) + row(table, SHIFT_MLP, width)).astype(LOW)
    cot = cotangent[rows, :]
    size = w_up.shape[1] // blocks
    total = None
    for b in range(blocks):
        at = slice(b * size, (b + 1) * size)
        low = b * size % width
        at_row = BIAS_UP + b * size // width
        bias_up = table[at_row : at_row + 1, low : low + size]
        pre = plain_dot(second, w_up[:, at]) + bias_up
        cdf = 0.5 * (1.0 + lax.erf(pre * 0.7071067811865476))
        active[:, at] = (pre * cdf).astype(LOW)
        slope = cdf + pre * (0.3989422804014327 * jnp.exp(-0.5 * (pre * pre)))
        grad = (right_trans(cot, w_down[at, :]) * slope).astype(LOW)
        g_pre[:, at] = grad
        bias = col_sum(grad.astype(HIGH))
        g_bias[:, at] = bias_before[:, at] + bias if seq else bias
        part = right_trans(grad, w_up[:, at])
        total = part if total is None else total + part
    g_second[rows, :] = total
    a2_t[...] = right_trans(order[...], second).astype(LOW)


def turn_back_kernel(*refs, seqs, length):
    table, cotangent, own, other, order, g_bias, cot_sum = refs[:7]
    hidden = refs[7 : 7 + seqs]
    g_hidden, gh, sums = refs[7 + seqs : 10 + seqs]
    gh_t = refs[10 + seqs :]
    width = cotangent.shape[1]
    totals = [0.0, 0.0, 0.0]
    for s in range(seqs):
        rows = slice(s * length, (s + 1) * length)
        unit, scale = unit_rows(hidden[s][...])
        grad = own[rows, :] + other[rows, :]
        values = norm_back(grad * row(table, GAIN_MLP, width), unit, scale)
        values = cotangent[rows, :].astype(HIGH) + values
        g_hidden[rows, :] = values
        low = values.astype(LOW)
        gh[rows, :] = low
        gh_t[s][...] = right_trans(order[...], low).astype(LOW)
        parts = (col_sum(grad * unit), col_sum(grad), col_sum(values))
        totals = [a + b for a, b in zip(totals, parts)]
    for i, total in enumerate(totals):
        sums[i : i + 1, :] = total
    sums[3:6, :] = jnp.zeros((3, width), HIGH)
    sums[6:7, :] = g_bias[:, :width]
    sums[7:8, :] = g_bias[:, width:]
    sums[8:9, :] = cot_sum[...]
    sums[9:, :] = jnp.zeros_like(sums[9:, :])


def back_kernel(*refs, seqs, length, crops):
    tokens, table, gh, w_out, w_q, w_k, w_v, q, k, v, lse, _ = refs[:12]
    sums, g_first = refs[12:14]
    g_qk, g_val = (refs[14 + i * seqs : 14 + (i + 1) * seqs] for i in range(2))
    width, local = tokens.shape[1], q.shape[1]
    low_half, masks = half_masks()
    full = slice(0, width)
    before = refs[11]
    sums[:3, :] = before[:3, :]
    sums[6:, :] = before[6:, :]

    def put(s, r, at, value):
        sums[r : r + 1, at] = sums[r : r + 1, at] + value if s else value

    for s in range(seqs):
        rows = slice(s * length, (s + 1) * length)
        g_o = right_trans(gh[rows, :], w_out[...]).astype(LOW)
        same = same_crop(table, crops + s, length)
        for t in range(local // PAIR):
            at = slice(t * PAIR, (t + 1) * PAIR)
            q_pair, k_pair, v_pair, o_pair = q[rows, at], k[rows, at], v[rows, at], g_o[:, at]
            got = []
            for half in range(2):
                h = 2 * t + half
                scores = right_trans(q_pair * masks[half], k_pair)
                probs = jnp.exp(jnp.where(same, scores, NEGATIVE) - lse[rows, h : h + 1])
                g_probs = right_trans(o_pair * masks[half], v_pair)
                inner = jnp.sum(g_probs * probs, axis=-1, keepdims=True)
                g_scores = (probs * (g_probs - inner)).astype(LOW)
                got.append(
                    (
                        plain_dot(g_scores, k_pair),
                        left_trans(g_scores, q_pair),
                        left_trans(probs.astype(LOW), o_pair),
                    )
                )
            g_q = (jnp.where(low_half, got[0][0], got[1][0]) * 0.125).astype(LOW)
            g_k = jnp.where(low_half, got[0][1], got[1][1]).astype(LOW)
            g_v = jnp.where(low_half, got[0][2], got[1][2]).astype(LOW)
            beside = slice(local + t * PAIR, local + (t + 1) * PAIR)
            g_qk[s][:, at] = g_q
            g_qk[s][:, beside] = g_k
            g_val[s][:, at] = g_v
            put(s, 5, at, col_sum(g_q.astype(HIGH)))
            put(s, 5, beside, col_sum(g_v.astype(HIGH)))
        part = right_trans(g_qk[s][:, :local], w_q[...])
        part = part + right_trans(g_qk[s][:, local:], w_k[...])
        part = part + right_trans(g_val[s][...], w_v[...])
        g_first[rows, :] = part
        unit_one, _ = unit_rows(tokens[rows, :].astype(HIGH))
        put(s, 3, full, col_sum(part * unit_one))
        put(s, 4, full, col_sum(part))


def base_kernel(table, tokens, g_hidden, own, base, unit_out, scale_out, *, length):
    gain = row(table, GAIN_ATTN, tokens.shape[1])
    for s in range(tokens.shape[0] // length):
        rows = slice(s * length, (s + 1) * length)
        part = own[rows, :]
        unit, scale = unit_rows(tokens[rows, :].astype(HIGH))
        base[rows, :] = g_hidden[rows, :] + norm_back(part * gain, unit, scale)
        unit_out[rows, :] = unit
        scale_out[rows, :] = scale


def last_kernel(table, base, unit, scale, other, g_tokens, *, length):
    gain = row(table, GAIN_ATTN, base.shape[1])
    for s in range(base.shape[0] // length):
        rows = slice(s * length, (s + 1) * length)
        grad = norm_back(other[rows, :] * gain, unit[rows, :], scale[rows, :])
        g_tokens[rows, :] = base[rows, :] + grad


def out_kernel(*refs, seqs, length):
    table, own, other = refs[:3]
    for s in range(seqs):
        rows = slice(s * length, (s + 1) * length)
        total = refs[3 + s][...] + (own[rows, :] + other[rows, :])
        refs[3 + seqs][rows, :] = (total + row(table, BIAS_DOWN, total.shape[1])).astype(LOW)


def mlp_kernel(w_down, *refs):
    length = refs[0].shape[0]
    for s, active in enumerate(refs[:-1]):
        refs[-1][s * length : (s + 1) * length, :] = plain_dot(active[...], w_down[...])


def products(plan, refs, at):
    for lefts, rights, column in plan:
        wide = refs[rights[0]].shape[1]
        step = min(512, wide)
        for n in range(0, wide, step):
            value = None
            for left, right in zip(lefts, rights):
                part = plain_dot(refs[left][at, :], refs[right][:, n : n + step].astype(LOW))
                value = part if value is None else value + part
            yield slice(column + n, column + n + step), value


def far_kernel(*refs, plan, start, pieces, small):
    outs = refs[-pieces:]
    size = start // pieces
    for o, out in enumerate(outs):
        at = slice(start + o * size, start + (o + 1) * size)
        for columns, value in products(plan, refs, at):
            out[:size, columns] = value
    if small:
        outs[0][size:, :] = refs[-pieces - 1][...]


def near_kernel(*refs, plan, pieces, small):
    outs, got = refs[-2:], refs[-2 - pieces - small :]
    half = outs[0].shape[0]
    for o, out in enumerate(outs):
        at = slice(o * half, (o + 1) * half)
        size = 2 * half // pieces
        low = o * half % size
        for columns, value in products(plan, refs, at):
            out[:half, columns] = value + got[o * half // size][low : low + half, columns]
    if small:
        outs[1][half:, :] = got[pieces][...] + got[0][2 * half // pieces :, :]


def step_kernel(*refs, small, joined):
    count = 2 if joined else 1
    keeps, sents, gots = (refs[i * count : (i + 1) * count] for i in range(3))
    outs = refs[3 * count :]
    at = 0
    for i in range(count):
        half = outs[i].shape[0]
        got = gots[i]
        outs[i][...] = keeps[i][:half, :] + got[:half, :]
        outs[count][at : at + half, :] = keeps[i][half:, :] + got[half : 2 * half, :]
        at += half
        if small and not i:
            outs[count][at : at + SMALL, :] = sents[i][2 * half :, :] + got[2 * half :, :]
            at += SMALL


def end_kernel(*refs, wide):
    keeps, got, outs = refs[:2], refs[2], refs[3:]
    at = o = 0
    for keep in keeps:
        size, each = keep.shape[0], keep.shape[1] // wide
        for w in range(wide):
            columns = slice(w * each, (w + 1) * each)
            outs[o][...] = keep[:, columns] + got[at : at + size, columns]
            o += 1
        at += size


def final_kernel(here, one, two, sent, got, *outs):
    size = one.shape[0]
    each = one.shape[1] // 2
    for o, (keep, at) in enumerate(((one, 0), (two, size + SMALL))):
        for w in range(2):
            columns = slice(w * each, (w + 1) * each)
            outs[2 * o + w][...] = keep[:, columns] + got[at : at + size, columns]
    total = sent[size : size + SMALL, :] + got[size : size + SMALL, :]
    bias_q, bias_v, bias_up, gain_mlp, shift_mlp, bias_out, bias_down, gains = outs[4:]
    width = total.shape[1]
    bias_q[...] = total[5, :each]
    bias_v[...] = total[5, each:]
    for i in range(bias_up.shape[0] // width):
        bias_up[i * width : (i + 1) * width] = total[6 + i, :]
    turned = pltpu.roll(total, lax.rem(width - here[0] * size, width), 1)
    for out, at in ((gain_mlp, 0), (shift_mlp, 1), (bias_out, 2), (bias_down, 8)):
        out[...] = turned[at, :size]
    gains[...] = turned[:8, : gains.shape[1]]


def gain_kernel(own, other, gain, shift):
    total = own[...] + other[...]
    gain[...] = total[3, : gain.shape[0]]
    shift[...] = total[4, : shift.shape[0]]


class Steps:
    def __init__(self):
        self.last = None

    def __call__(
        self, kernel, name, outs, args, scratch=(), limit=12, smem=0, whole=0, tie=0, alias=None, cost=0
    ):
        args = list(args)
        if self.last is not None:
            args[tie], _ = lax.optimization_barrier((args[tie], self.last))
        result = pl.pallas_call(
            kernel,
            name=name,
            out_shape=[jax.ShapeDtypeStruct(s, d) for s, d in outs],
            in_specs=[pl.BlockSpec(memory_space=pltpu.SMEM)] * smem
            + [pl.BlockSpec(memory_space=pl.ANY) if i in whole else VMEM for i in range(smem, len(args))]
            if whole
            else [pl.BlockSpec(memory_space=pltpu.SMEM)] * smem + [VMEM] * (len(args) - smem),
            out_specs=[VMEM] * len(outs),
            scratch_shapes=list(scratch),
            input_output_aliases=alias or {},
            compiler_params=pltpu.CompilerParams(vmem_limit_bytes=limit << 20),
            cost_estimate=pl.CostEstimate(flops=1000 + cost, bytes_accessed=1000, transcendentals=0),
        )(*args)
        self.last = result[0]
        return result


def send(values, bit, count):
    return lax.ppermute(values, "dp", [(i, i ^ (1 << bit)) for i in range(count)])


def swap(values):
    return lax.ppermute(values, "mp", [(0, 1), (1, 0)])


class Scatter:
    def __init__(self, steps, count, bits, plan, pieces=2, wide=1, small=None):
        self.steps, self.count, self.bits = steps, count, bits
        self.pieces, self.wide, self.small = pieces, wide, small
        self.plan, self.arrays, self.columns = [], [], 0
        for lefts, rights in plan:
            at, each = len(self.arrays), len(lefts)
            self.arrays += lefts + rights
            places = list(range(at, at + each)), list(range(at + each, at + 2 * each))
            self.plan.append((*places, self.columns))
            self.columns += rights[0].shape[1]
        self.rows = plan[0][0][0].shape[0] // 2
        self.extra = SMALL if small is not None else 0
        self.at = 1

    def shapes(self, *sizes):
        return [((n, self.columns), HIGH) for n in sizes]

    def far(self):
        size = self.rows // self.pieces
        kernel = partial(
            far_kernel,
            plan=self.plan,
            start=self.rows,
            pieces=self.pieces,
            small=bool(self.extra),
        )
        held = self.arrays + ([self.small] if self.extra else [])
        outs = self.shapes(size + self.extra, *[size] * (self.pieces - 1))
        outs = self.steps(kernel, "far", outs, held)
        self.got = [send(o, self.bits[0], self.count) for o in outs]

    def near(self):
        kernel = partial(
            near_kernel,
            plan=self.plan,
            pieces=self.pieces,
            small=bool(self.extra),
        )
        held = self.arrays + self.got + ([self.small] if self.extra else [])
        self.rows //= 2
        outs = self.shapes(self.rows, self.rows + self.extra)
        self.keep, self.sent = self.steps(kernel, "near", outs, held)
        self.got = send(self.sent, self.bits[1], self.count)

    def step(self):
        self.at += 1
        self.rows //= 2
        outs = self.shapes(self.rows, self.rows + self.extra)
        kernel = partial(step_kernel, small=bool(self.extra), joined=False)
        self.keep, self.sent = self.steps(kernel, "sum", outs, [self.keep, self.sent, self.got])
        self.got = send(self.sent, self.bits[self.at], self.count)


def join(one, two):
    for part in (one, two):
        part.at += 1
        part.rows //= 2
    outs = one.shapes(one.rows) + two.shapes(two.rows) + one.shapes(one.rows + two.rows + one.extra)
    kernel = partial(step_kernel, small=bool(one.extra), joined=True)
    held = [one.keep, two.keep, one.sent, two.sent, one.got, two.got]
    one.keep, two.keep, sent = one.steps(kernel, "sums", outs, held)
    got = send(sent, one.bits[one.at], one.count)
    while one.at + 1 < len(one.bits):
        one.at += 1
        half = one.rows // 2
        starts = (0, one.rows + one.extra)
        keeps, sents = [], []
        for part, start in zip((one, two), starts):
            total = part.keep + got[start : start + part.rows]
            keeps.append(total[:half])
            sents.append(total[half:])
        if one.extra:
            at = slice(one.rows, one.rows + one.extra)
            sents.insert(1, sent[at] + got[at])
        one.keep, two.keep = keeps
        one.rows = two.rows = half
        sent = jnp.concatenate(sents)
        got = send(sent, one.bits[one.at], one.count)
    return sent, got


def finish(one, two, got, cost=0):
    outs = []
    for part in (one, two):
        outs += [((part.rows, part.columns // part.wide), HIGH)] * part.wide
    kernel = partial(end_kernel, wide=one.wide)
    return one.steps(kernel, "end", outs, [one.keep, two.keep, got], cost=cost)


def body(
    tokens,
    crop_ids,
    w_query,
    w_key,
    w_value,
    bias_query,
    bias_value,
    w_out,
    bias_out,
    gain_attn,
    shift_attn,
    gain_mlp,
    shift_mlp,
    w_up,
    bias_up,
    w_down,
    bias_down,
    cotangent,
    count,
):
    width = tokens.shape[1]
    local = w_query.shape[1]
    hidden_units = w_up.shape[1]
    seqs, length = crop_ids.shape
    rows = seqs * length
    here = lax.axis_index("dp")
    scalar = here.reshape(1)
    bits = list(range(count.bit_length() - 1))
    orders = (bits, [0, 2, 1] + bits[3:])
    steps = Steps()
    piece = local // 4
    lines = [gain_attn, shift_attn, bias_query, bias_value, bias_out, gain_mlp, shift_mlp]
    lines += [bias_down, bias_up]
    crops = BIAS_UP + hidden_units // width
    held = [((piece, width), LOW), (crop_ids.shape, jnp.int32)] + [(v.shape, HIGH) for v in lines]
    mine, table = steps(
        load_kernel,
        "load",
        [((piece, width), HIGH), ((crops + seqs, width), HIGH)],
        [scalar, w_out, crop_ids] + lines,
        scratch=[pltpu.VMEM(*h) for h in held] + [pltpu.SemaphoreType.DMA((len(held),))],
        smem=1,
        whole=range(1, 3 + len(lines)),
        limit=63,
    )
    got = swap(mine)

    def like(*arrays):
        return [(a.shape, a.dtype) for a in arrays]

    front = steps(
        partial(front_kernel, length=length, seqs=seqs, crops=crops),
        "front",
        like(tokens, w_query, w_key, w_value)
        + [((rows, width), LOW)]
        + [((rows, local), LOW)] * 3
        + [((rows, 128), HIGH)]
        + [((length, local), HIGH)] * seqs,
        [tokens, w_query, w_key, w_value, table],
        scratch=[pltpu.SemaphoreType.DMA((4,))],
        whole=range(4),
        limit=58,
    )
    tokens, w_query, w_key, w_value, first, query, key_rows, value_rows, log_total = front[:9]
    mixed = list(front[9:])
    mixed_other = [swap(o) for o in mixed]

    got, _ = lax.optimization_barrier((got, first))
    beside = send(got, 1, count)
    pieces = [got, send(got, 0, count), beside, send(beside, 0, count)]
    turned = steps(
        partial(turn_kernel, count=count, orders=orders),
        "turn",
        like(cotangent, w_up, w_down, w_out)
        + [((width, width), LOW), ((1, width), HIGH)]
        + [((width, length), LOW)] * (3 * seqs),
        [scalar, first, cotangent, w_up, w_down, w_out],
        scratch=[pltpu.SemaphoreType.DMA((4,))],
        whole=range(2, 6),
        smem=1,
        tie=1,
        limit=44,
    )

    cotangent, w_up, w_down, w_out, order_b, cot_sum = turned[:6]
    a1_a, a1_b, cot_a = (list(turned[6 + i * seqs : 6 + (i + 1) * seqs]) for i in range(3))
    hidden, a2_b, active, g_pre, carried = [], [], [], [], []
    for s in range(seqs):
        result = steps(
            partial(middle_kernel, blocks=4, seq=s, length=length),
            "middle",
            [
                ((length, width), HIGH),
                ((width, length), LOW),
                ((length, hidden_units), LOW),
                ((length, hidden_units), LOW),
                ((1, hidden_units), HIGH),
                (((s + 1) * length, width), HIGH),
                ((local, width), LOW),
            ],
            [
                scalar,
                tokens,
                mixed[s],
                mixed_other[s],
                w_out,
                table,
                w_up,
                w_down,
                cotangent,
                order_b,
            ]
            + (carried if s else pieces),
            smem=1,
            tie=2,
        )
        for held, value in zip((hidden, a2_b, active, g_pre), result):
            held.append(value)
        carried = list(result[4:])
    bias_sum, second, _ = carried
    second_other = swap(second)

    down = Scatter(steps, count, orders[0], [(cot_a, active)])
    up = Scatter(steps, count, orders[1], [(a2_b, g_pre)])
    down.far()
    up.far()
    mlp_part = steps(mlp_kernel, "mlp", [((rows, width), HIGH)], [w_down] + active, tie=1)[0]
    mlp_other = swap(mlp_part)
    down.near()
    up.near()
    g_hidden, gh, sums, *gh_b = steps(
        partial(turn_back_kernel, seqs=seqs, length=length),
        "turn_back",
        [((rows, width), HIGH), ((rows, width), LOW), ((SMALL, width), HIGH)]
        + [((width, length), LOW)] * seqs,
        [table, cotangent, second, second_other, order_b, bias_sum, cot_sum] + hidden,
        tie=2,
        cost=9 * 10**9,
    )
    down.step()
    up.step()
    sums, g_first, *result = steps(
        partial(back_kernel, seqs=seqs, length=length, crops=crops),
        "back",
        [((SMALL, width), HIGH), ((rows, width), HIGH)]
        + [((length, 2 * local), LOW)] * seqs
        + [((length, local), LOW)] * seqs,
        [tokens, table, gh, w_out, w_query, w_key, w_value, query, key_rows, value_rows]
        + [log_total, sums],
        tie=2,
    )
    g_qk, g_val = (result[i * seqs : (i + 1) * seqs] for i in range(2))
    first_other = swap(g_first)
    heads = Scatter(steps, count, orders[0], [(a1_a, g_qk)], wide=2, small=sums)
    others = Scatter(steps, count, orders[1], [(a1_b, g_val), (gh_b, mixed)], wide=2)
    heads.far()
    others.far()
    _, mlp_got = join(down, up)
    heads.near()
    others.near()
    block_out = steps(
        partial(out_kernel, seqs=seqs, length=length),
        "out",
        [((rows, width), LOW)],
        [table, mlp_part, mlp_other] + hidden,
        tie=1,
    )[0]
    w_down_t, done_w_up = finish(down, up, mlp_got, cost=15 * 10**8)
    heads.step()
    others.step()
    sent, got = join(heads, others)
    base, unit, scale = steps(
        partial(base_kernel, length=length),
        "base",
        [((rows, width), HIGH)] * 2 + [((rows, 1), HIGH)],
        [table, tokens, g_hidden, g_first],
        tie=2,
    )
    grad_tokens = steps(
        partial(last_kernel, length=length),
        "last",
        [((rows, width), HIGH)],
        [table, base, unit, scale, first_other],
        tie=1,
    )[0]
    size = width // count
    (
        grad_w_q,
        grad_w_k,
        grad_w_v,
        w_out_t,
        done_bias_q,
        done_bias_v,
        done_bias_up,
        done_gain_mlp,
        done_shift_mlp,
        done_bias_out,
        done_bias_down,
        gains,
    ) = steps(
        final_kernel,
        "final",
        [((size, local), HIGH)] * 4
        + [((local,), HIGH)] * 2
        + [((hidden_units,), HIGH)]
        + [((size,), HIGH)] * 4
        + [((8, 128), HIGH)],
        [scalar, heads.keep, others.keep, sent, got],
        smem=1,
        tie=1,
    )
    done_gain_attn, done_shift_attn = steps(
        gain_kernel, "gains", [((size,), HIGH)] * 2, [gains, swap(gains)]
    )
    return (
        block_out,
        grad_tokens,
        grad_w_q,
        grad_w_k,
        grad_w_v,
        done_bias_q,
        done_bias_v,
        w_out_t.T,
        done_bias_out,
        done_gain_attn,
        done_shift_attn,
        done_gain_mlp,
        done_shift_mlp,
        done_w_up,
        done_bias_up,
        w_down_t.T,
        done_bias_down,
    )


def solution(mesh):
    placed = (
        P("dp", None),
        P("dp", None),
        P(None, "mp"),
        P(None, "mp"),
        P(None, "mp"),
        P("mp"),
        P("mp"),
        P("mp", None),
        P(),
        P(),
        P(),
        P(),
        P(),
        P(None, "mp"),
        P("mp"),
        P("mp", None),
        P(),
        P("dp", None),
    )
    return jax.shard_map(
        partial(body, count=mesh.shape["dp"]),
        mesh=mesh,
        in_specs=placed,
        out_specs=(
            P("dp", None),
            P("dp", None),
            P("dp", "mp"),
            P("dp", "mp"),
            P("dp", "mp"),
            P("mp"),
            P("mp"),
            P("mp", "dp"),
            P("dp"),
            P("dp"),
            P("dp"),
            P("dp"),
            P("dp"),
            P("dp", "mp"),
            P("mp"),
            P("mp", "dp"),
            P("dp"),
        ),
        check_vma=False,
    )
```

```python
from functools import partial

import jax
import jax.numpy as jnp
from jax import lax
from jax.experimental import pallas as pl
from jax.experimental.pallas import tpu as pltpu
from jax.sharding import PartitionSpec as P

HEAD_DIM = 64
PAIR = 2 * HEAD_DIM
EPS = 1e-06
NEGATIVE = -1e30
LOW = jnp.bfloat16
HIGH = jnp.float32
VMEM = pl.BlockSpec(memory_space=pltpu.VMEM)
SMALL = 16
GAIN_ATTN, SHIFT_ATTN, BIAS_Q, BIAS_V, BIAS_OUT, GAIN_MLP, SHIFT_MLP, BIAS_DOWN, BIAS_UP = range(9)


def plain_dot(left, right):
    return jnp.dot(left, right, preferred_element_type=HIGH)


def right_trans(left, right):
    return lax.dot_general(left, right, (((1,), (1,)), ((), ())), preferred_element_type=HIGH)


def left_trans(left, right):
    return lax.dot_general(left, right, (((0,), (0,)), ((), ())), preferred_element_type=HIGH)


def unit_rows(values):
    mean = jnp.mean(values, axis=-1, keepdims=True)
    centred = values - mean
    scale = lax.rsqrt(jnp.mean(centred * centred, axis=-1, keepdims=True) + EPS)
    return centred * scale, scale


def norm_back(grad_unit, unit, scale):
    inner = jnp.mean(grad_unit * unit, axis=-1, keepdims=True)
    return scale * (grad_unit - jnp.mean(grad_unit, axis=-1, keepdims=True) - unit * inner)


def half_masks():
    lane = lax.broadcasted_iota(jnp.int32, (1, PAIR), 1)
    first = lane < HEAD_DIM
    return first, (first.astype(HIGH).astype(LOW), (~first).astype(HIGH).astype(LOW))


def col_sum(values):
    return jnp.sum(values, axis=0, keepdims=True)


def row(table, at, size):
    return table[at : at + 1, :size]


def same_crop(table, slot, length):
    ids = row(table, slot, length)
    marks = lax.broadcasted_iota(jnp.int32, (SMALL, length), 0).astype(HIGH) == ids
    marks = marks.astype(HIGH).astype(LOW)
    return left_trans(marks, marks) > 0.5


def copies_of(sources, targets, sems):
    copies = [pltpu.make_async_copy(a, b, sems.at[i]) for i, (a, b) in enumerate(zip(sources, targets))]
    for copy in copies:
        copy.start()
    return copies


def load_kernel(here, w_out, crops, *refs):
    count = (len(refs) - 5) // 2
    vectors, (piece, table), sems = refs[:count], refs[count : count + 2], refs[-1]
    held = refs[count + 2 : -1]
    size = piece.shape[0]
    start = pl.multiple_of((here[0] & 3) * size, size)
    sources = [w_out.at[pl.ds(start, size), :], crops, *vectors]
    copies = copies_of(sources, held, sems)
    copies[0].wait()
    piece[...] = held[0][...].astype(HIGH)
    for copy in copies[1:]:
        copy.wait()
    table[...] = jnp.zeros_like(table)
    at, width = 0, table.shape[1]
    for vector in held[2:]:
        for low in range(0, vector.shape[0], width):
            part = min(width, vector.shape[0] - low)
            table[at : at + 1, :part] = vector[low : low + part].reshape(1, part)
            at += 1
    seqs, length = held[1].shape
    table[at : at + seqs, :length] = held[1][...].astype(HIGH)


def front_kernel(*refs, length, seqs, crops):
    sources, table, held = refs[:4], refs[4], refs[5:9]
    first_out, q, k, v, lse = refs[9:14]
    outs, sems = refs[14:-1], refs[-1]
    copies = copies_of(sources, held, sems)
    tokens, w_q, w_k, w_v = held
    copies[0].wait()
    unit, _ = unit_rows(tokens[...].astype(HIGH))
    local, width = w_q.shape[1], tokens.shape[1]
    first = (unit * row(table, GAIN_ATTN, width) + row(table, SHIFT_ATTN, width)).astype(LOW)
    first_out[...] = first
    for copy in copies[1:]:
        copy.wait()
    q_all = plain_dot(first, w_q[...]) + row(table, BIAS_Q, local)
    q_all = (q_all.astype(LOW) * 0.125).astype(LOW)
    k_all = plain_dot(first, w_k[...]).astype(LOW)
    v_all = (plain_dot(first, w_v[...]) + row(table, BIAS_V, local)).astype(LOW)
    q[...] = q_all
    k[...] = k_all
    v[...] = v_all
    low_half, masks = half_masks()
    for s, o in enumerate(outs):
        rows = slice(s * length, (s + 1) * length)
        same = same_crop(table, crops + s, length)
        for t in range(local // PAIR):
            at = slice(t * PAIR, (t + 1) * PAIR)
            q_pair, k_pair, v_pair = q_all[rows, at], k_all[rows, at], v_all[rows, at]
            got = []
            for half in range(2):
                scores = jnp.where(same, right_trans(q_pair * masks[half], k_pair), NEGATIVE)
                top = jnp.max(scores, axis=-1, keepdims=True)
                expo = jnp.exp(scores - top)
                total = jnp.sum(expo, axis=-1, keepdims=True)
                probs = (expo * (1.0 / total)).astype(LOW)
                got.append(plain_dot(probs, v_pair))
                h = 2 * t + half
                lse[rows, h : h + 1] = top + jnp.log(total)
            o[:, at] = jnp.where(low_half, got[0], got[1])


def relative_rows(here, width, count, bits):
    size = width // count
    place = lax.broadcasted_iota(jnp.int32, (width, 1), 0)
    block = ((place.astype(HIGH) + 0.5) * (1.0 / size)).astype(jnp.int32)
    mask = jnp.zeros_like(block)
    for p, bit in enumerate(bits):
        mask = mask + (((block >> (len(bits) - 1 - p)) & 1) << bit)
    source = (mask ^ here) * size + (place - block * size)
    marks = lax.broadcasted_iota(jnp.int32, (width, width), 1) == source
    return marks.astype(HIGH).astype(LOW)


def turn_kernel(here, first, *refs, count, orders):
    sources, held = refs[:4], refs[4:8]
    order_b, sums, sems = refs[8], refs[9], refs[-1]
    seqs = (len(refs) - 11) // 3
    a1_a, a1_b, cot_a = (refs[10 + i * seqs : 10 + (i + 1) * seqs] for i in range(3))
    length = first.shape[0] // seqs
    copies = copies_of(sources, held, sems)
    width = first.shape[1]
    order_a = relative_rows(here[0], width, count, orders[0])
    order = relative_rows(here[0], width, count, orders[1])
    order_b[...] = order
    for s in range(seqs):
        part = first[s * length : (s + 1) * length, :]
        a1_a[s][...] = right_trans(order_a, part).astype(LOW)
        a1_b[s][...] = right_trans(order, part).astype(LOW)
    for copy in copies:
        copy.wait()
    cot = held[0][...]
    for s in range(seqs):
        part = cot[s * length : (s + 1) * length, :]
        cot_a[s][...] = right_trans(order_a, part).astype(LOW)
    sums[...] = col_sum(cot.astype(HIGH))


def middle_kernel(*refs, blocks, seq, length):
    here, tokens, o_own, o_other, w_out, table, w_up, w_down, cotangent, order = refs[:10]
    hidden, a2_t, active, g_pre, g_second, g_bias, w_low = refs[-7:]
    rows = slice(seq * length, (seq + 1) * length)
    if seq:
        bias_before, w_before = refs[10:12]
        w_low[...] = w_before[...]
    else:
        for b, piece in enumerate(refs[10:14]):
            size = piece.shape[0]
            start = pl.multiple_of(((here[0] & 3) ^ b) * size, size)
            w_low[pl.ds(start, size), :] = piece[...].astype(LOW)
    attn = plain_dot(o_own[...].astype(LOW), w_out[...])
    attn = attn + plain_dot(o_other[...].astype(LOW), w_low[...])
    width = tokens.shape[1]
    values = tokens[rows, :].astype(HIGH) + (attn + row(table, BIAS_OUT, width))
    hidden[...] = values
    unit, _ = unit_rows(values)
    second = (unit * row(table, GAIN_MLP, width) + row(table, SHIFT_MLP, width)).astype(LOW)
    cot = cotangent[rows, :]
    size = w_up.shape[1] // blocks
    total = None
    for b in range(blocks):
        at = slice(b * size, (b + 1) * size)
        low = b * size % width
        at_row = BIAS_UP + b * size // width
        bias_up = table[at_row : at_row + 1, low : low + size]
        pre = plain_dot(second, w_up[:, at]) + bias_up
        cdf = 0.5 * (1.0 + lax.erf(pre * 0.7071067811865476))
        active[:, at] = (pre * cdf).astype(LOW)
        slope = cdf + pre * (0.3989422804014327 * jnp.exp(-0.5 * (pre * pre)))
        grad = (right_trans(cot, w_down[at, :]) * slope).astype(LOW)
        g_pre[:, at] = grad
        bias = col_sum(grad.astype(HIGH))
        g_bias[:, at] = bias_before[:, at] + bias if seq else bias
        part = right_trans(grad, w_up[:, at])
        total = part if total is None else total + part
    g_second[...] = total
    a2_t[...] = right_trans(order[...], second).astype(LOW)


def back_kernel(*refs, seq, length, crops):
    tokens, table, cotangent, hidden, own, other, order = refs[:7]
    w_out, w_q, w_k, w_v, q, k, v, lse = refs[7:15]
    before = refs[15:17]
    g_hidden, gh_t, g_qk, g_val, sums, g_first = refs[17:]
    width, local = tokens.shape[1], q.shape[1]
    rows = slice(seq * length, (seq + 1) * length)
    full = slice(0, width)
    if seq:
        sums_before, first_before = before
        g_first[: seq * length, :] = first_before[...]
        sums[6:, :] = sums_before[6:, :]
    else:
        g_bias, cot_sum = before
        sums[6:7, :] = g_bias[:, :width]
        sums[7:8, :] = g_bias[:, width:]
        sums[8:9, :] = cot_sum[...]
        sums[9:, :] = jnp.zeros_like(sums[9:, :])

    def put(r, at, value):
        sums[r : r + 1, at] = sums_before[r : r + 1, at] + value if seq else value

    unit, scale = unit_rows(hidden[...])
    grad = own[...] + other[...]
    put(0, full, col_sum(grad * unit))
    put(1, full, col_sum(grad))
    values = norm_back(grad * row(table, GAIN_MLP, width), unit, scale)
    values = cotangent[rows, :].astype(HIGH) + values
    g_hidden[...] = values
    put(2, full, col_sum(values))
    low = values.astype(LOW)
    gh_t[...] = right_trans(order[...], low).astype(LOW)
    g_o = right_trans(low, w_out[...]).astype(LOW)
    same = same_crop(table, crops + seq, length)
    low_half, masks = half_masks()
    for t in range(local // PAIR):
        at = slice(t * PAIR, (t + 1) * PAIR)
        q_pair, k_pair, v_pair, o_pair = q[rows, at], k[rows, at], v[rows, at], g_o[:, at]
        got = []
        for half in range(2):
            h = 2 * t + half
            scores = right_trans(q_pair * masks[half], k_pair)
            probs = jnp.exp(jnp.where(same, scores, NEGATIVE) - lse[rows, h : h + 1])
            g_probs = right_trans(o_pair * masks[half], v_pair)
            inner = jnp.sum(g_probs * probs, axis=-1, keepdims=True)
            g_scores = (probs * (g_probs - inner)).astype(LOW)
            got.append(
                (
                    plain_dot(g_scores, k_pair),
                    left_trans(g_scores, q_pair),
                    left_trans(probs.astype(LOW), o_pair),
                )
            )
        g_q = (jnp.where(low_half, got[0][0], got[1][0]) * 0.125).astype(LOW)
        g_k = jnp.where(low_half, got[0][1], got[1][1]).astype(LOW)
        g_v = jnp.where(low_half, got[0][2], got[1][2]).astype(LOW)
        beside = slice(local + t * PAIR, local + (t + 1) * PAIR)
        g_qk[:, at] = g_q
        g_qk[:, beside] = g_k
        g_val[:, at] = g_v
        put(5, at, col_sum(g_q.astype(HIGH)))
        put(5, beside, col_sum(g_v.astype(HIGH)))
    part = right_trans(g_qk[:, :local], w_q[...])
    part = part + right_trans(g_qk[:, local:], w_k[...])
    part = part + right_trans(g_val[...], w_v[...])
    g_first[rows, :] = part
    unit_one, _ = unit_rows(tokens[rows, :].astype(HIGH))
    put(3, full, col_sum(part * unit_one))
    put(4, full, col_sum(part))


def base_kernel(table, tokens, own, *refs, length):
    g_hidden, (base, unit_out, scale_out) = refs[:-3], refs[-3:]
    gain = row(table, GAIN_ATTN, tokens.shape[1])
    for s in range(tokens.shape[0] // length):
        rows = slice(s * length, (s + 1) * length)
        part = own[rows, :]
        unit, scale = unit_rows(tokens[rows, :].astype(HIGH))
        base[rows, :] = g_hidden[s][...] + norm_back(part * gain, unit, scale)
        unit_out[rows, :] = unit
        scale_out[rows, :] = scale


def last_kernel(table, base, unit, scale, other, g_tokens, *, length):
    gain = row(table, GAIN_ATTN, base.shape[1])
    for s in range(base.shape[0] // length):
        rows = slice(s * length, (s + 1) * length)
        grad = norm_back(other[rows, :] * gain, unit[rows, :], scale[rows, :])
        g_tokens[rows, :] = base[rows, :] + grad


def out_kernel(*refs, seqs, length):
    table, own, other = refs[:3]
    for s in range(seqs):
        rows = slice(s * length, (s + 1) * length)
        total = refs[3 + s][...] + (own[rows, :] + other[rows, :])
        refs[3 + seqs][rows, :] = (total + row(table, BIAS_DOWN, total.shape[1])).astype(LOW)


def mlp_kernel(w_down, *refs):
    length = refs[0].shape[0]
    for s, active in enumerate(refs[:-1]):
        refs[-1][s * length : (s + 1) * length, :] = plain_dot(active[...], w_down[...])


def products(plan, refs, at):
    for lefts, rights, column in plan:
        wide = refs[rights[0]].shape[1]
        step = min(512, wide)
        for n in range(0, wide, step):
            value = None
            for left, right in zip(lefts, rights):
                part = plain_dot(refs[left][at, :], refs[right][:, n : n + step].astype(LOW))
                value = part if value is None else value + part
            yield slice(column + n, column + n + step), value


def far_kernel(*refs, plan, start, pieces, small):
    outs = refs[-pieces:]
    size = start // pieces
    for o, out in enumerate(outs):
        at = slice(start + o * size, start + (o + 1) * size)
        for columns, value in products(plan, refs, at):
            out[:size, columns] = value
    if small:
        outs[0][size:, :] = refs[-pieces - 1][...]


def near_kernel(*refs, plan, pieces, small):
    outs, got = refs[-2:], refs[-2 - pieces - small :]
    half = outs[0].shape[0]
    for o, out in enumerate(outs):
        at = slice(o * half, (o + 1) * half)
        size = 2 * half // pieces
        low = o * half % size
        for columns, value in products(plan, refs, at):
            out[:half, columns] = value + got[o * half // size][low : low + half, columns]
    if small:
        outs[1][half:, :] = got[pieces][...] + got[0][2 * half // pieces :, :]


def step_kernel(*refs, small, joined):
    count = 2 if joined else 1
    keeps, sents, gots = (refs[i * count : (i + 1) * count] for i in range(3))
    outs = refs[3 * count :]
    at = 0
    for i in range(count):
        half = outs[i].shape[0]
        got = gots[i]
        outs[i][...] = keeps[i][:half, :] + got[:half, :]
        outs[count][at : at + half, :] = keeps[i][half:, :] + got[half : 2 * half, :]
        at += half
        if small and not i:
            outs[count][at : at + SMALL, :] = sents[i][2 * half :, :] + got[2 * half :, :]
            at += SMALL


def end_kernel(*refs, wide):
    count = (len(refs) - 1) // (1 + wide)
    keeps, got, outs = refs[:count], refs[count], refs[count + 1 :]
    at = o = 0
    for keep in keeps:
        size, each = keep.shape[0], keep.shape[1] // wide
        for w in range(wide):
            columns = slice(w * each, (w + 1) * each)
            outs[o][...] = keep[:, columns] + got[at : at + size, columns]
            o += 1
        at += size


def final_kernel(here, keep, sent, got, *outs):
    size = keep.shape[0]
    each = keep.shape[1] // 2
    for w in range(2):
        columns = slice(w * each, (w + 1) * each)
        outs[w][...] = keep[:, columns] + got[:size, columns]
    total = sent[size : size + SMALL, :] + got[size : size + SMALL, :]
    bias_q, bias_v, bias_up, gain_mlp, shift_mlp, bias_out, bias_down, gains = outs[2:]
    width = total.shape[1]
    bias_q[...] = total[5, :each]
    bias_v[...] = total[5, each:]
    for i in range(bias_up.shape[0] // width):
        bias_up[i * width : (i + 1) * width] = total[6 + i, :]
    turned = pltpu.roll(total, lax.rem(width - here[0] * size, width), 1)
    for out, at in ((gain_mlp, 0), (shift_mlp, 1), (bias_out, 2), (bias_down, 8)):
        out[...] = turned[at, :size]
    gains[...] = turned[:8, : gains.shape[1]]


def gain_kernel(own, other, gain, shift):
    total = own[...] + other[...]
    gain[...] = total[3, : gain.shape[0]]
    shift[...] = total[4, : shift.shape[0]]


class Steps:
    def __init__(self):
        self.last = None

    def __call__(
        self, kernel, name, outs, args, scratch=(), limit=12, smem=0, whole=0, tie=0, alias=None, cost=0
    ):
        args = list(args)
        if self.last is not None:
            args[tie], _ = lax.optimization_barrier((args[tie], self.last))
        result = pl.pallas_call(
            kernel,
            name=name,
            out_shape=[jax.ShapeDtypeStruct(s, d) for s, d in outs],
            in_specs=[pl.BlockSpec(memory_space=pltpu.SMEM)] * smem
            + [pl.BlockSpec(memory_space=pl.ANY) if i in whole else VMEM for i in range(smem, len(args))]
            if whole
            else [pl.BlockSpec(memory_space=pltpu.SMEM)] * smem + [VMEM] * (len(args) - smem),
            out_specs=[VMEM] * len(outs),
            scratch_shapes=list(scratch),
            input_output_aliases=alias or {},
            compiler_params=pltpu.CompilerParams(vmem_limit_bytes=limit << 20),
            cost_estimate=pl.CostEstimate(flops=1000 + cost, bytes_accessed=1000, transcendentals=0),
        )(*args)
        self.last = result[0]
        return result


def send(values, bit, count):
    return lax.ppermute(values, "dp", [(i, i ^ (1 << bit)) for i in range(count)])


def swap(values):
    return lax.ppermute(values, "mp", [(0, 1), (1, 0)])


class Scatter:
    def __init__(self, steps, count, bits, plan, pieces=2, wide=1, small=None):
        self.steps, self.count, self.bits = steps, count, bits
        self.pieces, self.wide, self.small = pieces, wide, small
        self.plan, self.arrays, self.columns = [], [], 0
        for lefts, rights in plan:
            at, each = len(self.arrays), len(lefts)
            self.arrays += lefts + rights
            places = list(range(at, at + each)), list(range(at + each, at + 2 * each))
            self.plan.append((*places, self.columns))
            self.columns += rights[0].shape[1]
        self.rows = plan[0][0][0].shape[0] // 2
        self.extra = SMALL if small is not None else 0
        self.at = 1

    def shapes(self, *sizes):
        return [((n, self.columns), HIGH) for n in sizes]

    def far(self):
        size = self.rows // self.pieces
        kernel = partial(
            far_kernel,
            plan=self.plan,
            start=self.rows,
            pieces=self.pieces,
            small=bool(self.extra),
        )
        held = self.arrays + ([self.small] if self.extra else [])
        outs = self.shapes(size + self.extra, *[size] * (self.pieces - 1))
        outs = self.steps(kernel, "far", outs, held)
        self.got = [send(o, self.bits[0], self.count) for o in outs]

    def near(self):
        kernel = partial(
            near_kernel,
            plan=self.plan,
            pieces=self.pieces,
            small=bool(self.extra),
        )
        held = self.arrays + self.got + ([self.small] if self.extra else [])
        self.rows //= 2
        outs = self.shapes(self.rows, self.rows + self.extra)
        self.keep, self.sent = self.steps(kernel, "near", outs, held)
        self.got = send(self.sent, self.bits[1], self.count)

    def rest(self):
        while self.at + 1 < len(self.bits):
            self.step()

    def step(self):
        self.at += 1
        self.rows //= 2
        outs = self.shapes(self.rows, self.rows + self.extra)
        kernel = partial(step_kernel, small=bool(self.extra), joined=False)
        self.keep, self.sent = self.steps(kernel, "sum", outs, [self.keep, self.sent, self.got])
        self.got = send(self.sent, self.bits[self.at], self.count)


def join(one, two):
    for part in (one, two):
        part.at += 1
        part.rows //= 2
    outs = one.shapes(one.rows) + two.shapes(two.rows) + one.shapes(one.rows + two.rows + one.extra)
    kernel = partial(step_kernel, small=bool(one.extra), joined=True)
    held = [one.keep, two.keep, one.sent, two.sent, one.got, two.got]
    one.keep, two.keep, sent = one.steps(kernel, "sums", outs, held)
    got = send(sent, one.bits[one.at], one.count)
    while one.at + 1 < len(one.bits):
        one.at += 1
        half = one.rows // 2
        starts = (0, one.rows + one.extra)
        keeps, sents = [], []
        for part, start in zip((one, two), starts):
            total = part.keep + got[start : start + part.rows]
            keeps.append(total[:half])
            sents.append(total[half:])
        if one.extra:
            at = slice(one.rows, one.rows + one.extra)
            sents.insert(1, sent[at] + got[at])
        one.keep, two.keep = keeps
        one.rows = two.rows = half
        sent = jnp.concatenate(sents)
        got = send(sent, one.bits[one.at], one.count)
    return sent, got


def finish(parts, got, cost=0):
    outs = []
    for part in parts:
        outs += [((part.rows, part.columns // part.wide), HIGH)] * part.wide
    kernel = partial(end_kernel, wide=parts[0].wide)
    held = [part.keep for part in parts] + [got]
    return parts[0].steps(kernel, "end", outs, held, cost=cost)


def body(
    tokens,
    crop_ids,
    w_query,
    w_key,
    w_value,
    bias_query,
    bias_value,
    w_out,
    bias_out,
    gain_attn,
    shift_attn,
    gain_mlp,
    shift_mlp,
    w_up,
    bias_up,
    w_down,
    bias_down,
    cotangent,
    count,
):
    width = tokens.shape[1]
    local = w_query.shape[1]
    hidden_units = w_up.shape[1]
    seqs, length = crop_ids.shape
    rows = seqs * length
    here = lax.axis_index("dp")
    scalar = here.reshape(1)
    bits = list(range(count.bit_length() - 1))
    orders = (bits, [0, 2, 1] + bits[3:])
    steps = Steps()
    piece = local // 4
    lines = [gain_attn, shift_attn, bias_query, bias_value, bias_out, gain_mlp, shift_mlp]
    lines += [bias_down, bias_up]
    crops = BIAS_UP + hidden_units // width
    held = [((piece, width), LOW), (crop_ids.shape, jnp.int32)] + [(v.shape, HIGH) for v in lines]
    mine, table = steps(
        load_kernel,
        "load",
        [((piece, width), HIGH), ((crops + seqs, width), HIGH)],
        [scalar, w_out, crop_ids] + lines,
        scratch=[pltpu.VMEM(*h) for h in held] + [pltpu.SemaphoreType.DMA((len(held),))],
        smem=1,
        whole=range(1, 3 + len(lines)),
        limit=63,
    )
    got = swap(mine)

    def like(*arrays):
        return [(a.shape, a.dtype) for a in arrays]

    front = steps(
        partial(front_kernel, length=length, seqs=seqs, crops=crops),
        "front",
        like(tokens, w_query, w_key, w_value)
        + [((rows, width), LOW)]
        + [((rows, local), LOW)] * 3
        + [((rows, 128), HIGH)]
        + [((length, local), HIGH)] * seqs,
        [tokens, w_query, w_key, w_value, table],
        scratch=[pltpu.SemaphoreType.DMA((4,))],
        whole=range(4),
        limit=58,
    )
    tokens, w_query, w_key, w_value, first, query, key_rows, value_rows, log_total = front[:9]
    mixed = list(front[9:])
    mixed_other = [swap(o) for o in mixed]

    got, _ = lax.optimization_barrier((got, first))
    beside = send(got, 1, count)
    pieces = [got, send(got, 0, count), beside, send(beside, 0, count)]
    turned = steps(
        partial(turn_kernel, count=count, orders=orders),
        "turn",
        like(cotangent, w_up, w_down, w_out)
        + [((width, width), LOW), ((1, width), HIGH)]
        + [((width, length), LOW)] * (3 * seqs),
        [scalar, first, cotangent, w_up, w_down, w_out],
        scratch=[pltpu.SemaphoreType.DMA((4,))],
        whole=range(2, 6),
        smem=1,
        tie=1,
        limit=44,
    )

    cotangent, w_up, w_down, w_out, order_b, cot_sum = turned[:6]
    a1_a, a1_b, cot_a = (list(turned[6 + i * seqs : 6 + (i + 1) * seqs]) for i in range(3))
    hidden, a2_b, active, g_pre, second, carried = [], [], [], [], [], []
    for s in range(seqs):
        result = steps(
            partial(middle_kernel, blocks=4, seq=s, length=length),
            "middle",
            [
                ((length, width), HIGH),
                ((width, length), LOW),
                ((length, hidden_units), LOW),
                ((length, hidden_units), LOW),
                ((length, width), HIGH),
                ((1, hidden_units), HIGH),
                ((local, width), LOW),
            ],
            [
                scalar,
                tokens,
                mixed[s],
                mixed_other[s],
                w_out,
                table,
                w_up,
                w_down,
                cotangent,
                order_b,
            ]
            + (carried if s else pieces),
            smem=1,
            tie=2,
        )
        for held, value in zip((hidden, a2_b, active, g_pre, second), result):
            held.append(value)
        carried = list(result[5:])
    bias_sum = carried[0]
    second_other = [swap(g) for g in second]

    down = Scatter(steps, count, orders[0], [(cot_a, active)])
    up = Scatter(steps, count, orders[1], [(a2_b, g_pre)])
    down.far()
    up.far()
    mlp_part = steps(mlp_kernel, "mlp", [((rows, width), HIGH)], [w_down] + active, tie=1)[0]
    mlp_other = swap(mlp_part)
    down.near()
    up.near()
    g_hidden, gh_b, g_qk, g_val, carried = [], [], [], [], [bias_sum, cot_sum]
    for s in range(seqs):
        if s == seqs - 1:
            down.step()
            up.step()
        result = steps(
            partial(back_kernel, seq=s, length=length, crops=crops),
            "back",
            [
                ((length, width), HIGH),
                ((width, length), LOW),
                ((length, 2 * local), LOW),
                ((length, local), LOW),
                ((SMALL, width), HIGH),
                (((s + 1) * length, width), HIGH),
            ],
            [tokens, table, cotangent, hidden[s], second[s], second_other[s], order_b]
            + [w_out, w_query, w_key, w_value, query, key_rows, value_rows, log_total]
            + carried,
            tie=4,
            cost=0 if s else 6 * 10**9,
        )
        for held, value in zip((g_hidden, gh_b, g_qk, g_val), result):
            held.append(value)
        carried = list(result[4:])
    sums, g_first = carried
    first_other = swap(g_first)
    heads = Scatter(steps, count, orders[0], [(a1_a, g_qk)], wide=2, small=sums)
    others = Scatter(steps, count, orders[1], [(a1_b, g_val), (gh_b, mixed)], wide=2)
    heads.far()
    others.far()
    _, mlp_got = join(down, up)
    heads.near()
    others.near()
    block_out = steps(
        partial(out_kernel, seqs=seqs, length=length),
        "out",
        [((rows, width), LOW)],
        [table, mlp_part, mlp_other] + hidden,
        tie=1,
        cost=3 * 10**9,
    )[0]
    heads.step()
    others.step()
    w_down_t, done_w_up = finish([down, up], mlp_got, 15 * 10**8)
    heads.rest()
    others.rest()
    base, unit, scale = steps(
        partial(base_kernel, length=length),
        "base",
        [((rows, width), HIGH)] * 2 + [((rows, 1), HIGH)],
        [table, tokens, g_first] + g_hidden,
        tie=2,
    )
    grad_tokens = steps(
        partial(last_kernel, length=length),
        "last",
        [((rows, width), HIGH)],
        [table, base, unit, scale, first_other],
        tie=1,
    )[0]
    size = width // count
    (
        grad_w_q,
        grad_w_k,
        done_bias_q,
        done_bias_v,
        done_bias_up,
        done_gain_mlp,
        done_shift_mlp,
        done_bias_out,
        done_bias_down,
        gains,
    ) = steps(
        final_kernel,
        "final",
        [((size, local), HIGH)] * 2
        + [((local,), HIGH)] * 2
        + [((hidden_units,), HIGH)]
        + [((size,), HIGH)] * 4
        + [((8, 128), HIGH)],
        [scalar, heads.keep, heads.sent, heads.got],
        smem=1,
        tie=1,
    )
    gains_other = swap(gains)
    grad_w_v, w_out_t = finish([others], others.got)
    done_gain_attn, done_shift_attn = steps(
        gain_kernel, "gains", [((size,), HIGH)] * 2, [gains, gains_other]
    )
    return (
        block_out,
        grad_tokens,
        grad_w_q,
        grad_w_k,
        grad_w_v,
        done_bias_q,
        done_bias_v,
        w_out_t.T,
        done_bias_out,
        done_gain_attn,
        done_shift_attn,
        done_gain_mlp,
        done_shift_mlp,
        done_w_up,
        done_bias_up,
        w_down_t.T,
        done_bias_down,
    )


def solution(mesh):
    placed = (
        P("dp", None),
        P("dp", None),
        P(None, "mp"),
        P(None, "mp"),
        P(None, "mp"),
        P("mp"),
        P("mp"),
        P("mp", None),
        P(),
        P(),
        P(),
        P(),
        P(),
        P(None, "mp"),
        P("mp"),
        P("mp", None),
        P(),
        P("dp", None),
    )
    return jax.shard_map(
        partial(body, count=mesh.shape["dp"]),
        mesh=mesh,
        in_specs=placed,
        out_specs=(
            P("dp", None),
            P("dp", None),
            P("dp", "mp"),
            P("dp", "mp"),
            P("dp", "mp"),
            P("mp"),
            P("mp"),
            P("mp", "dp"),
            P("dp"),
            P("dp"),
            P("dp"),
            P("dp"),
            P("dp"),
            P("dp", "mp"),
            P("mp"),
            P("mp", "dp"),
            P("dp"),
        ),
        check_vma=False,
    )
```

```python
from functools import partial

import jax
import jax.numpy as jnp
from jax import lax
from jax.experimental import pallas as pl
from jax.experimental.pallas import tpu as pltpu
from jax.sharding import PartitionSpec as P

HEAD_DIM = 64
PAIR = 2 * HEAD_DIM
EPS = 1e-06
NEGATIVE = -1e30
LOW = jnp.bfloat16
HIGH = jnp.float32
VMEM = pl.BlockSpec(memory_space=pltpu.VMEM)
SMALL = 16
GAIN_ATTN, SHIFT_ATTN, BIAS_Q, BIAS_V, BIAS_OUT, GAIN_MLP, SHIFT_MLP, BIAS_DOWN, BIAS_UP = range(9)


def plain_dot(left, right):
    return jnp.dot(left, right, preferred_element_type=HIGH)


def right_trans(left, right):
    return lax.dot_general(left, right, (((1,), (1,)), ((), ())), preferred_element_type=HIGH)


def left_trans(left, right):
    return lax.dot_general(left, right, (((0,), (0,)), ((), ())), preferred_element_type=HIGH)


def unit_rows(values):
    mean = jnp.mean(values, axis=-1, keepdims=True)
    centred = values - mean
    scale = lax.rsqrt(jnp.mean(centred * centred, axis=-1, keepdims=True) + EPS)
    return centred * scale, scale


def norm_back(grad_unit, unit, scale):
    inner = jnp.mean(grad_unit * unit, axis=-1, keepdims=True)
    return scale * (grad_unit - jnp.mean(grad_unit, axis=-1, keepdims=True) - unit * inner)


def half_masks():
    lane = lax.broadcasted_iota(jnp.int32, (1, PAIR), 1)
    first = lane < HEAD_DIM
    return first, (first.astype(HIGH).astype(LOW), (~first).astype(HIGH).astype(LOW))


def col_sum(values):
    return jnp.sum(values, axis=0, keepdims=True)


def row(table, at, size):
    return table[at : at + 1, :size]


def same_crop(table, slot, length):
    ids = row(table, slot, length)
    marks = lax.broadcasted_iota(jnp.int32, (SMALL, length), 0).astype(HIGH) == ids
    marks = marks.astype(HIGH).astype(LOW)
    return left_trans(marks, marks) > 0.5


def copies_of(sources, targets, sems):
    copies = [pltpu.make_async_copy(a, b, sems.at[i]) for i, (a, b) in enumerate(zip(sources, targets))]
    for copy in copies:
        copy.start()
    return copies


def load_kernel(here, w_out, crops, *refs):
    count = (len(refs) - 5) // 2
    vectors, (piece, table), sems = refs[:count], refs[count : count + 2], refs[-1]
    held = refs[count + 2 : -1]
    size = piece.shape[0]
    start = pl.multiple_of((here[0] & 3) * size, size)
    sources = [w_out.at[pl.ds(start, size), :], crops, *vectors]
    copies = copies_of(sources, held, sems)
    copies[0].wait()
    piece[...] = held[0][...].astype(HIGH)
    for copy in copies[1:]:
        copy.wait()
    table[...] = jnp.zeros_like(table)
    at, width = 0, table.shape[1]
    for vector in held[2:]:
        for low in range(0, vector.shape[0], width):
            part = min(width, vector.shape[0] - low)
            table[at : at + 1, :part] = vector[low : low + part].reshape(1, part)
            at += 1
    seqs, length = held[1].shape
    table[at : at + seqs, :length] = held[1][...].astype(HIGH)


def front_kernel(*refs, length, seqs, crops):
    sources, table, held = refs[:4], refs[4], refs[5:9]
    first_out, q, k, v, lse = refs[9:14]
    outs, sems = refs[14:-1], refs[-1]
    copies = copies_of(sources, held, sems)
    tokens, w_q, w_k, w_v = held
    copies[0].wait()
    unit, _ = unit_rows(tokens[...].astype(HIGH))
    local, width = w_q.shape[1], tokens.shape[1]
    first = (unit * row(table, GAIN_ATTN, width) + row(table, SHIFT_ATTN, width)).astype(LOW)
    first_out[...] = first
    for copy in copies[1:]:
        copy.wait()
    q_all = plain_dot(first, w_q[...]) + row(table, BIAS_Q, local)
    q_all = (q_all.astype(LOW) * 0.125).astype(LOW)
    k_all = plain_dot(first, w_k[...]).astype(LOW)
    v_all = (plain_dot(first, w_v[...]) + row(table, BIAS_V, local)).astype(LOW)
    q[...] = q_all
    k[...] = k_all
    v[...] = v_all
    low_half, masks = half_masks()
    for s, o in enumerate(outs):
        rows = slice(s * length, (s + 1) * length)
        same = same_crop(table, crops + s, length)
        for t in range(local // PAIR):
            at = slice(t * PAIR, (t + 1) * PAIR)
            q_pair, k_pair, v_pair = q_all[rows, at], k_all[rows, at], v_all[rows, at]
            got = []
            for half in range(2):
                scores = jnp.where(same, right_trans(q_pair * masks[half], k_pair), NEGATIVE)
                top = jnp.max(scores, axis=-1, keepdims=True)
                expo = jnp.exp(scores - top)
                total = jnp.sum(expo, axis=-1, keepdims=True)
                probs = (expo * (1.0 / total)).astype(LOW)
                got.append(plain_dot(probs, v_pair))
                h = 2 * t + half
                lse[rows, h : h + 1] = top + jnp.log(total)
            o[:, at] = jnp.where(low_half, got[0], got[1])


def relative_rows(here, width, count, bits):
    size = width // count
    place = lax.broadcasted_iota(jnp.int32, (width, 1), 0)
    block = ((place.astype(HIGH) + 0.5) * (1.0 / size)).astype(jnp.int32)
    mask = jnp.zeros_like(block)
    for p, bit in enumerate(bits):
        mask = mask + (((block >> (len(bits) - 1 - p)) & 1) << bit)
    source = (mask ^ here) * size + (place - block * size)
    marks = lax.broadcasted_iota(jnp.int32, (width, width), 1) == source
    return marks.astype(HIGH).astype(LOW)


def turn_kernel(here, *refs, count, orders):
    sources, held = refs[:4], (refs[-2], *refs[4:7])
    order_b, sums, sems = refs[7], refs[8], refs[-1]
    seqs = (len(refs) - 11) // 3
    a1_a, a1_b, cot_a = (refs[9 + i * seqs : 9 + (i + 1) * seqs] for i in range(3))
    first = refs[-2]
    length = first.shape[0] // seqs
    copies = copies_of(sources, held, sems)
    width = first.shape[1]
    order_a = relative_rows(here[0], width, count, orders[0])
    order = relative_rows(here[0], width, count, orders[1])
    order_b[...] = order
    copies[0].wait()
    for s in range(seqs):
        part = first[s * length : (s + 1) * length, :]
        a1_a[s][...] = right_trans(order_a, part).astype(LOW)
        a1_b[s][...] = right_trans(order, part).astype(LOW)
    for copy in copies[1:]:
        copy.wait()
    cot = held[1][...]
    for s in range(seqs):
        part = cot[s * length : (s + 1) * length, :]
        cot_a[s][...] = right_trans(order_a, part).astype(LOW)
    sums[...] = col_sum(cot.astype(HIGH))


def low_kernel(values, out):
    out[...] = values[...].astype(LOW)


def gather_kernel(here, *refs):
    for b, piece in enumerate(refs[:-1]):
        size = piece.shape[0]
        start = pl.multiple_of(((here[0] & 3) ^ b) * size, size)
        refs[-1][pl.ds(start, size), :] = piece[...].astype(LOW)


def middle_kernel(*refs, blocks, seq, length):
    tokens, o_own, o_other, w_out, w_low, table, w_up, w_down, cotangent, order = refs[:10]
    hidden, a2_t, active, g_pre, g_second, g_bias = refs[-6:]
    rows = slice(seq * length, (seq + 1) * length)
    attn = plain_dot(o_own[...].astype(LOW), w_out[...])
    attn = attn + plain_dot(o_other[...].astype(LOW), w_low[...])
    width = tokens.shape[1]
    values = tokens[rows, :].astype(HIGH) + (attn + row(table, BIAS_OUT, width))
    hidden[...] = values
    unit, _ = unit_rows(values)
    second = (unit * row(table, GAIN_MLP, width) + row(table, SHIFT_MLP, width)).astype(LOW)
    cot = cotangent[rows, :]
    size = w_up.shape[1] // blocks
    total = None
    for b in range(blocks):
        at = slice(b * size, (b + 1) * size)
        low = b * size % width
        at_row = BIAS_UP + b * size // width
        bias_up = table[at_row : at_row + 1, low : low + size]
        pre = plain_dot(second, w_up[:, at]) + bias_up
        cdf = 0.5 * (1.0 + lax.erf(pre * 0.7071067811865476))
        active[:, at] = (pre * cdf).astype(LOW)
        slope = cdf + pre * (0.3989422804014327 * jnp.exp(-0.5 * (pre * pre)))
        grad = (right_trans(cot, w_down[at, :]) * slope).astype(LOW)
        g_pre[:, at] = grad
        bias = col_sum(grad.astype(HIGH))
        g_bias[:, at] = refs[10][:, at] + bias if seq else bias
        part = right_trans(grad, w_up[:, at])
        total = part if total is None else total + part
    g_second[...] = total
    a2_t[...] = right_trans(order[...], second).astype(LOW)


def back_kernel(*refs, seq, length, crops):
    tokens, table, cotangent, hidden, own, other, order = refs[:7]
    w_out, w_q, w_k, w_v, q, k, v, lse = refs[7:15]
    before = refs[15:17]
    g_hidden, gh_t, g_qk, g_val, sums, g_first = refs[17:]
    width, local = tokens.shape[1], q.shape[1]
    rows = slice(seq * length, (seq + 1) * length)
    full = slice(0, width)
    if seq:
        sums_before, first_before = before
        g_first[: seq * length, :] = first_before[...]
        sums[6:, :] = sums_before[6:, :]
    else:
        g_bias, cot_sum = before
        sums[6:7, :] = g_bias[:, :width]
        sums[7:8, :] = g_bias[:, width:]
        sums[8:9, :] = cot_sum[...]
        sums[9:, :] = jnp.zeros_like(sums[9:, :])

    def put(r, at, value):
        sums[r : r + 1, at] = sums_before[r : r + 1, at] + value if seq else value

    unit, scale = unit_rows(hidden[...])
    grad = own[...] + other[...]
    put(0, full, col_sum(grad * unit))
    put(1, full, col_sum(grad))
    values = norm_back(grad * row(table, GAIN_MLP, width), unit, scale)
    values = cotangent[rows, :].astype(HIGH) + values
    g_hidden[...] = values
    put(2, full, col_sum(values))
    low = values.astype(LOW)
    gh_t[...] = right_trans(order[...], low).astype(LOW)
    g_o = right_trans(low, w_out[...]).astype(LOW)
    same = same_crop(table, crops + seq, length)
    low_half, masks = half_masks()
    for t in range(local // PAIR):
        at = slice(t * PAIR, (t + 1) * PAIR)
        q_pair, k_pair, v_pair, o_pair = q[rows, at], k[rows, at], v[rows, at], g_o[:, at]
        got = []
        for half in range(2):
            h = 2 * t + half
            scores = right_trans(q_pair * masks[half], k_pair)
            probs = jnp.exp(jnp.where(same, scores, NEGATIVE) - lse[rows, h : h + 1])
            g_probs = right_trans(o_pair * masks[half], v_pair)
            inner = jnp.sum(g_probs * probs, axis=-1, keepdims=True)
            g_scores = (probs * (g_probs - inner)).astype(LOW)
            got.append(
                (
                    plain_dot(g_scores, k_pair),
                    left_trans(g_scores, q_pair),
                    left_trans(probs.astype(LOW), o_pair),
                )
            )
        g_q = (jnp.where(low_half, got[0][0], got[1][0]) * 0.125).astype(LOW)
        g_k = jnp.where(low_half, got[0][1], got[1][1]).astype(LOW)
        g_v = jnp.where(low_half, got[0][2], got[1][2]).astype(LOW)
        beside = slice(local + t * PAIR, local + (t + 1) * PAIR)
        g_qk[:, at] = g_q
        g_qk[:, beside] = g_k
        g_val[:, at] = g_v
        put(5, at, col_sum(g_q.astype(HIGH)))
        put(5, beside, col_sum(g_v.astype(HIGH)))
    part = right_trans(g_qk[:, :local], w_q[...])
    part = part + right_trans(g_qk[:, local:], w_k[...])
    part = part + right_trans(g_val[...], w_v[...])
    g_first[rows, :] = part
    unit_one, _ = unit_rows(tokens[rows, :].astype(HIGH))
    put(3, full, col_sum(part * unit_one))
    put(4, full, col_sum(part))


def base_kernel(table, tokens, own, *refs, length):
    g_hidden, (base, unit_out, scale_out) = refs[:-3], refs[-3:]
    gain = row(table, GAIN_ATTN, tokens.shape[1])
    for s in range(tokens.shape[0] // length):
        rows = slice(s * length, (s + 1) * length)
        part = own[rows, :]
        unit, scale = unit_rows(tokens[rows, :].astype(HIGH))
        base[rows, :] = g_hidden[s][...] + norm_back(part * gain, unit, scale)
        unit_out[rows, :] = unit
        scale_out[rows, :] = scale


def last_kernel(table, base, unit, scale, other, g_tokens, *, length):
    gain = row(table, GAIN_ATTN, base.shape[1])
    for s in range(base.shape[0] // length):
        rows = slice(s * length, (s + 1) * length)
        grad = norm_back(other[rows, :] * gain, unit[rows, :], scale[rows, :])
        g_tokens[rows, :] = base[rows, :] + grad


def out_kernel(*refs, seqs, length):
    table, own, other = refs[:3]
    for s in range(seqs):
        rows = slice(s * length, (s + 1) * length)
        total = refs[3 + s][...] + (own[rows, :] + other[rows, :])
        refs[3 + seqs][rows, :] = (total + row(table, BIAS_DOWN, total.shape[1])).astype(LOW)


def mlp_kernel(w_down, *refs):
    length = refs[0].shape[0]
    for s, active in enumerate(refs[:-1]):
        refs[-1][s * length : (s + 1) * length, :] = plain_dot(active[...], w_down[...])


def products(plan, refs, at):
    for lefts, rights, column in plan:
        wide = refs[rights[0]].shape[1]
        step = min(512, wide)
        for n in range(0, wide, step):
            value = None
            for left, right in zip(lefts, rights):
                part = plain_dot(refs[left][at, :], refs[right][:, n : n + step].astype(LOW))
                value = part if value is None else value + part
            yield slice(column + n, column + n + step), value


def far_kernel(*refs, plan, start, pieces, small):
    outs = refs[-pieces:]
    size = start // pieces
    for o, out in enumerate(outs):
        at = slice(start + o * size, start + (o + 1) * size)
        for columns, value in products(plan, refs, at):
            out[:size, columns] = value
    if small:
        outs[0][size:, :] = refs[-pieces - 1][...]


def near_kernel(*refs, plan, pieces, small):
    outs, got = refs[-2:], refs[-2 - pieces - small :]
    half = outs[0].shape[0]
    for o, out in enumerate(outs):
        at = slice(o * half, (o + 1) * half)
        size = 2 * half // pieces
        low = o * half % size
        for columns, value in products(plan, refs, at):
            out[:half, columns] = value + got[o * half // size][low : low + half, columns]
    if small:
        outs[1][half:, :] = got[pieces][...] + got[0][2 * half // pieces :, :]


def step_kernel(*refs, small, joined):
    count = 2 if joined else 1
    keeps, sents, gots = (refs[i * count : (i + 1) * count] for i in range(3))
    outs = refs[3 * count :]
    at = 0
    for i in range(count):
        half = outs[i].shape[0]
        got = gots[i]
        outs[i][...] = keeps[i][:half, :] + got[:half, :]
        outs[count][at : at + half, :] = keeps[i][half:, :] + got[half : 2 * half, :]
        at += half
        if small and not i:
            outs[count][at : at + SMALL, :] = sents[i][2 * half :, :] + got[2 * half :, :]
            at += SMALL


def end_kernel(*refs, wide):
    count = (len(refs) - 1) // (1 + wide)
    keeps, got, outs = refs[:count], refs[count], refs[count + 1 :]
    at = o = 0
    for keep in keeps:
        size, each = keep.shape[0], keep.shape[1] // wide
        for w in range(wide):
            columns = slice(w * each, (w + 1) * each)
            outs[o][...] = keep[:, columns] + got[at : at + size, columns]
            o += 1
        at += size


def vector_kernel(here, sent, got, *outs, size):
    total = sent[size : size + SMALL, :] + got[size : size + SMALL, :]
    bias_q, bias_v, bias_up, gain_mlp, shift_mlp, bias_out, bias_down, gains = outs
    width, each = total.shape[1], bias_q.shape[0]
    bias_q[...] = total[5, :each]
    bias_v[...] = total[5, each:]
    for i in range(bias_up.shape[0] // width):
        bias_up[i * width : (i + 1) * width] = total[6 + i, :]
    turned = pltpu.roll(total, lax.rem(width - here[0] * size, width), 1)
    for out, at in ((gain_mlp, 0), (shift_mlp, 1), (bias_out, 2), (bias_down, 8)):
        out[...] = turned[at, :size]
    gains[...] = turned[:8, : gains.shape[1]]


def gain_kernel(own, other, gain, shift):
    total = own[...] + other[...]
    gain[...] = total[3, : gain.shape[0]]
    shift[...] = total[4, : shift.shape[0]]


class Steps:
    def __init__(self):
        self.last = None

    def __call__(
        self, kernel, name, outs, args, scratch=(), limit=12, smem=0, whole=0, tie=0, alias=None, cost=0
    ):
        args = list(args)
        if self.last is not None:
            args[tie], _ = lax.optimization_barrier((args[tie], self.last))
        result = pl.pallas_call(
            kernel,
            name=name,
            out_shape=[jax.ShapeDtypeStruct(s, d) for s, d in outs],
            in_specs=[pl.BlockSpec(memory_space=pltpu.SMEM)] * smem
            + [pl.BlockSpec(memory_space=pl.ANY) if i in whole else VMEM for i in range(smem, len(args))]
            if whole
            else [pl.BlockSpec(memory_space=pltpu.SMEM)] * smem + [VMEM] * (len(args) - smem),
            out_specs=[VMEM] * len(outs),
            scratch_shapes=list(scratch),
            input_output_aliases=alias or {},
            compiler_params=pltpu.CompilerParams(vmem_limit_bytes=limit << 20),
            cost_estimate=pl.CostEstimate(flops=1000 + cost, bytes_accessed=1000, transcendentals=0),
        )(*args)
        self.last = result[0]
        return result


def send(values, bit, count):
    return lax.ppermute(values, "dp", [(i, i ^ (1 << bit)) for i in range(count)])


def swap(values):
    return lax.ppermute(values, "mp", [(0, 1), (1, 0)])


class Scatter:
    def __init__(self, steps, count, bits, plan, pieces=2, wide=1, small=None):
        self.steps, self.count, self.bits = steps, count, bits
        self.pieces, self.wide, self.small = pieces, wide, small
        self.plan, self.arrays, self.columns = [], [], 0
        for lefts, rights in plan:
            at, each = len(self.arrays), len(lefts)
            self.arrays += lefts + rights
            places = list(range(at, at + each)), list(range(at + each, at + 2 * each))
            self.plan.append((*places, self.columns))
            self.columns += rights[0].shape[1]
        self.rows = plan[0][0][0].shape[0] // 2
        self.extra = SMALL if small is not None else 0
        self.at = 1

    def shapes(self, *sizes):
        return [((n, self.columns), HIGH) for n in sizes]

    def far(self):
        size = self.rows // self.pieces
        kernel = partial(
            far_kernel,
            plan=self.plan,
            start=self.rows,
            pieces=self.pieces,
            small=bool(self.extra),
        )
        held = self.arrays + ([self.small] if self.extra else [])
        outs = self.shapes(size + self.extra, *[size] * (self.pieces - 1))
        outs = self.steps(kernel, "far", outs, held)
        self.got = [send(o, self.bits[0], self.count) for o in outs]

    def near(self):
        kernel = partial(
            near_kernel,
            plan=self.plan,
            pieces=self.pieces,
            small=bool(self.extra),
        )
        held = self.arrays + self.got + ([self.small] if self.extra else [])
        self.rows //= 2
        outs = self.shapes(self.rows, self.rows + self.extra)
        self.keep, self.sent = self.steps(kernel, "near", outs, held)
        self.got = send(self.sent, self.bits[1], self.count)

    def rest(self):
        while self.at + 1 < len(self.bits):
            self.step()

    def step(self):
        self.at += 1
        self.rows //= 2
        outs = self.shapes(self.rows, self.rows + self.extra)
        kernel = partial(step_kernel, small=bool(self.extra), joined=False)
        self.keep, self.sent = self.steps(kernel, "sum", outs, [self.keep, self.sent, self.got])
        self.got = send(self.sent, self.bits[self.at], self.count)


def join(one, two):
    for part in (one, two):
        part.at += 1
        part.rows //= 2
    outs = one.shapes(one.rows) + two.shapes(two.rows) + one.shapes(one.rows + two.rows + one.extra)
    kernel = partial(step_kernel, small=bool(one.extra), joined=True)
    held = [one.keep, two.keep, one.sent, two.sent, one.got, two.got]
    one.keep, two.keep, sent = one.steps(kernel, "sums", outs, held)
    got = send(sent, one.bits[one.at], one.count)
    while one.at + 1 < len(one.bits):
        one.at += 1
        half = one.rows // 2
        starts = (0, one.rows + one.extra)
        keeps, sents = [], []
        for part, start in zip((one, two), starts):
            total = part.keep + got[start : start + part.rows]
            keeps.append(total[:half])
            sents.append(total[half:])
        if one.extra:
            at = slice(one.rows, one.rows + one.extra)
            sents.insert(1, sent[at] + got[at])
        one.keep, two.keep = keeps
        one.rows = two.rows = half
        sent = jnp.concatenate(sents)
        got = send(sent, one.bits[one.at], one.count)
    return sent, got


def finish(parts, got, cost=0):
    outs = []
    for part in parts:
        outs += [((part.rows, part.columns // part.wide), HIGH)] * part.wide
    kernel = partial(end_kernel, wide=parts[0].wide)
    held = [part.keep for part in parts] + [got]
    return parts[0].steps(kernel, "end", outs, held, cost=cost)


def body(
    tokens,
    crop_ids,
    w_query,
    w_key,
    w_value,
    bias_query,
    bias_value,
    w_out,
    bias_out,
    gain_attn,
    shift_attn,
    gain_mlp,
    shift_mlp,
    w_up,
    bias_up,
    w_down,
    bias_down,
    cotangent,
    count,
):
    width = tokens.shape[1]
    local = w_query.shape[1]
    hidden_units = w_up.shape[1]
    seqs, length = crop_ids.shape
    rows = seqs * length
    here = lax.axis_index("dp")
    scalar = here.reshape(1)
    bits = list(range(count.bit_length() - 1))
    orders = (bits, [0, 2, 1] + bits[3:])
    steps = Steps()
    piece = local // 4
    lines = [gain_attn, shift_attn, bias_query, bias_value, bias_out, gain_mlp, shift_mlp]
    lines += [bias_down, bias_up]
    crops = BIAS_UP + hidden_units // width
    held = [((piece, width), LOW), (crop_ids.shape, jnp.int32)] + [(v.shape, HIGH) for v in lines]
    mine, table = steps(
        load_kernel,
        "load",
        [((piece, width), HIGH), ((crops + seqs, width), HIGH)],
        [scalar, w_out, crop_ids] + lines,
        scratch=[pltpu.VMEM(*h) for h in held] + [pltpu.SemaphoreType.DMA((len(held),))],
        smem=1,
        whole=range(1, 3 + len(lines)),
        limit=63,
    )
    got = swap(mine)

    def like(*arrays):
        return [(a.shape, a.dtype) for a in arrays]

    front = steps(
        partial(front_kernel, length=length, seqs=seqs, crops=crops),
        "front",
        like(tokens, w_query, w_key, w_value)
        + [((rows, width), LOW)]
        + [((rows, local), LOW)] * 3
        + [((rows, 128), HIGH)]
        + [((length, local), HIGH)] * seqs,
        [tokens, w_query, w_key, w_value, table],
        scratch=[pltpu.SemaphoreType.DMA((4,))],
        whole=range(4),
        limit=58,
    )
    tokens, w_query, w_key, w_value, first, query, key_rows, value_rows, log_total = front[:9]
    mixed = list(front[9:])
    mixed_other = [swap(o) for o in mixed]

    got, _ = lax.optimization_barrier((got, first))
    beside = send(got, 1, count)
    pieces = [got, send(got, 0, count), beside]
    turned = steps(
        partial(turn_kernel, count=count, orders=orders),
        "turn",
        like(cotangent, w_up, w_out)
        + [((width, width), LOW), ((1, width), HIGH)]
        + [((width, length), LOW)] * (3 * seqs),
        [scalar, first, cotangent, w_up, w_out],
        scratch=[pltpu.VMEM((rows, width), LOW), pltpu.SemaphoreType.DMA((4,))],
        whole=range(1, 5),
        smem=1,
        tie=1,
        limit=44,
    )

    cotangent, w_up, w_out, order_b, cot_sum = turned[:5]
    a1_a, a1_b, cot_a = (list(turned[5 + i * seqs : 5 + (i + 1) * seqs]) for i in range(3))
    beside, _ = lax.optimization_barrier((beside, order_b))
    pieces.append(send(beside, 0, count))
    mixed_other[0] = steps(low_kernel, "low", [((length, local), LOW)], [mixed_other[0]], cost=31 * 10**8)[0]
    w_low = steps(
        gather_kernel, "gather", [((local, width), LOW)], [scalar] + pieces, smem=1, tie=1
    )[0]
    hidden, a2_b, active, g_pre, second, carried = [], [], [], [], [], []
    for s in range(seqs):
        result = steps(
            partial(middle_kernel, blocks=4, seq=s, length=length),
            "middle",
            [
                ((length, width), HIGH),
                ((width, length), LOW),
                ((length, hidden_units), LOW),
                ((length, hidden_units), LOW),
                ((length, width), HIGH),
                ((1, hidden_units), HIGH),
            ],
            [
                tokens,
                mixed[s],
                mixed_other[s],
                w_out,
                w_low,
                table,
                w_up,
                w_down,
                cotangent,
                order_b,
            ]
            + carried,
            tie=1,
        )
        for held, value in zip((hidden, a2_b, active, g_pre, second), result):
            held.append(value)
        carried = list(result[5:])
    bias_sum = carried[0]
    second_other = [swap(g) for g in second]

    down = Scatter(steps, count, orders[0], [(cot_a, active)])
    up = Scatter(steps, count, orders[1], [(a2_b, g_pre)])
    down.far()
    up.far()
    mlp_part = steps(mlp_kernel, "mlp", [((rows, width), HIGH)], [w_down] + active, tie=1)[0]
    mlp_other = swap(mlp_part)
    down.near()
    up.near()
    g_hidden, gh_b, g_qk, g_val, carried = [], [], [], [], [bias_sum, cot_sum]
    for s in range(seqs):
        if s == seqs - 1:
            down.step()
            up.step()
        result = steps(
            partial(back_kernel, seq=s, length=length, crops=crops),
            "back",
            [
                ((length, width), HIGH),
                ((width, length), LOW),
                ((length, 2 * local), LOW),
                ((length, local), LOW),
                ((SMALL, width), HIGH),
                (((s + 1) * length, width), HIGH),
            ],
            [tokens, table, cotangent, hidden[s], second[s], second_other[s], order_b]
            + [w_out, w_query, w_key, w_value, query, key_rows, value_rows, log_total]
            + carried,
            tie=4,
            cost=0 if s else 6 * 10**9,
        )
        for held, value in zip((g_hidden, gh_b, g_qk, g_val), result):
            held.append(value)
        carried = list(result[4:])
    sums, g_first = carried
    first_other = swap(g_first)
    heads = Scatter(steps, count, orders[0], [(a1_a, g_qk)], wide=2, small=sums)
    others = Scatter(steps, count, orders[1], [(a1_b, g_val), (gh_b, mixed)], wide=2)
    heads.far()
    others.far()
    _, mlp_got = join(down, up)
    heads.near()
    others.near()
    block_out = steps(
        partial(out_kernel, seqs=seqs, length=length),
        "out",
        [((rows, width), LOW)],
        [table, mlp_part, mlp_other] + hidden,
        tie=1,
        cost=3 * 10**9,
    )[0]
    heads.step()
    others.step()
    w_down_t, done_w_up = finish([down, up], mlp_got, 15 * 10**8)
    heads.rest()
    others.rest()
    base, unit, scale = steps(
        partial(base_kernel, length=length),
        "base",
        [((rows, width), HIGH)] * 2 + [((rows, 1), HIGH)],
        [table, tokens, g_first] + g_hidden,
        tie=2,
    )
    grad_tokens = steps(
        partial(last_kernel, length=length),
        "last",
        [((rows, width), HIGH)],
        [table, base, unit, scale, first_other],
        tie=1,
    )[0]
    size = width // count
    (
        done_bias_q,
        done_bias_v,
        done_bias_up,
        done_gain_mlp,
        done_shift_mlp,
        done_bias_out,
        done_bias_down,
        gains,
    ) = steps(
        partial(vector_kernel, size=size),
        "vectors",
        [((local,), HIGH)] * 2
        + [((hidden_units,), HIGH)]
        + [((size,), HIGH)] * 4
        + [((8, 128), HIGH)],
        [scalar, heads.sent, heads.got],
        smem=1,
        tie=1,
    )
    gains_other = swap(gains)
    grad_w_q, grad_w_k = finish([heads], heads.got)
    grad_w_v, w_out_t = finish([others], others.got)
    done_gain_attn, done_shift_attn = steps(
        gain_kernel, "gains", [((size,), HIGH)] * 2, [gains, gains_other]
    )
    return (
        block_out,
        grad_tokens,
        grad_w_q,
        grad_w_k,
        grad_w_v,
        done_bias_q,
        done_bias_v,
        w_out_t.T,
        done_bias_out,
        done_gain_attn,
        done_shift_attn,
        done_gain_mlp,
        done_shift_mlp,
        done_w_up,
        done_bias_up,
        w_down_t.T,
        done_bias_down,
    )


def solution(mesh):
    placed = (
        P("dp", None),
        P("dp", None),
        P(None, "mp"),
        P(None, "mp"),
        P(None, "mp"),
        P("mp"),
        P("mp"),
        P("mp", None),
        P(),
        P(),
        P(),
        P(),
        P(),
        P(None, "mp"),
        P("mp"),
        P("mp", None),
        P(),
        P("dp", None),
    )
    return jax.shard_map(
        partial(body, count=mesh.shape["dp"]),
        mesh=mesh,
        in_specs=placed,
        out_specs=(
            P("dp", None),
            P("dp", None),
            P("dp", "mp"),
            P("dp", "mp"),
            P("dp", "mp"),
            P("mp"),
            P("mp"),
            P("mp", "dp"),
            P("dp"),
            P("dp"),
            P("dp"),
            P("dp"),
            P("dp"),
            P("dp", "mp"),
            P("mp"),
            P("mp", "dp"),
            P("dp"),
        ),
        check_vma=False,
    )
```

```python
from functools import partial

import jax
import jax.numpy as jnp
from jax import lax
from jax.experimental import pallas as pl
from jax.experimental.pallas import tpu as pltpu
from jax.sharding import PartitionSpec as P

HEAD_DIM = 64
PAIR = 2 * HEAD_DIM
EPS = 1e-06
NEGATIVE = -1e30
LOW = jnp.bfloat16
HIGH = jnp.float32
VMEM = pl.BlockSpec(memory_space=pltpu.VMEM)
SMALL = 16
GAIN_ATTN, SHIFT_ATTN, BIAS_Q, BIAS_V, BIAS_OUT, GAIN_MLP, SHIFT_MLP, BIAS_DOWN, BIAS_UP = range(9)


def plain_dot(left, right):
    return jnp.dot(left, right, preferred_element_type=HIGH)


def right_trans(left, right):
    return lax.dot_general(left, right, (((1,), (1,)), ((), ())), preferred_element_type=HIGH)


def left_trans(left, right):
    return lax.dot_general(left, right, (((0,), (0,)), ((), ())), preferred_element_type=HIGH)


def unit_rows(values):
    mean = jnp.mean(values, axis=-1, keepdims=True)
    centred = values - mean
    scale = lax.rsqrt(jnp.mean(centred * centred, axis=-1, keepdims=True) + EPS)
    return centred * scale, scale


def norm_back(grad_unit, unit, scale):
    inner = jnp.mean(grad_unit * unit, axis=-1, keepdims=True)
    return scale * (grad_unit - jnp.mean(grad_unit, axis=-1, keepdims=True) - unit * inner)


def half_masks():
    lane = lax.broadcasted_iota(jnp.int32, (1, PAIR), 1)
    first = lane < HEAD_DIM
    return first, (first.astype(HIGH).astype(LOW), (~first).astype(HIGH).astype(LOW))


def col_sum(values):
    return jnp.sum(values, axis=0, keepdims=True)


def row(table, at, size):
    return table[at : at + 1, :size]


def same_crop(table, slot, length):
    ids = row(table, slot, length)
    marks = lax.broadcasted_iota(jnp.int32, (SMALL, length), 0).astype(HIGH) == ids
    marks = marks.astype(HIGH).astype(LOW)
    return left_trans(marks, marks) > 0.5


def copies_of(sources, targets, sems):
    copies = [pltpu.make_async_copy(a, b, sems.at[i]) for i, (a, b) in enumerate(zip(sources, targets))]
    for copy in copies:
        copy.start()
    return copies


def load_kernel(here, w_out, crops, *refs):
    count = (len(refs) - 5) // 2
    vectors, (piece, table), sems = refs[:count], refs[count : count + 2], refs[-1]
    held = refs[count + 2 : -1]
    size = piece.shape[0]
    start = pl.multiple_of((here[0] & 3) * size, size)
    sources = [w_out.at[pl.ds(start, size), :], crops, *vectors]
    copies = copies_of(sources, held, sems)
    copies[0].wait()
    piece[...] = held[0][...].astype(HIGH)
    for copy in copies[1:]:
        copy.wait()
    table[...] = jnp.zeros_like(table)
    at, width = 0, table.shape[1]
    for vector in held[2:]:
        for low in range(0, vector.shape[0], width):
            part = min(width, vector.shape[0] - low)
            table[at : at + 1, :part] = vector[low : low + part].reshape(1, part)
            at += 1
    seqs, length = held[1].shape
    table[at : at + seqs, :length] = held[1][...].astype(HIGH)


def front_kernel(*refs, length, seqs, crops):
    sources, count = refs[:5], 5 + seqs
    targets, held, kept, sems = refs[5 : 5 + count], refs[5 + count : 10 + count], refs[10 + count : -1], refs[-1]
    copies = copies_of(sources, held, sems)
    tokens, table, w_q, w_k, w_v = held
    first_out, q, k, v, lse, *outs = kept
    stores = [pltpu.make_async_copy(a, b, sems.at[5 + i]) for i, (a, b) in enumerate(zip(kept, targets))]
    copies[0].wait()
    unit, _ = unit_rows(tokens[...].astype(HIGH))
    copies[1].wait()
    local, width = w_q.shape[1], tokens.shape[1]
    first = (unit * row(table, GAIN_ATTN, width) + row(table, SHIFT_ATTN, width)).astype(LOW)
    first_out[...] = first
    stores[0].start()
    for copy in copies[2:]:
        copy.wait()
    q_all = plain_dot(first, w_q[...]) + row(table, BIAS_Q, local)
    q_all = (q_all.astype(LOW) * 0.125).astype(LOW)
    k_all = plain_dot(first, w_k[...]).astype(LOW)
    v_all = (plain_dot(first, w_v[...]) + row(table, BIAS_V, local)).astype(LOW)
    q[...] = q_all
    k[...] = k_all
    v[...] = v_all
    for store in stores[1:4]:
        store.start()
    low_half, masks = half_masks()
    for s, o in enumerate(outs):
        rows = slice(s * length, (s + 1) * length)
        same = same_crop(table, crops + s, length)
        for t in range(local // PAIR):
            at = slice(t * PAIR, (t + 1) * PAIR)
            q_pair, k_pair, v_pair = q_all[rows, at], k_all[rows, at], v_all[rows, at]
            got = []
            for half in range(2):
                scores = jnp.where(same, right_trans(q_pair * masks[half], k_pair), NEGATIVE)
                top = jnp.max(scores, axis=-1, keepdims=True)
                expo = jnp.exp(scores - top)
                total = jnp.sum(expo, axis=-1, keepdims=True)
                probs = (expo * (1.0 / total)).astype(LOW)
                got.append(plain_dot(probs, v_pair))
                h = 2 * t + half
                lse[rows, h : h + 1] = top + jnp.log(total)
            o[:, at] = jnp.where(low_half, got[0], got[1])
        stores[5 + s].start()
    stores[4].start()
    for store in stores:
        store.wait()


def relative_rows(here, width, count, bits):
    size = width // count
    place = lax.broadcasted_iota(jnp.int32, (width, 1), 0)
    block = ((place.astype(HIGH) + 0.5) * (1.0 / size)).astype(jnp.int32)
    mask = jnp.zeros_like(block)
    for p, bit in enumerate(bits):
        mask = mask + (((block >> (len(bits) - 1 - p)) & 1) << bit)
    source = (mask ^ here) * size + (place - block * size)
    marks = lax.broadcasted_iota(jnp.int32, (width, width), 1) == source
    return marks.astype(HIGH).astype(LOW)


def turn_kernel(here, *refs, count, orders):
    sources, held = refs[:4], (refs[-2], *refs[4:7])
    order_b, sums, sems = refs[7], refs[8], refs[-1]
    seqs = (len(refs) - 11) // 3
    a1_a, a1_b, cot_a = (refs[9 + i * seqs : 9 + (i + 1) * seqs] for i in range(3))
    first = refs[-2]
    length = first.shape[0] // seqs
    copies = copies_of(sources, held, sems)
    width = first.shape[1]
    order_a = relative_rows(here[0], width, count, orders[0])
    order = relative_rows(here[0], width, count, orders[1])
    order_b[...] = order
    copies[0].wait()
    for s in range(seqs):
        part = first[s * length : (s + 1) * length, :]
        a1_a[s][...] = right_trans(order_a, part).astype(LOW)
        a1_b[s][...] = right_trans(order, part).astype(LOW)
    for copy in copies[1:]:
        copy.wait()
    cot = held[1][...]
    for s in range(seqs):
        part = cot[s * length : (s + 1) * length, :]
        cot_a[s][...] = right_trans(order_a, part).astype(LOW)
    sums[...] = col_sum(cot.astype(HIGH))


def low_kernel(values, out):
    out[...] = values[...].astype(LOW)


def gather_kernel(here, *refs):
    for b, piece in enumerate(refs[:-1]):
        size = piece.shape[0]
        start = pl.multiple_of(((here[0] & 3) ^ b) * size, size)
        refs[-1][pl.ds(start, size), :] = piece[...].astype(LOW)


def middle_kernel(*refs, blocks, seq, length):
    tokens, o_own, o_other, w_out, w_low, table, w_up, w_down, cotangent, order = refs[:10]
    hidden, a2_t, active, g_pre, g_second, g_bias = refs[-6:]
    rows = slice(seq * length, (seq + 1) * length)
    attn = plain_dot(o_own[...].astype(LOW), w_out[...])
    attn = attn + plain_dot(o_other[...].astype(LOW), w_low[...])
    width = tokens.shape[1]
    values = tokens[rows, :].astype(HIGH) + (attn + row(table, BIAS_OUT, width))
    hidden[...] = values
    unit, _ = unit_rows(values)
    second = (unit * row(table, GAIN_MLP, width) + row(table, SHIFT_MLP, width)).astype(LOW)
    cot = cotangent[rows, :]
    size = w_up.shape[1] // blocks
    total = None
    for b in range(blocks):
        at = slice(b * size, (b + 1) * size)
        low = b * size % width
        at_row = BIAS_UP + b * size // width
        bias_up = table[at_row : at_row + 1, low : low + size]
        pre = plain_dot(second, w_up[:, at]) + bias_up
        cdf = 0.5 * (1.0 + lax.erf(pre * 0.7071067811865476))
        active[:, at] = (pre * cdf).astype(LOW)
        slope = cdf + pre * (0.3989422804014327 * jnp.exp(-0.5 * (pre * pre)))
        grad = (right_trans(cot, w_down[at, :]) * slope).astype(LOW)
        g_pre[:, at] = grad
        bias = col_sum(grad.astype(HIGH))
        g_bias[:, at] = refs[10][:, at] + bias if seq else bias
        part = right_trans(grad, w_up[:, at])
        total = part if total is None else total + part
    g_second[...] = total
    a2_t[...] = right_trans(order[...], second).astype(LOW)


def back_kernel(*refs, seq, length, crops):
    tokens, table, cotangent, hidden, own, other, order = refs[:7]
    w_out, w_q, w_k, w_v, q, k, v, lse = refs[7:15]
    before = refs[15:17]
    g_hidden, gh_t, g_qk, g_val, sums, g_first = refs[17:]
    width, local = tokens.shape[1], q.shape[1]
    rows = slice(seq * length, (seq + 1) * length)
    full = slice(0, width)
    if seq:
        sums_before, first_before = before
        g_first[: seq * length, :] = first_before[...]
        sums[6:, :] = sums_before[6:, :]
    else:
        g_bias, cot_sum = before
        sums[6:7, :] = g_bias[:, :width]
        sums[7:8, :] = g_bias[:, width:]
        sums[8:9, :] = cot_sum[...]
        sums[9:, :] = jnp.zeros_like(sums[9:, :])

    def put(r, at, value):
        sums[r : r + 1, at] = sums_before[r : r + 1, at] + value if seq else value

    unit, scale = unit_rows(hidden[...])
    grad = own[...] + other[...]
    put(0, full, col_sum(grad * unit))
    put(1, full, col_sum(grad))
    values = norm_back(grad * row(table, GAIN_MLP, width), unit, scale)
    values = cotangent[rows, :].astype(HIGH) + values
    g_hidden[...] = values
    put(2, full, col_sum(values))
    low = values.astype(LOW)
    gh_t[...] = right_trans(order[...], low).astype(LOW)
    g_o = right_trans(low, w_out[...]).astype(LOW)
    same = same_crop(table, crops + seq, length)
    low_half, masks = half_masks()
    for t in range(local // PAIR):
        at = slice(t * PAIR, (t + 1) * PAIR)
        q_pair, k_pair, v_pair, o_pair = q[rows, at], k[rows, at], v[rows, at], g_o[:, at]
        got = []
        for half in range(2):
            h = 2 * t + half
            scores = right_trans(q_pair * masks[half], k_pair)
            probs = jnp.exp(jnp.where(same, scores, NEGATIVE) - lse[rows, h : h + 1])
            g_probs = right_trans(o_pair * masks[half], v_pair)
            inner = jnp.sum(g_probs * probs, axis=-1, keepdims=True)
            g_scores = (probs * (g_probs - inner)).astype(LOW)
            got.append(
                (
                    plain_dot(g_scores, k_pair),
                    left_trans(g_scores, q_pair),
                    left_trans(probs.astype(LOW), o_pair),
                )
            )
        g_q = (jnp.where(low_half, got[0][0], got[1][0]) * 0.125).astype(LOW)
        g_k = jnp.where(low_half, got[0][1], got[1][1]).astype(LOW)
        g_v = jnp.where(low_half, got[0][2], got[1][2]).astype(LOW)
        beside = slice(local + t * PAIR, local + (t + 1) * PAIR)
        g_qk[:, at] = g_q
        g_qk[:, beside] = g_k
        g_val[:, at] = g_v
        put(5, at, col_sum(g_q.astype(HIGH)))
        put(5, beside, col_sum(g_v.astype(HIGH)))
    part = right_trans(g_qk[:, :local], w_q[...])
    part = part + right_trans(g_qk[:, local:], w_k[...])
    part = part + right_trans(g_val[...], w_v[...])
    g_first[rows, :] = part
    unit_one, _ = unit_rows(tokens[rows, :].astype(HIGH))
    put(3, full, col_sum(part * unit_one))
    put(4, full, col_sum(part))


def base_kernel(table, tokens, own, *refs, length):
    g_hidden, (base, unit_out, scale_out) = refs[:-3], refs[-3:]
    gain = row(table, GAIN_ATTN, tokens.shape[1])
    for s in range(tokens.shape[0] // length):
        rows = slice(s * length, (s + 1) * length)
        part = own[rows, :]
        unit, scale = unit_rows(tokens[rows, :].astype(HIGH))
        base[rows, :] = g_hidden[s][...] + norm_back(part * gain, unit, scale)
        unit_out[rows, :] = unit
        scale_out[rows, :] = scale


def last_kernel(table, base, unit, scale, other, g_tokens, *, length):
    gain = row(table, GAIN_ATTN, base.shape[1])
    for s in range(base.shape[0] // length):
        rows = slice(s * length, (s + 1) * length)
        grad = norm_back(other[rows, :] * gain, unit[rows, :], scale[rows, :])
        g_tokens[rows, :] = base[rows, :] + grad


def out_kernel(*refs, seqs, length):
    table, own, other = refs[:3]
    for s in range(seqs):
        rows = slice(s * length, (s + 1) * length)
        total = refs[3 + s][...] + (own[rows, :] + other[rows, :])
        refs[3 + seqs][rows, :] = (total + row(table, BIAS_DOWN, total.shape[1])).astype(LOW)


def mlp_kernel(w_down, *refs):
    length = refs[0].shape[0]
    for s, active in enumerate(refs[:-1]):
        refs[-1][s * length : (s + 1) * length, :] = plain_dot(active[...], w_down[...])


def products(plan, refs, at):
    for lefts, rights, column in plan:
        wide = refs[rights[0]].shape[1]
        step = min(512, wide)
        for n in range(0, wide, step):
            value = None
            for left, right in zip(lefts, rights):
                part = plain_dot(refs[left][at, :], refs[right][:, n : n + step].astype(LOW))
                value = part if value is None else value + part
            yield slice(column + n, column + n + step), value


def far_kernel(*refs, plan, start, pieces, small):
    outs = refs[-pieces:]
    size = start // pieces
    for o, out in enumerate(outs):
        at = slice(start + o * size, start + (o + 1) * size)
        for columns, value in products(plan, refs, at):
            out[:size, columns] = value
    if small:
        outs[0][size:, :] = refs[-pieces - 1][...]


def part_kernel(*refs, plan, start, added):
    out = refs[-1]
    at = slice(start, start + out.shape[0])
    for columns, value in products(plan, refs, at):
        out[:, columns] = value + refs[-2][:, columns] if added else value


def near_kernel(*refs, plan, pieces, small):
    outs, got = refs[-2:], refs[-2 - pieces - small :]
    half = outs[0].shape[0]
    for o, out in enumerate(outs):
        at = slice(o * half, (o + 1) * half)
        size = 2 * half // pieces
        low = o * half % size
        for columns, value in products(plan, refs, at):
            out[:half, columns] = value + got[o * half // size][low : low + half, columns]
    if small:
        outs[1][half:, :] = got[pieces][...] + got[0][2 * half // pieces :, :]


def step_kernel(*refs, small, joined):
    count = 2 if joined else 1
    keeps, sents, gots = (refs[i * count : (i + 1) * count] for i in range(3))
    outs = refs[3 * count :]
    at = 0
    for i in range(count):
        half = outs[i].shape[0]
        got = gots[i]
        outs[i][...] = keeps[i][:half, :] + got[:half, :]
        outs[count][at : at + half, :] = keeps[i][half:, :] + got[half : 2 * half, :]
        at += half
        if small and not i:
            outs[count][at : at + SMALL, :] = sents[i][2 * half :, :] + got[2 * half :, :]
            at += SMALL


def end_kernel(*refs, wide):
    count = (len(refs) - 1) // (1 + wide)
    keeps, got, outs = refs[:count], refs[count], refs[count + 1 :]
    at = o = 0
    for keep in keeps:
        size, each = keep.shape[0], keep.shape[1] // wide
        for w in range(wide):
            columns = slice(w * each, (w + 1) * each)
            outs[o][...] = keep[:, columns] + got[at : at + size, columns]
            o += 1
        at += size


def vector_kernel(here, sent, got, *outs, size):
    total = sent[size : size + SMALL, :] + got[size : size + SMALL, :]
    bias_q, bias_v, bias_up, gain_mlp, shift_mlp, bias_out, bias_down, gains = outs
    width, each = total.shape[1], bias_q.shape[0]
    bias_q[...] = total[5, :each]
    bias_v[...] = total[5, each:]
    for i in range(bias_up.shape[0] // width):
        bias_up[i * width : (i + 1) * width] = total[6 + i, :]
    turned = pltpu.roll(total, lax.rem(width - here[0] * size, width), 1)
    for out, at in ((gain_mlp, 0), (shift_mlp, 1), (bias_out, 2), (bias_down, 8)):
        out[...] = turned[at, :size]
    gains[...] = turned[:8, : gains.shape[1]]


def gain_kernel(own, other, gain, shift):
    total = own[...] + other[...]
    gain[...] = total[3, : gain.shape[0]]
    shift[...] = total[4, : shift.shape[0]]


class Steps:
    def __init__(self):
        self.last = None

    def __call__(
        self, kernel, name, outs, args, scratch=(), limit=12, smem=0, whole=(), tie=0, alias=None, cost=0, out_whole=False
    ):
        args = list(args)
        if self.last is not None:
            args[tie], _ = lax.optimization_barrier((args[tie], self.last))
        result = pl.pallas_call(
            kernel,
            name=name,
            out_shape=[jax.ShapeDtypeStruct(s, d) for s, d in outs],
            in_specs=[pl.BlockSpec(memory_space=pltpu.SMEM)] * smem
            + [pl.BlockSpec(memory_space=pl.ANY) if i in whole else VMEM for i in range(smem, len(args))]
            if whole
            else [pl.BlockSpec(memory_space=pltpu.SMEM)] * smem + [VMEM] * (len(args) - smem),
            out_specs=[pl.BlockSpec(memory_space=pl.ANY) if out_whole else VMEM] * len(outs),
            scratch_shapes=list(scratch),
            input_output_aliases=alias or {},
            compiler_params=pltpu.CompilerParams(vmem_limit_bytes=limit << 20),
            cost_estimate=pl.CostEstimate(flops=1000 + cost, bytes_accessed=1000, transcendentals=0),
        )(*args)
        self.last = result[0]
        return result


def send(values, bit, count):
    return lax.ppermute(values, "dp", [(i, i ^ (1 << bit)) for i in range(count)])


def swap(values):
    return lax.ppermute(values, "mp", [(0, 1), (1, 0)])


class Scatter:
    def __init__(self, steps, count, bits, plan, pieces=2, wide=1, small=None):
        self.steps, self.count, self.bits = steps, count, bits
        self.pieces, self.wide, self.small = pieces, wide, small
        self.plan, self.arrays, self.columns = [], [], 0
        for lefts, rights in plan:
            at, each = len(self.arrays), len(lefts)
            self.arrays += lefts + rights
            places = list(range(at, at + each)), list(range(at + each, at + 2 * each))
            self.plan.append((*places, self.columns))
            self.columns += rights[0].shape[1]
        self.rows = plan[0][0][0].shape[0] // 2
        self.extra = SMALL if small is not None else 0
        self.at = 1

    def shapes(self, *sizes):
        return [((n, self.columns), HIGH) for n in sizes]

    def far(self):
        size = self.rows // self.pieces
        kernel = partial(
            far_kernel,
            plan=self.plan,
            start=self.rows,
            pieces=self.pieces,
            small=bool(self.extra),
        )
        held = self.arrays + ([self.small] if self.extra else [])
        outs = self.shapes(size + self.extra, *[size] * (self.pieces - 1))
        outs = self.steps(kernel, "far", outs, held)
        self.got = [send(o, self.bits[0], self.count) for o in outs]

    def near(self):
        kernel = partial(
            near_kernel,
            plan=self.plan,
            pieces=self.pieces,
            small=bool(self.extra),
        )
        held = self.arrays + self.got + ([self.small] if self.extra else [])
        self.rows //= 2
        outs = self.shapes(self.rows, self.rows + self.extra)
        self.keep, self.sent = self.steps(kernel, "near", outs, held)
        self.got = send(self.sent, self.bits[1], self.count)

    def part(self, start, added):
        kernel = partial(part_kernel, plan=self.plan, start=start * self.rows // 2, added=len(added))
        outs = self.shapes(self.rows // 2)
        return self.steps(kernel, "part", outs, self.arrays + added)[0]

    def far_part(self, sent):
        return send(self.part(2 + sent, []), self.bits[0], self.count)

    def near_sent(self, got):
        self.sent = self.part(1, [got])
        self.got = send(self.sent, self.bits[1], self.count)

    def near_keep(self, got):
        self.keep = self.part(0, [got])
        self.rows //= 2

    def rest(self):
        while self.at + 1 < len(self.bits):
            self.step()

    def step(self):
        self.at += 1
        self.rows //= 2
        outs = self.shapes(self.rows, self.rows + self.extra)
        kernel = partial(step_kernel, small=bool(self.extra), joined=False)
        self.keep, self.sent = self.steps(kernel, "sum", outs, [self.keep, self.sent, self.got])
        self.got = send(self.sent, self.bits[self.at], self.count)


def join(one, two):
    for part in (one, two):
        part.at += 1
        part.rows //= 2
    outs = one.shapes(one.rows) + two.shapes(two.rows) + one.shapes(one.rows + two.rows + one.extra)
    kernel = partial(step_kernel, small=bool(one.extra), joined=True)
    held = [one.keep, two.keep, one.sent, two.sent, one.got, two.got]
    one.keep, two.keep, sent = one.steps(kernel, "sums", outs, held)
    got = send(sent, one.bits[one.at], one.count)
    while one.at + 1 < len(one.bits):
        one.at += 1
        half = one.rows // 2
        starts = (0, one.rows + one.extra)
        keeps, sents = [], []
        for part, start in zip((one, two), starts):
            total = part.keep + got[start : start + part.rows]
            keeps.append(total[:half])
            sents.append(total[half:])
        if one.extra:
            at = slice(one.rows, one.rows + one.extra)
            sents.insert(1, sent[at] + got[at])
        one.keep, two.keep = keeps
        one.rows = two.rows = half
        sent = jnp.concatenate(sents)
        got = send(sent, one.bits[one.at], one.count)
    return sent, got


def finish(parts, got, cost=0):
    outs = []
    for part in parts:
        outs += [((part.rows, part.columns // part.wide), HIGH)] * part.wide
    kernel = partial(end_kernel, wide=parts[0].wide)
    held = [part.keep for part in parts] + [got]
    return parts[0].steps(kernel, "end", outs, held, cost=cost)


def body(
    tokens,
    crop_ids,
    w_query,
    w_key,
    w_value,
    bias_query,
    bias_value,
    w_out,
    bias_out,
    gain_attn,
    shift_attn,
    gain_mlp,
    shift_mlp,
    w_up,
    bias_up,
    w_down,
    bias_down,
    cotangent,
    count,
):
    width = tokens.shape[1]
    local = w_query.shape[1]
    hidden_units = w_up.shape[1]
    seqs, length = crop_ids.shape
    rows = seqs * length
    here = lax.axis_index("dp")
    scalar = here.reshape(1)
    bits = list(range(count.bit_length() - 1))
    orders = (bits, [0, 2, 1] + bits[3:])
    steps = Steps()
    piece = local // 4
    lines = [gain_attn, shift_attn, bias_query, bias_value, bias_out, gain_mlp, shift_mlp]
    lines += [bias_down, bias_up]
    crops = BIAS_UP + hidden_units // width
    held = [((piece, width), LOW), (crop_ids.shape, jnp.int32)] + [(v.shape, HIGH) for v in lines]
    mine, table = steps(
        load_kernel,
        "load",
        [((piece, width), HIGH), ((crops + seqs, width), HIGH)],
        [scalar, w_out, crop_ids] + lines,
        scratch=[pltpu.VMEM(*h) for h in held] + [pltpu.SemaphoreType.DMA((len(held),))],
        smem=1,
        whole=range(1, 3 + len(lines)),
        limit=63,
    )
    got = swap(mine)

    def like(*arrays):
        return [(a.shape, a.dtype) for a in arrays]

    loaded = [tokens, table, w_query, w_key, w_value]
    made = [((rows, width), LOW)] + [((rows, local), LOW)] * 3
    made += [((rows, 128), HIGH)] + [((length, local), HIGH)] * seqs
    first, query, key_rows, value_rows, log_total, *mixed = steps(
        partial(front_kernel, length=length, seqs=seqs, crops=crops),
        "front",
        made,
        loaded,
        scratch=[pltpu.VMEM(*v) for v in like(*loaded) + made]
        + [pltpu.SemaphoreType.DMA((len(loaded) + len(made),))],
        whole=range(5),
        out_whole=True,
        tie=1,
        limit=58,
    )
    mixed_other = [swap(o) for o in mixed]

    got, _ = lax.optimization_barrier((got, first))
    beside = send(got, 1, count)
    pieces = [got, send(got, 0, count), beside]
    turned = steps(
        partial(turn_kernel, count=count, orders=orders),
        "turn",
        like(cotangent, w_up, w_out)
        + [((width, width), LOW), ((1, width), HIGH)]
        + [((width, length), LOW)] * (3 * seqs),
        [scalar, first, cotangent, w_up, w_out],
        scratch=[pltpu.VMEM((rows, width), LOW), pltpu.SemaphoreType.DMA((4,))],
        whole=range(1, 5),
        smem=1,
        tie=1,
        limit=44,
    )

    cotangent, w_up, w_out, order_b, cot_sum = turned[:5]
    a1_a, a1_b, cot_a = (list(turned[5 + i * seqs : 5 + (i + 1) * seqs]) for i in range(3))
    beside, _ = lax.optimization_barrier((beside, order_b))
    pieces.append(send(beside, 0, count))
    mixed_other[0] = steps(low_kernel, "low", [((length, local), LOW)], [mixed_other[0]], cost=31 * 10**8)[0]
    w_low = steps(
        gather_kernel, "gather", [((local, width), LOW)], [scalar] + pieces, smem=1, tie=1
    )[0]
    hidden, a2_b, active, g_pre, second, carried = [], [], [], [], [], []
    for s in range(seqs):
        result = steps(
            partial(middle_kernel, blocks=4, seq=s, length=length),
            "middle",
            [
                ((length, width), HIGH),
                ((width, length), LOW),
                ((length, hidden_units), LOW),
                ((length, hidden_units), LOW),
                ((length, width), HIGH),
                ((1, hidden_units), HIGH),
            ],
            [
                tokens,
                mixed[s],
                mixed_other[s],
                w_out,
                w_low,
                table,
                w_up,
                w_down,
                cotangent,
                order_b,
            ]
            + carried,
            tie=1,
        )
        for held, value in zip((hidden, a2_b, active, g_pre, second), result):
            held.append(value)
        carried = list(result[5:])
    bias_sum = carried[0]
    second_other = [swap(g) for g in second]

    down = Scatter(steps, count, orders[0], [(cot_a, active)])
    up = Scatter(steps, count, orders[1], [(a2_b, g_pre)])
    parts = [one.far_part(sent) for sent in (1, 0) for one in (down, up)]
    down.near_sent(parts[0])
    up.near_sent(parts[1])
    mlp_part = steps(mlp_kernel, "mlp", [((rows, width), HIGH)], [w_down] + active, tie=1)[0]
    mlp_other = swap(mlp_part)
    down.near_keep(parts[2])
    up.near_keep(parts[3])
    g_hidden, gh_b, g_qk, g_val, carried = [], [], [], [], [bias_sum, cot_sum]
    for s in range(seqs):
        if s == seqs - 1:
            down.step()
            up.step()
        result = steps(
            partial(back_kernel, seq=s, length=length, crops=crops),
            "back",
            [
                ((length, width), HIGH),
                ((width, length), LOW),
                ((length, 2 * local), LOW),
                ((length, local), LOW),
                ((SMALL, width), HIGH),
                (((s + 1) * length, width), HIGH),
            ],
            [tokens, table, cotangent, hidden[s], second[s], second_other[s], order_b]
            + [w_out, w_query, w_key, w_value, query, key_rows, value_rows, log_total]
            + carried,
            tie=4,
            cost=0 if s else 6 * 10**9,
        )
        for held, value in zip((g_hidden, gh_b, g_qk, g_val), result):
            held.append(value)
        carried = list(result[4:])
    sums, g_first = carried
    first_other = swap(g_first)
    heads = Scatter(steps, count, orders[0], [(a1_a, g_qk)], wide=2, small=sums)
    others = Scatter(steps, count, orders[1], [(a1_b, g_val), (gh_b, mixed)], wide=2)
    heads.far()
    others.far()
    _, mlp_got = join(down, up)
    heads.near()
    others.near()
    block_out = steps(
        partial(out_kernel, seqs=seqs, length=length),
        "out",
        [((rows, width), LOW)],
        [table, mlp_part, mlp_other] + hidden,
        tie=1,
        cost=3 * 10**9,
    )[0]
    heads.step()
    others.step()
    w_down_t, done_w_up = finish([down, up], mlp_got, 15 * 10**8)
    heads.rest()
    others.rest()
    base, unit, scale = steps(
        partial(base_kernel, length=length),
        "base",
        [((rows, width), HIGH)] * 2 + [((rows, 1), HIGH)],
        [table, tokens, g_first] + g_hidden,
        tie=2,
    )
    size = width // count
    (
        done_bias_q,
        done_bias_v,
        done_bias_up,
        done_gain_mlp,
        done_shift_mlp,
        done_bias_out,
        done_bias_down,
        gains,
    ) = steps(
        partial(vector_kernel, size=size),
        "vectors",
        [((local,), HIGH)] * 2
        + [((hidden_units,), HIGH)]
        + [((size,), HIGH)] * 4
        + [((8, 128), HIGH)],
        [scalar, heads.sent, heads.got],
        smem=1,
        tie=1,
    )
    gains_other = swap(gains)
    grad_w_q, grad_w_k = finish([heads], heads.got)
    grad_w_v, w_out_t = finish([others], others.got)
    grad_tokens = steps(
        partial(last_kernel, length=length),
        "last",
        [((rows, width), HIGH)],
        [table, base, unit, scale, first_other],
        tie=1,
    )[0]
    done_gain_attn, done_shift_attn = steps(
        gain_kernel, "gains", [((size,), HIGH)] * 2, [gains, gains_other]
    )
    return (
        block_out,
        grad_tokens,
        grad_w_q,
        grad_w_k,
        grad_w_v,
        done_bias_q,
        done_bias_v,
        w_out_t.T,
        done_bias_out,
        done_gain_attn,
        done_shift_attn,
        done_gain_mlp,
        done_shift_mlp,
        done_w_up,
        done_bias_up,
        w_down_t.T,
        done_bias_down,
    )


def solution(mesh):
    placed = (
        P("dp", None),
        P("dp", None),
        P(None, "mp"),
        P(None, "mp"),
        P(None, "mp"),
        P("mp"),
        P("mp"),
        P("mp", None),
        P(),
        P(),
        P(),
        P(),
        P(),
        P(None, "mp"),
        P("mp"),
        P("mp", None),
        P(),
        P("dp", None),
    )
    return jax.shard_map(
        partial(body, count=mesh.shape["dp"]),
        mesh=mesh,
        in_specs=placed,
        out_specs=(
            P("dp", None),
            P("dp", None),
            P("dp", "mp"),
            P("dp", "mp"),
            P("dp", "mp"),
            P("mp"),
            P("mp"),
            P("mp", "dp"),
            P("dp"),
            P("dp"),
            P("dp"),
            P("dp"),
            P("dp"),
            P("dp", "mp"),
            P("mp"),
            P("mp", "dp"),
            P("dp"),
        ),
        check_vma=False,
    )
```

```python
from functools import partial

import jax
import jax.numpy as jnp
from jax import lax
from jax.experimental import pallas as pl
from jax.experimental.pallas import tpu as pltpu
from jax.sharding import PartitionSpec as P

HEAD_DIM = 64
PAIR = 2 * HEAD_DIM
EPS = 1e-06
NEGATIVE = -1e30
LOW = jnp.bfloat16
HIGH = jnp.float32
VMEM = pl.BlockSpec(memory_space=pltpu.VMEM)
SMALL = 16
GAIN_ATTN, SHIFT_ATTN, BIAS_Q, BIAS_V, BIAS_OUT, GAIN_MLP, SHIFT_MLP, BIAS_DOWN, BIAS_UP = range(9)


def plain_dot(left, right):
    return jnp.dot(left, right, preferred_element_type=HIGH)


def right_trans(left, right):
    return lax.dot_general(left, right, (((1,), (1,)), ((), ())), preferred_element_type=HIGH)


def left_trans(left, right):
    return lax.dot_general(left, right, (((0,), (0,)), ((), ())), preferred_element_type=HIGH)


def unit_rows(values):
    mean = jnp.mean(values, axis=-1, keepdims=True)
    centred = values - mean
    scale = lax.rsqrt(jnp.mean(centred * centred, axis=-1, keepdims=True) + EPS)
    return centred * scale, scale


def norm_back(grad_unit, unit, scale):
    inner = jnp.mean(grad_unit * unit, axis=-1, keepdims=True)
    return scale * (grad_unit - jnp.mean(grad_unit, axis=-1, keepdims=True) - unit * inner)


def half_masks():
    lane = lax.broadcasted_iota(jnp.int32, (1, PAIR), 1)
    first = lane < HEAD_DIM
    return first, (first.astype(HIGH).astype(LOW), (~first).astype(HIGH).astype(LOW))


def col_sum(values):
    return jnp.sum(values, axis=0, keepdims=True)


def row(table, at, size):
    return table[at : at + 1, :size]


def same_crop(table, slot, length):
    ids = row(table, slot, length)
    marks = lax.broadcasted_iota(jnp.int32, (SMALL, length), 0).astype(HIGH) == ids
    marks = marks.astype(HIGH).astype(LOW)
    return left_trans(marks, marks) > 0.5


def copies_of(sources, targets, sems):
    copies = [pltpu.make_async_copy(a, b, sems.at[i]) for i, (a, b) in enumerate(zip(sources, targets))]
    for copy in copies:
        copy.start()
    return copies


def load_kernel(here, w_out, crops, *refs):
    count = (len(refs) - 5) // 2
    vectors, (piece, table), sems = refs[:count], refs[count : count + 2], refs[-1]
    held = refs[count + 2 : -1]
    size = piece.shape[0]
    start = pl.multiple_of((here[0] & 3) * size, size)
    sources = [w_out.at[pl.ds(start, size), :], crops, *vectors]
    copies = copies_of(sources, held, sems)
    copies[0].wait()
    piece[...] = held[0][...].astype(HIGH)
    for copy in copies[1:]:
        copy.wait()
    table[...] = jnp.zeros_like(table)
    at, width = 0, table.shape[1]
    for vector in held[2:]:
        for low in range(0, vector.shape[0], width):
            part = min(width, vector.shape[0] - low)
            table[at : at + 1, :part] = vector[low : low + part].reshape(1, part)
            at += 1
    seqs, length = held[1].shape
    table[at : at + seqs, :length] = held[1][...].astype(HIGH)


def front_kernel(*refs, length, seqs, crops):
    sources, count = refs[:5], 5 + seqs
    targets, held, kept, sems = refs[5 : 5 + count], refs[5 + count : 10 + count], refs[10 + count : -1], refs[-1]
    copies = copies_of(sources, held, sems)
    tokens, table, w_q, w_k, w_v = held
    first_out, q, k, v, lse, *outs = kept
    stores = [pltpu.make_async_copy(a, b, sems.at[5 + i]) for i, (a, b) in enumerate(zip(kept, targets))]
    copies[0].wait()
    unit, _ = unit_rows(tokens[...].astype(HIGH))
    copies[1].wait()
    local, width = w_q.shape[1], tokens.shape[1]
    first = (unit * row(table, GAIN_ATTN, width) + row(table, SHIFT_ATTN, width)).astype(LOW)
    first_out[...] = first
    stores[0].start()
    for copy in copies[2:]:
        copy.wait()
    q_all = plain_dot(first, w_q[...]) + row(table, BIAS_Q, local)
    q_all = (q_all.astype(LOW) * 0.125).astype(LOW)
    k_all = plain_dot(first, w_k[...]).astype(LOW)
    v_all = (plain_dot(first, w_v[...]) + row(table, BIAS_V, local)).astype(LOW)
    q[...] = q_all
    k[...] = k_all
    v[...] = v_all
    for store in stores[1:4]:
        store.start()
    low_half, masks = half_masks()
    for s, o in enumerate(outs):
        rows = slice(s * length, (s + 1) * length)
        same = same_crop(table, crops + s, length)
        for t in range(local // PAIR):
            at = slice(t * PAIR, (t + 1) * PAIR)
            q_pair, k_pair, v_pair = q_all[rows, at], k_all[rows, at], v_all[rows, at]
            got = []
            for half in range(2):
                scores = jnp.where(same, right_trans(q_pair * masks[half], k_pair), NEGATIVE)
                top = jnp.max(scores, axis=-1, keepdims=True)
                expo = jnp.exp(scores - top)
                total = jnp.sum(expo, axis=-1, keepdims=True)
                probs = (expo * (1.0 / total)).astype(LOW)
                got.append(plain_dot(probs, v_pair))
                h = 2 * t + half
                lse[rows, h : h + 1] = top + jnp.log(total)
            o[:, at] = jnp.where(low_half, got[0], got[1])
        stores[5 + s].start()
    stores[4].start()
    for store in stores:
        store.wait()


def relative_rows(here, width, count, bits):
    size = width // count
    place = lax.broadcasted_iota(jnp.int32, (width, 1), 0)
    block = ((place.astype(HIGH) + 0.5) * (1.0 / size)).astype(jnp.int32)
    mask = jnp.zeros_like(block)
    for p, bit in enumerate(bits):
        mask = mask + (((block >> (len(bits) - 1 - p)) & 1) << bit)
    source = (mask ^ here) * size + (place - block * size)
    marks = lax.broadcasted_iota(jnp.int32, (width, width), 1) == source
    return marks.astype(HIGH).astype(LOW)


def turn_kernel(here, *refs, count, orders):
    sources, held = refs[:4], (refs[-2], *refs[4:7])
    order_b, sums, sems = refs[7], refs[8], refs[-1]
    seqs = (len(refs) - 11) // 3
    a1_a, a1_b, cot_a = (refs[9 + i * seqs : 9 + (i + 1) * seqs] for i in range(3))
    first = refs[-2]
    length = first.shape[0] // seqs
    copies = copies_of(sources, held, sems)
    width = first.shape[1]
    order_a = relative_rows(here[0], width, count, orders[0])
    order = relative_rows(here[0], width, count, orders[1])
    order_b[...] = order
    copies[0].wait()
    for s in range(seqs):
        part = first[s * length : (s + 1) * length, :]
        a1_a[s][...] = right_trans(order_a, part).astype(LOW)
        a1_b[s][...] = right_trans(order, part).astype(LOW)
    for copy in copies[1:]:
        copy.wait()
    cot = held[1][...]
    for s in range(seqs):
        part = cot[s * length : (s + 1) * length, :]
        cot_a[s][...] = right_trans(order_a, part).astype(LOW)
    sums[...] = col_sum(cot.astype(HIGH))


def low_kernel(values, out):
    out[...] = values[...].astype(LOW)


def gather_kernel(here, *refs):
    for b, piece in enumerate(refs[:-1]):
        size = piece.shape[0]
        start = pl.multiple_of(((here[0] & 3) ^ b) * size, size)
        refs[-1][pl.ds(start, size), :] = piece[...].astype(LOW)


def middle_kernel(*refs, blocks, seq, length):
    tokens, o_own, o_other, w_out, w_low, table, w_up, w_down, cotangent, order = refs[:10]
    hidden, a2_t, active, g_pre, g_second, g_bias = refs[-6:]
    rows = slice(seq * length, (seq + 1) * length)
    attn = plain_dot(o_own[...].astype(LOW), w_out[...])
    attn = attn + plain_dot(o_other[...].astype(LOW), w_low[...])
    width = tokens.shape[1]
    values = tokens[rows, :].astype(HIGH) + (attn + row(table, BIAS_OUT, width))
    hidden[...] = values
    unit, _ = unit_rows(values)
    second = (unit * row(table, GAIN_MLP, width) + row(table, SHIFT_MLP, width)).astype(LOW)
    cot = cotangent[rows, :]
    size = w_up.shape[1] // blocks
    total = None
    for b in range(blocks):
        at = slice(b * size, (b + 1) * size)
        low = b * size % width
        at_row = BIAS_UP + b * size // width
        bias_up = table[at_row : at_row + 1, low : low + size]
        pre = plain_dot(second, w_up[:, at]) + bias_up
        cdf = 0.5 * (1.0 + lax.erf(pre * 0.7071067811865476))
        active[:, at] = (pre * cdf).astype(LOW)
        slope = cdf + pre * (0.3989422804014327 * jnp.exp(-0.5 * (pre * pre)))
        grad = (right_trans(cot, w_down[at, :]) * slope).astype(LOW)
        g_pre[:, at] = grad
        bias = col_sum(grad.astype(HIGH))
        g_bias[:, at] = refs[10][:, at] + bias if seq else bias
        part = right_trans(grad, w_up[:, at])
        total = part if total is None else total + part
    g_second[...] = total
    a2_t[...] = right_trans(order[...], second).astype(LOW)


def back_kernel(*refs, seq, length, crops):
    tokens, table, cotangent, hidden, own, other, order = refs[:7]
    w_out, w_q, w_k, w_v, q, k, v, lse = refs[7:15]
    before = refs[15:17]
    g_hidden, gh_t, g_qk, g_val, sums, g_first = refs[17:]
    width, local = tokens.shape[1], q.shape[1]
    rows = slice(seq * length, (seq + 1) * length)
    full = slice(0, width)
    if seq:
        sums_before, first_before = before
        g_first[: seq * length, :] = first_before[...]
        sums[6:, :] = sums_before[6:, :]
    else:
        g_bias, cot_sum = before
        sums[6:7, :] = g_bias[:, :width]
        sums[7:8, :] = g_bias[:, width:]
        sums[8:9, :] = cot_sum[...]
        sums[9:, :] = jnp.zeros_like(sums[9:, :])

    def put(r, at, value):
        sums[r : r + 1, at] = sums_before[r : r + 1, at] + value if seq else value

    unit, scale = unit_rows(hidden[...])
    grad = own[...] + other[...]
    put(0, full, col_sum(grad * unit))
    put(1, full, col_sum(grad))
    values = norm_back(grad * row(table, GAIN_MLP, width), unit, scale)
    values = cotangent[rows, :].astype(HIGH) + values
    g_hidden[...] = values
    put(2, full, col_sum(values))
    low = values.astype(LOW)
    gh_t[...] = right_trans(order[...], low).astype(LOW)
    g_o = right_trans(low, w_out[...]).astype(LOW)
    same = same_crop(table, crops + seq, length)
    low_half, masks = half_masks()
    for t in range(local // PAIR):
        at = slice(t * PAIR, (t + 1) * PAIR)
        q_pair, k_pair, v_pair, o_pair = q[rows, at], k[rows, at], v[rows, at], g_o[:, at]
        got = []
        for half in range(2):
            h = 2 * t + half
            scores = right_trans(q_pair * masks[half], k_pair)
            probs = jnp.exp(jnp.where(same, scores, NEGATIVE) - lse[rows, h : h + 1])
            g_probs = right_trans(o_pair * masks[half], v_pair)
            inner = jnp.sum(g_probs * probs, axis=-1, keepdims=True)
            g_scores = (probs * (g_probs - inner)).astype(LOW)
            got.append(
                (
                    plain_dot(g_scores, k_pair),
                    left_trans(g_scores, q_pair),
                    left_trans(probs.astype(LOW), o_pair),
                )
            )
        g_q = (jnp.where(low_half, got[0][0], got[1][0]) * 0.125).astype(LOW)
        g_k = jnp.where(low_half, got[0][1], got[1][1]).astype(LOW)
        g_v = jnp.where(low_half, got[0][2], got[1][2]).astype(LOW)
        beside = slice(local + t * PAIR, local + (t + 1) * PAIR)
        g_qk[:, at] = g_q
        g_qk[:, beside] = g_k
        g_val[:, at] = g_v
        put(5, at, col_sum(g_q.astype(HIGH)))
        put(5, beside, col_sum(g_v.astype(HIGH)))
    part = right_trans(g_qk[:, :local], w_q[...])
    part = part + right_trans(g_qk[:, local:], w_k[...])
    part = part + right_trans(g_val[...], w_v[...])
    g_first[rows, :] = part
    unit_one, _ = unit_rows(tokens[rows, :].astype(HIGH))
    put(3, full, col_sum(part * unit_one))
    put(4, full, col_sum(part))


def base_kernel(table, tokens, own, *refs, length):
    g_hidden, (base, unit_out, scale_out) = refs[:-3], refs[-3:]
    gain = row(table, GAIN_ATTN, tokens.shape[1])
    for s in range(tokens.shape[0] // length):
        rows = slice(s * length, (s + 1) * length)
        part = own[rows, :]
        unit, scale = unit_rows(tokens[rows, :].astype(HIGH))
        base[rows, :] = g_hidden[s][...] + norm_back(part * gain, unit, scale)
        unit_out[rows, :] = unit
        scale_out[rows, :] = scale


def last_kernel(table, base, unit, scale, other, g_tokens, *, length):
    gain = row(table, GAIN_ATTN, base.shape[1])
    for s in range(base.shape[0] // length):
        rows = slice(s * length, (s + 1) * length)
        grad = norm_back(other[rows, :] * gain, unit[rows, :], scale[rows, :])
        g_tokens[rows, :] = base[rows, :] + grad


def out_kernel(*refs, seqs, length):
    table, own, other = refs[:3]
    for s in range(seqs):
        rows = slice(s * length, (s + 1) * length)
        total = refs[3 + s][...] + (own[rows, :] + other[rows, :])
        refs[3 + seqs][rows, :] = (total + row(table, BIAS_DOWN, total.shape[1])).astype(LOW)


def mlp_kernel(w_down, *refs):
    length = refs[0].shape[0]
    for s, active in enumerate(refs[:-1]):
        refs[-1][s * length : (s + 1) * length, :] = plain_dot(active[...], w_down[...])


def products(plan, refs, at):
    for lefts, rights, column in plan:
        wide = refs[rights[0]].shape[1]
        step = min(512, wide)
        for n in range(0, wide, step):
            value = None
            for left, right in zip(lefts, rights):
                part = plain_dot(refs[left][at, :], refs[right][:, n : n + step].astype(LOW))
                value = part if value is None else value + part
            yield slice(column + n, column + n + step), value


def far_kernel(*refs, plan, start, pieces, small):
    outs = refs[-pieces:]
    size = start // pieces
    for o, out in enumerate(outs):
        at = slice(start + o * size, start + (o + 1) * size)
        for columns, value in products(plan, refs, at):
            out[:size, columns] = value
    if small:
        outs[0][size:, :] = refs[-pieces - 1][...]


def part_kernel(*refs, plan, start, added):
    out = refs[-1]
    at = slice(start, start + out.shape[0])
    for columns, value in products(plan, refs, at):
        out[:, columns] = value + refs[-2][:, columns] if added else value


def near_kernel(*refs, plan, pieces, small):
    outs, got = refs[-2:], refs[-2 - pieces - small :]
    half = outs[0].shape[0]
    for o, out in enumerate(outs):
        at = slice(o * half, (o + 1) * half)
        size = 2 * half // pieces
        low = o * half % size
        for columns, value in products(plan, refs, at):
            out[:half, columns] = value + got[o * half // size][low : low + half, columns]
    if small:
        outs[1][half:, :] = got[pieces][...] + got[0][2 * half // pieces :, :]


def step_kernel(*refs, small, joined):
    count = 2 if joined else 1
    keeps, sents, gots = (refs[i * count : (i + 1) * count] for i in range(3))
    outs = refs[3 * count :]
    at = 0
    for i in range(count):
        half = outs[i].shape[0]
        got = gots[i]
        outs[i][...] = keeps[i][:half, :] + got[:half, :]
        outs[count][at : at + half, :] = keeps[i][half:, :] + got[half : 2 * half, :]
        at += half
        if small and not i:
            outs[count][at : at + SMALL, :] = sents[i][2 * half :, :] + got[2 * half :, :]
            at += SMALL


def end_kernel(*refs, wide):
    count = (len(refs) - 1) // (1 + wide)
    keeps, got, outs = refs[:count], refs[count], refs[count + 1 :]
    at = o = 0
    for keep in keeps:
        size, each = keep.shape[0], keep.shape[1] // wide
        for w in range(wide):
            columns = slice(w * each, (w + 1) * each)
            outs[o][...] = keep[:, columns] + got[at : at + size, columns]
            o += 1
        at += size


def vector_kernel(here, sent, got, *outs, size):
    total = sent[size : size + SMALL, :] + got[size : size + SMALL, :]
    bias_q, bias_v, bias_up, gain_mlp, shift_mlp, bias_out, bias_down, gains = outs
    width, each = total.shape[1], bias_q.shape[0]
    bias_q[...] = total[5, :each]
    bias_v[...] = total[5, each:]
    for i in range(bias_up.shape[0] // width):
        bias_up[i * width : (i + 1) * width] = total[6 + i, :]
    turned = pltpu.roll(total, lax.rem(width - here[0] * size, width), 1)
    for out, at in ((gain_mlp, 0), (shift_mlp, 1), (bias_out, 2), (bias_down, 8)):
        out[...] = turned[at, :size]
    gains[...] = turned[:8, : gains.shape[1]]


def gain_kernel(own, other, gain, shift):
    total = own[...] + other[...]
    gain[...] = total[3, : gain.shape[0]]
    shift[...] = total[4, : shift.shape[0]]


class Steps:
    def __init__(self):
        self.last = None

    def __call__(
        self, kernel, name, outs, args, scratch=(), limit=12, smem=0, whole=(), tie=0, alias=None, cost=0, out_whole=False
    ):
        args = list(args)
        if self.last is not None:
            args[tie], _ = lax.optimization_barrier((args[tie], self.last))
        result = pl.pallas_call(
            kernel,
            name=name,
            out_shape=[jax.ShapeDtypeStruct(s, d) for s, d in outs],
            in_specs=[pl.BlockSpec(memory_space=pltpu.SMEM)] * smem
            + [pl.BlockSpec(memory_space=pl.ANY) if i in whole else VMEM for i in range(smem, len(args))]
            if whole
            else [pl.BlockSpec(memory_space=pltpu.SMEM)] * smem + [VMEM] * (len(args) - smem),
            out_specs=[pl.BlockSpec(memory_space=pl.ANY) if out_whole else VMEM] * len(outs),
            scratch_shapes=list(scratch),
            input_output_aliases=alias or {},
            compiler_params=pltpu.CompilerParams(vmem_limit_bytes=limit << 20),
            cost_estimate=pl.CostEstimate(flops=1000 + cost, bytes_accessed=1000, transcendentals=0),
        )(*args)
        self.last = result[0]
        return result


def send(values, bit, count):
    return lax.ppermute(values, "dp", [(i, i ^ (1 << bit)) for i in range(count)])


def swap(values):
    return lax.ppermute(values, "mp", [(0, 1), (1, 0)])


class Scatter:
    def __init__(self, steps, count, bits, plan, pieces=2, wide=1, small=None):
        self.steps, self.count, self.bits = steps, count, bits
        self.pieces, self.wide, self.small = pieces, wide, small
        self.plan, self.arrays, self.columns = [], [], 0
        for lefts, rights in plan:
            at, each = len(self.arrays), len(lefts)
            self.arrays += lefts + rights
            places = list(range(at, at + each)), list(range(at + each, at + 2 * each))
            self.plan.append((*places, self.columns))
            self.columns += rights[0].shape[1]
        self.rows = plan[0][0][0].shape[0] // 2
        self.extra = SMALL if small is not None else 0
        self.at = 1

    def shapes(self, *sizes):
        return [((n, self.columns), HIGH) for n in sizes]

    def far(self):
        size = self.rows // self.pieces
        kernel = partial(
            far_kernel,
            plan=self.plan,
            start=self.rows,
            pieces=self.pieces,
            small=bool(self.extra),
        )
        held = self.arrays + ([self.small] if self.extra else [])
        outs = self.shapes(size + self.extra, *[size] * (self.pieces - 1))
        outs = self.steps(kernel, "far", outs, held)
        self.got = [send(o, self.bits[0], self.count) for o in outs]

    def near(self):
        kernel = partial(
            near_kernel,
            plan=self.plan,
            pieces=self.pieces,
            small=bool(self.extra),
        )
        held = self.arrays + self.got + ([self.small] if self.extra else [])
        self.rows //= 2
        outs = self.shapes(self.rows, self.rows + self.extra)
        self.keep, self.sent = self.steps(kernel, "near", outs, held)
        self.got = send(self.sent, self.bits[1], self.count)

    def part(self, start, added):
        kernel = partial(part_kernel, plan=self.plan, start=start * self.rows // 2, added=len(added))
        outs = self.shapes(self.rows // 2)
        return self.steps(kernel, "part", outs, self.arrays + added)[0]

    def far_part(self, sent):
        return send(self.part(2 + sent, []), self.bits[0], self.count)

    def near_sent(self, got):
        self.sent = self.part(1, [got])
        self.got = send(self.sent, self.bits[1], self.count)

    def near_keep(self, got):
        self.keep = self.part(0, [got])
        self.rows //= 2

    def rest(self):
        while self.at + 1 < len(self.bits):
            self.step()

    def step(self):
        self.at += 1
        self.rows //= 2
        outs = self.shapes(self.rows, self.rows + self.extra)
        kernel = partial(step_kernel, small=bool(self.extra), joined=False)
        self.keep, self.sent = self.steps(kernel, "sum", outs, [self.keep, self.sent, self.got])
        self.got = send(self.sent, self.bits[self.at], self.count)


def join(one, two):
    for part in (one, two):
        part.at += 1
        part.rows //= 2
    outs = one.shapes(one.rows) + two.shapes(two.rows) + one.shapes(one.rows + two.rows + one.extra)
    kernel = partial(step_kernel, small=bool(one.extra), joined=True)
    held = [one.keep, two.keep, one.sent, two.sent, one.got, two.got]
    one.keep, two.keep, sent = one.steps(kernel, "sums", outs, held)
    got = send(sent, one.bits[one.at], one.count)
    while one.at + 1 < len(one.bits):
        one.at += 1
        half = one.rows // 2
        starts = (0, one.rows + one.extra)
        keeps, sents = [], []
        for part, start in zip((one, two), starts):
            total = part.keep + got[start : start + part.rows]
            keeps.append(total[:half])
            sents.append(total[half:])
        if one.extra:
            at = slice(one.rows, one.rows + one.extra)
            sents.insert(1, sent[at] + got[at])
        one.keep, two.keep = keeps
        one.rows = two.rows = half
        sent = jnp.concatenate(sents)
        got = send(sent, one.bits[one.at], one.count)
    return sent, got


def finish(parts, got, cost=0):
    outs = []
    for part in parts:
        outs += [((part.rows, part.columns // part.wide), HIGH)] * part.wide
    kernel = partial(end_kernel, wide=parts[0].wide)
    held = [part.keep for part in parts] + [got]
    return parts[0].steps(kernel, "end", outs, held, cost=cost)


def body(
    tokens,
    crop_ids,
    w_query,
    w_key,
    w_value,
    bias_query,
    bias_value,
    w_out,
    bias_out,
    gain_attn,
    shift_attn,
    gain_mlp,
    shift_mlp,
    w_up,
    bias_up,
    w_down,
    bias_down,
    cotangent,
    count,
):
    width = tokens.shape[1]
    local = w_query.shape[1]
    hidden_units = w_up.shape[1]
    seqs, length = crop_ids.shape
    rows = seqs * length
    here = lax.axis_index("dp")
    scalar = here.reshape(1)
    bits = list(range(count.bit_length() - 1))
    orders = (bits, [0, 2, 1] + bits[3:])
    steps = Steps()
    piece = local // 4
    lines = [gain_attn, shift_attn, bias_query, bias_value, bias_out, gain_mlp, shift_mlp]
    lines += [bias_down, bias_up]
    crops = BIAS_UP + hidden_units // width
    held = [((piece, width), LOW), (crop_ids.shape, jnp.int32)] + [(v.shape, HIGH) for v in lines]
    mine, table = steps(
        load_kernel,
        "load",
        [((piece, width), HIGH), ((crops + seqs, width), HIGH)],
        [scalar, w_out, crop_ids] + lines,
        scratch=[pltpu.VMEM(*h) for h in held] + [pltpu.SemaphoreType.DMA((len(held),))],
        smem=1,
        whole=range(1, 3 + len(lines)),
        limit=63,
    )
    got = swap(mine)

    def like(*arrays):
        return [(a.shape, a.dtype) for a in arrays]

    loaded = [tokens, table, w_query, w_key, w_value]
    made = [((rows, width), LOW)] + [((rows, local), LOW)] * 3
    made += [((rows, 128), HIGH)] + [((length, local), HIGH)] * seqs
    first, query, key_rows, value_rows, log_total, *mixed = steps(
        partial(front_kernel, length=length, seqs=seqs, crops=crops),
        "front",
        made,
        loaded,
        scratch=[pltpu.VMEM(*v) for v in like(*loaded) + made]
        + [pltpu.SemaphoreType.DMA((len(loaded) + len(made),))],
        whole=range(5),
        out_whole=True,
        tie=1,
        limit=58,
    )
    mixed_other = [swap(o) for o in mixed]

    got, _ = lax.optimization_barrier((got, first))
    beside = send(got, 1, count)
    pieces = [got, send(got, 0, count), beside]
    turned = steps(
        partial(turn_kernel, count=count, orders=orders),
        "turn",
        like(cotangent, w_up, w_out)
        + [((width, width), LOW), ((1, width), HIGH)]
        + [((width, length), LOW)] * (3 * seqs),
        [scalar, first, cotangent, w_up, w_out],
        scratch=[pltpu.VMEM((rows, width), LOW), pltpu.SemaphoreType.DMA((4,))],
        whole=range(1, 5),
        smem=1,
        tie=1,
        limit=44,
    )

    cotangent, w_up, w_out, order_b, cot_sum = turned[:5]
    a1_a, a1_b, cot_a = (list(turned[5 + i * seqs : 5 + (i + 1) * seqs]) for i in range(3))
    beside, _ = lax.optimization_barrier((beside, order_b))
    pieces.append(send(beside, 0, count))
    mixed_other[0] = steps(low_kernel, "low", [((length, local), LOW)], [mixed_other[0]], cost=31 * 10**8)[0]
    w_low = steps(
        gather_kernel, "gather", [((local, width), LOW)], [scalar] + pieces, smem=1, tie=1
    )[0]
    hidden, a2_b, active, g_pre, second, carried = [], [], [], [], [], []
    for s in range(seqs):
        result = steps(
            partial(middle_kernel, blocks=2, seq=s, length=length),
            "middle",
            [
                ((length, width), HIGH),
                ((width, length), LOW),
                ((length, hidden_units), LOW),
                ((length, hidden_units), LOW),
                ((length, width), HIGH),
                ((1, hidden_units), HIGH),
            ],
            [
                tokens,
                mixed[s],
                mixed_other[s],
                w_out,
                w_low,
                table,
                w_up,
                w_down,
                cotangent,
                order_b,
            ]
            + carried,
            tie=1,
        )
        for held, value in zip((hidden, a2_b, active, g_pre, second), result):
            held.append(value)
        carried = list(result[5:])
    bias_sum = carried[0]
    second_other = [swap(g) for g in second]

    down = Scatter(steps, count, orders[0], [(cot_a, active)])
    up = Scatter(steps, count, orders[1], [(a2_b, g_pre)])
    parts = [one.far_part(sent) for sent in (1, 0) for one in (down, up)]
    down.near_sent(parts[0])
    up.near_sent(parts[1])
    mlp_part = steps(mlp_kernel, "mlp", [((rows, width), HIGH)], [w_down] + active, tie=1)[0]
    mlp_other = swap(mlp_part)
    down.near_keep(parts[2])
    up.near_keep(parts[3])
    g_hidden, gh_b, g_qk, g_val, carried = [], [], [], [], [bias_sum, cot_sum]
    for s in range(seqs):
        if s == seqs - 1:
            down.step()
            up.step()
        result = steps(
            partial(back_kernel, seq=s, length=length, crops=crops),
            "back",
            [
                ((length, width), HIGH),
                ((width, length), LOW),
                ((length, 2 * local), LOW),
                ((length, local), LOW),
                ((SMALL, width), HIGH),
                (((s + 1) * length, width), HIGH),
            ],
            [tokens, table, cotangent, hidden[s], second[s], second_other[s], order_b]
            + [w_out, w_query, w_key, w_value, query, key_rows, value_rows, log_total]
            + carried,
            tie=4,
            cost=0 if s else 6 * 10**9,
        )
        for held, value in zip((g_hidden, gh_b, g_qk, g_val), result):
            held.append(value)
        carried = list(result[4:])
    sums, g_first = carried
    first_other = swap(g_first)
    heads = Scatter(steps, count, orders[0], [(a1_a, g_qk)], wide=2, small=sums)
    others = Scatter(steps, count, orders[1], [(a1_b, g_val), (gh_b, mixed)], wide=2)
    heads.far()
    others.far()
    _, mlp_got = join(down, up)
    heads.near()
    others.near()
    heads.step()
    block_out = steps(
        partial(out_kernel, seqs=seqs, length=length),
        "out",
        [((rows, width), LOW)],
        [table, mlp_part, mlp_other] + hidden,
        tie=1,
        cost=3 * 10**9,
    )[0]
    others.step()
    w_down_t, done_w_up = finish([down, up], mlp_got, 15 * 10**8)
    heads.rest()
    others.rest()
    base, unit, scale = steps(
        partial(base_kernel, length=length),
        "base",
        [((rows, width), HIGH)] * 2 + [((rows, 1), HIGH)],
        [table, tokens, g_first] + g_hidden,
        tie=2,
    )
    size = width // count
    (
        done_bias_q,
        done_bias_v,
        done_bias_up,
        done_gain_mlp,
        done_shift_mlp,
        done_bias_out,
        done_bias_down,
        gains,
    ) = steps(
        partial(vector_kernel, size=size),
        "vectors",
        [((local,), HIGH)] * 2
        + [((hidden_units,), HIGH)]
        + [((size,), HIGH)] * 4
        + [((8, 128), HIGH)],
        [scalar, heads.sent, heads.got],
        smem=1,
        tie=1,
    )
    gains_other = swap(gains)
    grad_w_q, grad_w_k = finish([heads], heads.got)
    grad_w_v, w_out_t = finish([others], others.got)
    grad_tokens = steps(
        partial(last_kernel, length=length),
        "last",
        [((rows, width), HIGH)],
        [table, base, unit, scale, first_other],
        tie=1,
    )[0]
    done_gain_attn, done_shift_attn = steps(
        gain_kernel, "gains", [((size,), HIGH)] * 2, [gains, gains_other]
    )
    return (
        block_out,
        grad_tokens,
        grad_w_q,
        grad_w_k,
        grad_w_v,
        done_bias_q,
        done_bias_v,
        w_out_t.T,
        done_bias_out,
        done_gain_attn,
        done_shift_attn,
        done_gain_mlp,
        done_shift_mlp,
        done_w_up,
        done_bias_up,
        w_down_t.T,
        done_bias_down,
    )


def solution(mesh):
    placed = (
        P("dp", None),
        P("dp", None),
        P(None, "mp"),
        P(None, "mp"),
        P(None, "mp"),
        P("mp"),
        P("mp"),
        P("mp", None),
        P(),
        P(),
        P(),
        P(),
        P(),
        P(None, "mp"),
        P("mp"),
        P("mp", None),
        P(),
        P("dp", None),
    )
    return jax.shard_map(
        partial(body, count=mesh.shape["dp"]),
        mesh=mesh,
        in_specs=placed,
        out_specs=(
            P("dp", None),
            P("dp", None),
            P("dp", "mp"),
            P("dp", "mp"),
            P("dp", "mp"),
            P("mp"),
            P("mp"),
            P("mp", "dp"),
            P("dp"),
            P("dp"),
            P("dp"),
            P("dp"),
            P("dp"),
            P("dp", "mp"),
            P("mp"),
            P("mp", "dp"),
            P("dp"),
        ),
        check_vma=False,
    )
```

```python
from functools import partial

import jax
import jax.numpy as jnp
from jax import lax
from jax.experimental import pallas as pl
from jax.experimental.pallas import tpu as pltpu
from jax.sharding import PartitionSpec as P

HEAD_DIM = 64
PAIR = 2 * HEAD_DIM
EPS = 1e-06
NEGATIVE = -1e30
LOW = jnp.bfloat16
HIGH = jnp.float32
VMEM = pl.BlockSpec(memory_space=pltpu.VMEM)
SMALL = 16
GAIN_ATTN, SHIFT_ATTN, BIAS_Q, BIAS_V, BIAS_OUT, GAIN_MLP, SHIFT_MLP, BIAS_DOWN, BIAS_UP = range(9)


def plain_dot(left, right):
    return jnp.dot(left, right, preferred_element_type=HIGH)


def right_trans(left, right):
    return lax.dot_general(left, right, (((1,), (1,)), ((), ())), preferred_element_type=HIGH)


def left_trans(left, right):
    return lax.dot_general(left, right, (((0,), (0,)), ((), ())), preferred_element_type=HIGH)


def unit_rows(values):
    mean = jnp.mean(values, axis=-1, keepdims=True)
    centred = values - mean
    scale = lax.rsqrt(jnp.mean(centred * centred, axis=-1, keepdims=True) + EPS)
    return centred * scale, scale


def norm_back(grad_unit, unit, scale):
    inner = jnp.mean(grad_unit * unit, axis=-1, keepdims=True)
    return scale * (grad_unit - jnp.mean(grad_unit, axis=-1, keepdims=True) - unit * inner)


def half_masks():
    lane = lax.broadcasted_iota(jnp.int32, (1, PAIR), 1)
    first = lane < HEAD_DIM
    return first, (first.astype(HIGH).astype(LOW), (~first).astype(HIGH).astype(LOW))


def col_sum(values):
    return jnp.sum(values, axis=0, keepdims=True)


def row(table, at, size):
    return table[at : at + 1, :size]


def same_crop(table, slot, length):
    ids = row(table, slot, length)
    marks = lax.broadcasted_iota(jnp.int32, (SMALL, length), 0).astype(HIGH) == ids
    marks = marks.astype(HIGH).astype(LOW)
    return left_trans(marks, marks) > 0.5


def copies_of(sources, targets, sems):
    copies = [pltpu.make_async_copy(a, b, sems.at[i]) for i, (a, b) in enumerate(zip(sources, targets))]
    for copy in copies:
        copy.start()
    return copies


def load_kernel(here, w_out, crops, *refs):
    count = (len(refs) - 5) // 2
    vectors, (piece, table), sems = refs[:count], refs[count : count + 2], refs[-1]
    held = refs[count + 2 : -1]
    size = piece.shape[0]
    start = pl.multiple_of((here[0] & 3) * size, size)
    sources = [w_out.at[pl.ds(start, size), :], crops, *vectors]
    copies = copies_of(sources, held, sems)
    copies[0].wait()
    piece[...] = held[0][...].astype(HIGH)
    for copy in copies[1:]:
        copy.wait()
    table[...] = jnp.zeros_like(table)
    at, width = 0, table.shape[1]
    for vector in held[2:]:
        for low in range(0, vector.shape[0], width):
            part = min(width, vector.shape[0] - low)
            table[at : at + 1, :part] = vector[low : low + part].reshape(1, part)
            at += 1
    seqs, length = held[1].shape
    table[at : at + seqs, :length] = held[1][...].astype(HIGH)


def front_kernel(*refs, length, seqs, crops):
    sources, count = refs[:5], 5 + seqs
    targets, held, kept, sems = refs[5 : 5 + count], refs[5 + count : 10 + count], refs[10 + count : -1], refs[-1]
    copies = copies_of(sources, held, sems)
    tokens, table, w_q, w_k, w_v = held
    first_out, q, k, v, lse, *outs = kept
    stores = [pltpu.make_async_copy(a, b, sems.at[5 + i]) for i, (a, b) in enumerate(zip(kept, targets))]
    copies[0].wait()
    unit, _ = unit_rows(tokens[...].astype(HIGH))
    copies[1].wait()
    local, width = w_q.shape[1], tokens.shape[1]
    first = (unit * row(table, GAIN_ATTN, width) + row(table, SHIFT_ATTN, width)).astype(LOW)
    first_out[...] = first
    stores[0].start()
    for copy in copies[2:]:
        copy.wait()
    q_all = plain_dot(first, w_q[...]) + row(table, BIAS_Q, local)
    q_all = (q_all.astype(LOW) * 0.125).astype(LOW)
    k_all = plain_dot(first, w_k[...]).astype(LOW)
    v_all = (plain_dot(first, w_v[...]) + row(table, BIAS_V, local)).astype(LOW)
    q[...] = q_all
    k[...] = k_all
    v[...] = v_all
    for store in stores[1:4]:
        store.start()
    low_half, masks = half_masks()
    for s, o in enumerate(outs):
        rows = slice(s * length, (s + 1) * length)
        same = same_crop(table, crops + s, length)
        for t in range(local // PAIR):
            at = slice(t * PAIR, (t + 1) * PAIR)
            q_pair, k_pair, v_pair = q_all[rows, at], k_all[rows, at], v_all[rows, at]
            got = []
            for half in range(2):
                scores = jnp.where(same, right_trans(q_pair * masks[half], k_pair), NEGATIVE)
                top = jnp.max(scores, axis=-1, keepdims=True)
                expo = jnp.exp(scores - top)
                total = jnp.sum(expo, axis=-1, keepdims=True)
                probs = (expo * (1.0 / total)).astype(LOW)
                got.append(plain_dot(probs, v_pair))
                h = 2 * t + half
                lse[rows, h : h + 1] = top + jnp.log(total)
            o[:, at] = jnp.where(low_half, got[0], got[1])
        stores[5 + s].start()
    stores[4].start()
    for store in stores:
        store.wait()


def relative_rows(here, width, count, bits):
    size = width // count
    place = lax.broadcasted_iota(jnp.int32, (width, 1), 0)
    block = ((place.astype(HIGH) + 0.5) * (1.0 / size)).astype(jnp.int32)
    mask = jnp.zeros_like(block)
    for p, bit in enumerate(bits):
        mask = mask + (((block >> (len(bits) - 1 - p)) & 1) << bit)
    source = (mask ^ here) * size + (place - block * size)
    marks = lax.broadcasted_iota(jnp.int32, (width, width), 1) == source
    return marks.astype(HIGH).astype(LOW)


def turn_kernel(here, *refs, count, orders):
    sources, held = refs[:4], (refs[-2], *refs[4:7])
    order_b, sums, sems = refs[7], refs[8], refs[-1]
    seqs = (len(refs) - 11) // 3
    a1_a, a1_b, cot_a = (refs[9 + i * seqs : 9 + (i + 1) * seqs] for i in range(3))
    first = refs[-2]
    length = first.shape[0] // seqs
    copies = copies_of(sources, held, sems)
    width = first.shape[1]
    order_a = relative_rows(here[0], width, count, orders[0])
    order = relative_rows(here[0], width, count, orders[1])
    order_b[...] = order
    copies[0].wait()
    for s in range(seqs):
        part = first[s * length : (s + 1) * length, :]
        a1_a[s][...] = right_trans(order_a, part).astype(LOW)
        a1_b[s][...] = right_trans(order, part).astype(LOW)
    for copy in copies[1:]:
        copy.wait()
    cot = held[1][...]
    for s in range(seqs):
        part = cot[s * length : (s + 1) * length, :]
        cot_a[s][...] = right_trans(order_a, part).astype(LOW)
    sums[...] = col_sum(cot.astype(HIGH))


def low_kernel(values, out):
    out[...] = values[...].astype(LOW)


def gather_kernel(here, *refs):
    for b, piece in enumerate(refs[:-1]):
        size = piece.shape[0]
        start = pl.multiple_of(((here[0] & 3) ^ b) * size, size)
        refs[-1][pl.ds(start, size), :] = piece[...].astype(LOW)


def middle_kernel(*refs, blocks, seq, length):
    tokens, o_own, o_other, w_out, w_low, table, w_up, w_down, cotangent, order = refs[:10]
    hidden, a2_t, active, g_pre, g_second, g_bias = refs[-6:]
    rows = slice(seq * length, (seq + 1) * length)
    attn = plain_dot(o_own[...].astype(LOW), w_out[...])
    attn = attn + plain_dot(o_other[...].astype(LOW), w_low[...])
    width = tokens.shape[1]
    values = tokens[rows, :].astype(HIGH) + (attn + row(table, BIAS_OUT, width))
    hidden[...] = values
    unit, _ = unit_rows(values)
    second = (unit * row(table, GAIN_MLP, width) + row(table, SHIFT_MLP, width)).astype(LOW)
    cot = cotangent[rows, :]
    size = w_up.shape[1] // blocks
    total = None
    for b in range(blocks):
        at = slice(b * size, (b + 1) * size)
        low = b * size % width
        at_row = BIAS_UP + b * size // width
        bias_up = table[at_row : at_row + 1, low : low + size]
        pre = plain_dot(second, w_up[:, at]) + bias_up
        cdf = 0.5 * (1.0 + lax.erf(pre * 0.7071067811865476))
        active[:, at] = (pre * cdf).astype(LOW)
        slope = cdf + pre * (0.3989422804014327 * jnp.exp(-0.5 * (pre * pre)))
        grad = (right_trans(cot, w_down[at, :]) * slope).astype(LOW)
        g_pre[:, at] = grad
        bias = col_sum(grad.astype(HIGH))
        g_bias[:, at] = refs[10][:, at] + bias if seq else bias
        part = right_trans(grad, w_up[:, at])
        total = part if total is None else total + part
    g_second[...] = total
    a2_t[...] = right_trans(order[...], second).astype(LOW)


def back_kernel(*refs, seq, length, crops):
    tokens, table, cotangent, hidden, own, other, order = refs[:7]
    w_out, w_q, w_k, w_v, q, k, v, lse = refs[7:15]
    before = refs[15:17]
    g_hidden, gh_t, g_qk, g_val, sums, g_first = refs[17:]
    width, local = tokens.shape[1], q.shape[1]
    rows = slice(seq * length, (seq + 1) * length)
    full = slice(0, width)
    if seq:
        sums_before, first_before = before
        g_first[: seq * length, :] = first_before[...]
        sums[6:, :] = sums_before[6:, :]
    else:
        g_bias, cot_sum = before
        sums[6:7, :] = g_bias[:, :width]
        sums[7:8, :] = g_bias[:, width:]
        sums[8:9, :] = cot_sum[...]
        sums[9:, :] = jnp.zeros_like(sums[9:, :])

    def put(r, at, value):
        sums[r : r + 1, at] = sums_before[r : r + 1, at] + value if seq else value

    unit, scale = unit_rows(hidden[...])
    grad = own[...] + other[...]
    put(0, full, col_sum(grad * unit))
    put(1, full, col_sum(grad))
    values = norm_back(grad * row(table, GAIN_MLP, width), unit, scale)
    values = cotangent[rows, :].astype(HIGH) + values
    g_hidden[...] = values
    put(2, full, col_sum(values))
    low = values.astype(LOW)
    gh_t[...] = right_trans(order[...], low).astype(LOW)
    g_o = right_trans(low, w_out[...]).astype(LOW)
    same = same_crop(table, crops + seq, length)
    low_half, masks = half_masks()
    for t in range(local // PAIR):
        at = slice(t * PAIR, (t + 1) * PAIR)
        q_pair, k_pair, v_pair, o_pair = q[rows, at], k[rows, at], v[rows, at], g_o[:, at]
        got = []
        for half in range(2):
            h = 2 * t + half
            scores = right_trans(q_pair * masks[half], k_pair)
            probs = jnp.exp(jnp.where(same, scores, NEGATIVE) - lse[rows, h : h + 1])
            g_probs = right_trans(o_pair * masks[half], v_pair)
            inner = jnp.sum(g_probs * probs, axis=-1, keepdims=True)
            g_scores = (probs * (g_probs - inner)).astype(LOW)
            got.append(
                (
                    plain_dot(g_scores, k_pair),
                    left_trans(g_scores, q_pair),
                    left_trans(probs.astype(LOW), o_pair),
                )
            )
        g_q = (jnp.where(low_half, got[0][0], got[1][0]) * 0.125).astype(LOW)
        g_k = jnp.where(low_half, got[0][1], got[1][1]).astype(LOW)
        g_v = jnp.where(low_half, got[0][2], got[1][2]).astype(LOW)
        beside = slice(local + t * PAIR, local + (t + 1) * PAIR)
        g_qk[:, at] = g_q
        g_qk[:, beside] = g_k
        g_val[:, at] = g_v
        put(5, at, col_sum(g_q.astype(HIGH)))
        put(5, beside, col_sum(g_v.astype(HIGH)))
    part = right_trans(g_qk[:, :local], w_q[...])
    part = part + right_trans(g_qk[:, local:], w_k[...])
    part = part + right_trans(g_val[...], w_v[...])
    g_first[rows, :] = part
    unit_one, _ = unit_rows(tokens[rows, :].astype(HIGH))
    put(3, full, col_sum(part * unit_one))
    put(4, full, col_sum(part))


def base_kernel(table, tokens, own, *refs, length):
    g_hidden, (base, unit_out, scale_out) = refs[:-3], refs[-3:]
    gain = row(table, GAIN_ATTN, tokens.shape[1])
    for s in range(tokens.shape[0] // length):
        rows = slice(s * length, (s + 1) * length)
        part = own[rows, :]
        unit, scale = unit_rows(tokens[rows, :].astype(HIGH))
        base[rows, :] = g_hidden[s][...] + norm_back(part * gain, unit, scale)
        unit_out[rows, :] = unit
        scale_out[rows, :] = scale


def last_kernel(table, base, unit, scale, other, g_tokens, *, length):
    gain = row(table, GAIN_ATTN, base.shape[1])
    for s in range(base.shape[0] // length):
        rows = slice(s * length, (s + 1) * length)
        grad = norm_back(other[rows, :] * gain, unit[rows, :], scale[rows, :])
        g_tokens[rows, :] = base[rows, :] + grad


def out_kernel(*refs, seqs, length):
    table, own, other = refs[:3]
    for s in range(seqs):
        rows = slice(s * length, (s + 1) * length)
        total = refs[3 + s][...] + (own[rows, :] + other[rows, :])
        refs[3 + seqs][rows, :] = (total + row(table, BIAS_DOWN, total.shape[1])).astype(LOW)


def mlp_kernel(w_down, *refs):
    length = refs[0].shape[0]
    for s, active in enumerate(refs[:-1]):
        refs[-1][s * length : (s + 1) * length, :] = plain_dot(active[...], w_down[...])


def products(plan, refs, at):
    for lefts, rights, column in plan:
        wide = refs[rights[0]].shape[1]
        step = min(512, wide)
        for n in range(0, wide, step):
            value = None
            for left, right in zip(lefts, rights):
                part = plain_dot(refs[left][at, :], refs[right][:, n : n + step].astype(LOW))
                value = part if value is None else value + part
            yield slice(column + n, column + n + step), value


def far_kernel(*refs, plan, start, pieces, small):
    outs = refs[-pieces:]
    size = start // pieces
    for o, out in enumerate(outs):
        at = slice(start + o * size, start + (o + 1) * size)
        for columns, value in products(plan, refs, at):
            out[:size, columns] = value
    if small:
        outs[0][size:, :] = refs[-pieces - 1][...]


def part_kernel(*refs, plan, start, added):
    out = refs[-1]
    at = slice(start, start + out.shape[0])
    for columns, value in products(plan, refs, at):
        out[:, columns] = value + refs[-2][:, columns] if added else value


def near_kernel(*refs, plan, pieces, small):
    outs, got = refs[-2:], refs[-2 - pieces - small :]
    half = outs[0].shape[0]
    for o, out in enumerate(outs):
        at = slice(o * half, (o + 1) * half)
        size = 2 * half // pieces
        low = o * half % size
        for columns, value in products(plan, refs, at):
            out[:half, columns] = value + got[o * half // size][low : low + half, columns]
    if small:
        outs[1][half:, :] = got[pieces][...] + got[0][2 * half // pieces :, :]


def step_kernel(*refs, small, joined):
    count = 2 if joined else 1
    keeps, sents, gots = (refs[i * count : (i + 1) * count] for i in range(3))
    outs = refs[3 * count :]
    at = 0
    for i in range(count):
        half = outs[i].shape[0]
        got = gots[i]
        outs[i][...] = keeps[i][:half, :] + got[:half, :]
        outs[count][at : at + half, :] = keeps[i][half:, :] + got[half : 2 * half, :]
        at += half
        if small and not i:
            outs[count][at : at + SMALL, :] = sents[i][2 * half :, :] + got[2 * half :, :]
            at += SMALL


def end_kernel(*refs, wide):
    count = (len(refs) - 1) // (1 + wide)
    keeps, got, outs = refs[:count], refs[count], refs[count + 1 :]
    at = o = 0
    for keep in keeps:
        size, each = keep.shape[0], keep.shape[1] // wide
        for w in range(wide):
            columns = slice(w * each, (w + 1) * each)
            outs[o][...] = keep[:, columns] + got[at : at + size, columns]
            o += 1
        at += size


def vector_kernel(here, sent, got, *outs, size):
    total = sent[size : size + SMALL, :] + got[size : size + SMALL, :]
    bias_q, bias_v, bias_up, gain_mlp, shift_mlp, bias_out, bias_down, gains = outs
    width, each = total.shape[1], bias_q.shape[0]
    bias_q[...] = total[5, :each]
    bias_v[...] = total[5, each:]
    for i in range(bias_up.shape[0] // width):
        bias_up[i * width : (i + 1) * width] = total[6 + i, :]
    turned = pltpu.roll(total, lax.rem(width - here[0] * size, width), 1)
    for out, at in ((gain_mlp, 0), (shift_mlp, 1), (bias_out, 2), (bias_down, 8)):
        out[...] = turned[at, :size]
    gains[...] = turned[:8, : gains.shape[1]]


def gain_kernel(own, other, gain, shift):
    total = own[...] + other[...]
    gain[...] = total[3, : gain.shape[0]]
    shift[...] = total[4, : shift.shape[0]]


class Steps:
    def __init__(self):
        self.last = None

    def __call__(
        self, kernel, name, outs, args, scratch=(), limit=12, smem=0, whole=(), tie=0, alias=None, cost=0, out_whole=False
    ):
        args = list(args)
        if self.last is not None:
            args[tie], _ = lax.optimization_barrier((args[tie], self.last))
        result = pl.pallas_call(
            kernel,
            name=name,
            out_shape=[jax.ShapeDtypeStruct(s, d) for s, d in outs],
            in_specs=[pl.BlockSpec(memory_space=pltpu.SMEM)] * smem
            + [pl.BlockSpec(memory_space=pl.ANY) if i in whole else VMEM for i in range(smem, len(args))]
            if whole
            else [pl.BlockSpec(memory_space=pltpu.SMEM)] * smem + [VMEM] * (len(args) - smem),
            out_specs=[pl.BlockSpec(memory_space=pl.ANY) if out_whole else VMEM] * len(outs),
            scratch_shapes=list(scratch),
            input_output_aliases=alias or {},
            compiler_params=pltpu.CompilerParams(vmem_limit_bytes=limit << 20),
            cost_estimate=pl.CostEstimate(flops=1000 + cost, bytes_accessed=1000, transcendentals=0),
        )(*args)
        self.last = result[0]
        return result


def send(values, bit, count):
    return lax.ppermute(values, "dp", [(i, i ^ (1 << bit)) for i in range(count)])


def swap(values):
    return lax.ppermute(values, "mp", [(0, 1), (1, 0)])


class Scatter:
    def __init__(self, steps, count, bits, plan, pieces=2, wide=1, small=None):
        self.steps, self.count, self.bits = steps, count, bits
        self.pieces, self.wide, self.small = pieces, wide, small
        self.plan, self.arrays, self.columns = [], [], 0
        for lefts, rights in plan:
            at, each = len(self.arrays), len(lefts)
            self.arrays += lefts + rights
            places = list(range(at, at + each)), list(range(at + each, at + 2 * each))
            self.plan.append((*places, self.columns))
            self.columns += rights[0].shape[1]
        self.rows = plan[0][0][0].shape[0] // 2
        self.extra = SMALL if small is not None else 0
        self.at = 1

    def shapes(self, *sizes):
        return [((n, self.columns), HIGH) for n in sizes]

    def far(self):
        size = self.rows // self.pieces
        kernel = partial(
            far_kernel,
            plan=self.plan,
            start=self.rows,
            pieces=self.pieces,
            small=bool(self.extra),
        )
        held = self.arrays + ([self.small] if self.extra else [])
        outs = self.shapes(size + self.extra, *[size] * (self.pieces - 1))
        outs = self.steps(kernel, "far", outs, held)
        self.got = [send(o, self.bits[0], self.count) for o in outs]

    def near(self):
        kernel = partial(
            near_kernel,
            plan=self.plan,
            pieces=self.pieces,
            small=bool(self.extra),
        )
        held = self.arrays + self.got + ([self.small] if self.extra else [])
        self.rows //= 2
        outs = self.shapes(self.rows, self.rows + self.extra)
        self.keep, self.sent = self.steps(kernel, "near", outs, held)
        self.got = send(self.sent, self.bits[1], self.count)

    def part(self, start, added):
        kernel = partial(part_kernel, plan=self.plan, start=start * self.rows // 2, added=len(added))
        outs = self.shapes(self.rows // 2)
        return self.steps(kernel, "part", outs, self.arrays + added)[0]

    def far_parts(self):
        kernel = partial(far_kernel, plan=self.plan, start=self.rows, pieces=2, small=False)
        kept, sent = self.steps(kernel, "far", self.shapes(*[self.rows // 2] * 2), self.arrays)
        return [send(o, self.bits[0], self.count) for o in (sent, kept)]

    def near_sent(self, got):
        self.sent = self.part(1, [got])
        self.got = send(self.sent, self.bits[1], self.count)

    def near_keep(self, got):
        self.keep = self.part(0, [got])
        self.rows //= 2

    def rest(self):
        while self.at + 1 < len(self.bits):
            self.step()

    def step(self):
        self.at += 1
        self.rows //= 2
        outs = self.shapes(self.rows, self.rows + self.extra)
        kernel = partial(step_kernel, small=bool(self.extra), joined=False)
        self.keep, self.sent = self.steps(kernel, "sum", outs, [self.keep, self.sent, self.got])
        self.got = send(self.sent, self.bits[self.at], self.count)


def join(one, two):
    for part in (one, two):
        part.at += 1
        part.rows //= 2
    outs = one.shapes(one.rows) + two.shapes(two.rows) + one.shapes(one.rows + two.rows + one.extra)
    kernel = partial(step_kernel, small=bool(one.extra), joined=True)
    held = [one.keep, two.keep, one.sent, two.sent, one.got, two.got]
    one.keep, two.keep, sent = one.steps(kernel, "sums", outs, held)
    got = send(sent, one.bits[one.at], one.count)
    while one.at + 1 < len(one.bits):
        one.at += 1
        half = one.rows // 2
        starts = (0, one.rows + one.extra)
        keeps, sents = [], []
        for part, start in zip((one, two), starts):
            total = part.keep + got[start : start + part.rows]
            keeps.append(total[:half])
            sents.append(total[half:])
        if one.extra:
            at = slice(one.rows, one.rows + one.extra)
            sents.insert(1, sent[at] + got[at])
        one.keep, two.keep = keeps
        one.rows = two.rows = half
        sent = jnp.concatenate(sents)
        got = send(sent, one.bits[one.at], one.count)
    return sent, got


def finish(parts, got, cost=0):
    outs = []
    for part in parts:
        outs += [((part.rows, part.columns // part.wide), HIGH)] * part.wide
    kernel = partial(end_kernel, wide=parts[0].wide)
    held = [part.keep for part in parts] + [got]
    return parts[0].steps(kernel, "end", outs, held, cost=cost)


def body(
    tokens,
    crop_ids,
    w_query,
    w_key,
    w_value,
    bias_query,
    bias_value,
    w_out,
    bias_out,
    gain_attn,
    shift_attn,
    gain_mlp,
    shift_mlp,
    w_up,
    bias_up,
    w_down,
    bias_down,
    cotangent,
    count,
):
    width = tokens.shape[1]
    local = w_query.shape[1]
    hidden_units = w_up.shape[1]
    seqs, length = crop_ids.shape
    rows = seqs * length
    here = lax.axis_index("dp")
    scalar = here.reshape(1)
    bits = list(range(count.bit_length() - 1))
    orders = (bits, [0, 2, 1] + bits[3:])
    steps = Steps()
    piece = local // 4
    lines = [gain_attn, shift_attn, bias_query, bias_value, bias_out, gain_mlp, shift_mlp]
    lines += [bias_down, bias_up]
    crops = BIAS_UP + hidden_units // width
    held = [((piece, width), LOW), (crop_ids.shape, jnp.int32)] + [(v.shape, HIGH) for v in lines]
    mine, table = steps(
        load_kernel,
        "load",
        [((piece, width), HIGH), ((crops + seqs, width), HIGH)],
        [scalar, w_out, crop_ids] + lines,
        scratch=[pltpu.VMEM(*h) for h in held] + [pltpu.SemaphoreType.DMA((len(held),))],
        smem=1,
        whole=range(1, 3 + len(lines)),
        limit=63,
    )
    got = swap(mine)

    def like(*arrays):
        return [(a.shape, a.dtype) for a in arrays]

    loaded = [tokens, table, w_query, w_key, w_value]
    made = [((rows, width), LOW)] + [((rows, local), LOW)] * 3
    made += [((rows, 128), HIGH)] + [((length, local), HIGH)] * seqs
    first, query, key_rows, value_rows, log_total, *mixed = steps(
        partial(front_kernel, length=length, seqs=seqs, crops=crops),
        "front",
        made,
        loaded,
        scratch=[pltpu.VMEM(*v) for v in like(*loaded) + made]
        + [pltpu.SemaphoreType.DMA((len(loaded) + len(made),))],
        whole=range(5),
        out_whole=True,
        tie=1,
        limit=58,
    )
    mixed_other = [swap(o) for o in mixed]

    got, _ = lax.optimization_barrier((got, first))
    beside = send(got, 1, count)
    pieces = [got, send(got, 0, count), beside]
    turned = steps(
        partial(turn_kernel, count=count, orders=orders),
        "turn",
        like(cotangent, w_up, w_out)
        + [((width, width), LOW), ((1, width), HIGH)]
        + [((width, length), LOW)] * (3 * seqs),
        [scalar, first, cotangent, w_up, w_out],
        scratch=[pltpu.VMEM((rows, width), LOW), pltpu.SemaphoreType.DMA((4,))],
        whole=range(1, 5),
        smem=1,
        tie=1,
        limit=44,
    )

    cotangent, w_up, w_out, order_b, cot_sum = turned[:5]
    a1_a, a1_b, cot_a = (list(turned[5 + i * seqs : 5 + (i + 1) * seqs]) for i in range(3))
    beside, _ = lax.optimization_barrier((beside, order_b))
    pieces.append(send(beside, 0, count))
    mixed_other[0] = steps(low_kernel, "low", [((length, local), LOW)], [mixed_other[0]], cost=31 * 10**8)[0]
    w_low = steps(
        gather_kernel, "gather", [((local, width), LOW)], [scalar] + pieces, smem=1, tie=1
    )[0]
    hidden, a2_b, active, g_pre, second, carried = [], [], [], [], [], []
    for s in range(seqs):
        result = steps(
            partial(middle_kernel, blocks=2, seq=s, length=length),
            "middle",
            [
                ((length, width), HIGH),
                ((width, length), LOW),
                ((length, hidden_units), LOW),
                ((length, hidden_units), LOW),
                ((length, width), HIGH),
                ((1, hidden_units), HIGH),
            ],
            [
                tokens,
                mixed[s],
                mixed_other[s],
                w_out,
                w_low,
                table,
                w_up,
                w_down,
                cotangent,
                order_b,
            ]
            + carried,
            tie=1,
        )
        for held, value in zip((hidden, a2_b, active, g_pre, second), result):
            held.append(value)
        carried = list(result[5:])
    bias_sum = carried[0]
    second_other = [swap(g) for g in second]

    down = Scatter(steps, count, orders[0], [(cot_a, active)])
    up = Scatter(steps, count, orders[1], [(a2_b, g_pre)])
    (down_sent, down_kept), (up_sent, up_kept) = [one.far_parts() for one in (down, up)]
    down.near_sent(down_sent)
    up.near_sent(up_sent)
    mlp_part = steps(mlp_kernel, "mlp", [((rows, width), HIGH)], [w_down] + active, tie=1)[0]
    mlp_other = swap(mlp_part)
    down.near_keep(down_kept)
    up.near_keep(up_kept)
    g_hidden, gh_b, g_qk, g_val, carried = [], [], [], [], [bias_sum, cot_sum]
    for s in range(seqs):
        if s == seqs - 1:
            down.step()
            up.step()
        result = steps(
            partial(back_kernel, seq=s, length=length, crops=crops),
            "back",
            [
                ((length, width), HIGH),
                ((width, length), LOW),
                ((length, 2 * local), LOW),
                ((length, local), LOW),
                ((SMALL, width), HIGH),
                (((s + 1) * length, width), HIGH),
            ],
            [tokens, table, cotangent, hidden[s], second[s], second_other[s], order_b]
            + [w_out, w_query, w_key, w_value, query, key_rows, value_rows, log_total]
            + carried,
            tie=4,
            cost=0 if s else 6 * 10**9,
        )
        for held, value in zip((g_hidden, gh_b, g_qk, g_val), result):
            held.append(value)
        carried = list(result[4:])
    sums, g_first = carried
    first_other = swap(g_first)
    heads = Scatter(steps, count, orders[0], [(a1_a, g_qk)], wide=2, small=sums)
    others = Scatter(steps, count, orders[1], [(a1_b, g_val), (gh_b, mixed)], wide=2)
    heads.far()
    others.far()
    _, mlp_got = join(down, up)
    heads.near()
    others.near()
    heads.step()
    block_out = steps(
        partial(out_kernel, seqs=seqs, length=length),
        "out",
        [((rows, width), LOW)],
        [table, mlp_part, mlp_other] + hidden,
        tie=1,
        cost=3 * 10**9,
    )[0]
    others.step()
    w_down_t, done_w_up = finish([down, up], mlp_got, 15 * 10**8)
    heads.rest()
    others.rest()
    base, unit, scale = steps(
        partial(base_kernel, length=length),
        "base",
        [((rows, width), HIGH)] * 2 + [((rows, 1), HIGH)],
        [table, tokens, g_first] + g_hidden,
        tie=2,
    )
    size = width // count
    (
        done_bias_q,
        done_bias_v,
        done_bias_up,
        done_gain_mlp,
        done_shift_mlp,
        done_bias_out,
        done_bias_down,
        gains,
    ) = steps(
        partial(vector_kernel, size=size),
        "vectors",
        [((local,), HIGH)] * 2
        + [((hidden_units,), HIGH)]
        + [((size,), HIGH)] * 4
        + [((8, 128), HIGH)],
        [scalar, heads.sent, heads.got],
        smem=1,
        tie=1,
    )
    gains_other = swap(gains)
    grad_w_q, grad_w_k = finish([heads], heads.got)
    grad_w_v, w_out_t = finish([others], others.got)
    grad_tokens = steps(
        partial(last_kernel, length=length),
        "last",
        [((rows, width), HIGH)],
        [table, base, unit, scale, first_other],
        tie=1,
    )[0]
    done_gain_attn, done_shift_attn = steps(
        gain_kernel, "gains", [((size,), HIGH)] * 2, [gains, gains_other]
    )
    return (
        block_out,
        grad_tokens,
        grad_w_q,
        grad_w_k,
        grad_w_v,
        done_bias_q,
        done_bias_v,
        w_out_t.T,
        done_bias_out,
        done_gain_attn,
        done_shift_attn,
        done_gain_mlp,
        done_shift_mlp,
        done_w_up,
        done_bias_up,
        w_down_t.T,
        done_bias_down,
    )


def solution(mesh):
    placed = (
        P("dp", None),
        P("dp", None),
        P(None, "mp"),
        P(None, "mp"),
        P(None, "mp"),
        P("mp"),
        P("mp"),
        P("mp", None),
        P(),
        P(),
        P(),
        P(),
        P(),
        P(None, "mp"),
        P("mp"),
        P("mp", None),
        P(),
        P("dp", None),
    )
    return jax.shard_map(
        partial(body, count=mesh.shape["dp"]),
        mesh=mesh,
        in_specs=placed,
        out_specs=(
            P("dp", None),
            P("dp", None),
            P("dp", "mp"),
            P("dp", "mp"),
            P("dp", "mp"),
            P("mp"),
            P("mp"),
            P("mp", "dp"),
            P("dp"),
            P("dp"),
            P("dp"),
            P("dp"),
            P("dp"),
            P("dp", "mp"),
            P("mp"),
            P("mp", "dp"),
            P("dp"),
        ),
        check_vma=False,
    )
```

```python
from functools import partial

import jax
import jax.numpy as jnp
from jax import lax
from jax.experimental import pallas as pl
from jax.experimental.pallas import tpu as pltpu
from jax.sharding import PartitionSpec as P

HEAD_DIM = 64
PAIR = 2 * HEAD_DIM
EPS = 1e-06
NEGATIVE = -1e30
LOW = jnp.bfloat16
HIGH = jnp.float32
VMEM = pl.BlockSpec(memory_space=pltpu.VMEM)
SMALL = 16
GAIN_ATTN, SHIFT_ATTN, BIAS_Q, BIAS_V, BIAS_OUT, GAIN_MLP, SHIFT_MLP, BIAS_DOWN, BIAS_UP = range(9)


def plain_dot(left, right):
    return jnp.dot(left, right, preferred_element_type=HIGH)


def right_trans(left, right):
    return lax.dot_general(left, right, (((1,), (1,)), ((), ())), preferred_element_type=HIGH)


def left_trans(left, right):
    return lax.dot_general(left, right, (((0,), (0,)), ((), ())), preferred_element_type=HIGH)


def unit_rows(values):
    mean = jnp.mean(values, axis=-1, keepdims=True)
    centred = values - mean
    scale = lax.rsqrt(jnp.mean(centred * centred, axis=-1, keepdims=True) + EPS)
    return centred * scale, scale


def norm_back(grad_unit, unit, scale):
    inner = jnp.mean(grad_unit * unit, axis=-1, keepdims=True)
    return scale * (grad_unit - jnp.mean(grad_unit, axis=-1, keepdims=True) - unit * inner)


def half_masks():
    lane = lax.broadcasted_iota(jnp.int32, (1, PAIR), 1)
    first = lane < HEAD_DIM
    return first, (first.astype(HIGH).astype(LOW), (~first).astype(HIGH).astype(LOW))


def col_sum(values):
    return jnp.sum(values, axis=0, keepdims=True)


def row(table, at, size):
    return table[at : at + 1, :size]


def same_crop(table, slot, length):
    ids = row(table, slot, length)
    marks = lax.broadcasted_iota(jnp.int32, (SMALL, length), 0).astype(HIGH) == ids
    marks = marks.astype(HIGH).astype(LOW)
    return left_trans(marks, marks) > 0.5


def copies_of(sources, targets, sems):
    copies = [pltpu.make_async_copy(a, b, sems.at[i]) for i, (a, b) in enumerate(zip(sources, targets))]
    for copy in copies:
        copy.start()
    return copies


def load_kernel(here, w_out, crops, *refs):
    count = (len(refs) - 5) // 2
    vectors, (piece, table), sems = refs[:count], refs[count : count + 2], refs[-1]
    held = refs[count + 2 : -1]
    size = piece.shape[0]
    start = pl.multiple_of((here[0] & 3) * size, size)
    sources = [w_out.at[pl.ds(start, size), :], crops, *vectors]
    copies = copies_of(sources, held, sems)
    copies[0].wait()
    piece[...] = held[0][...].astype(HIGH)
    for copy in copies[1:]:
        copy.wait()
    table[...] = jnp.zeros_like(table)
    at, width = 0, table.shape[1]
    for vector in held[2:]:
        for low in range(0, vector.shape[0], width):
            part = min(width, vector.shape[0] - low)
            table[at : at + 1, :part] = vector[low : low + part].reshape(1, part)
            at += 1
    seqs, length = held[1].shape
    table[at : at + seqs, :length] = held[1][...].astype(HIGH)


def front_kernel(*refs, length, seqs, crops):
    sources, count = refs[:5], 5 + seqs
    targets, held, kept, sems = refs[5 : 5 + count], refs[5 + count : 10 + count], refs[10 + count : -1], refs[-1]
    copies = copies_of(sources, held, sems)
    tokens, table, w_q, w_k, w_v = held
    first_out, q, k, v, lse, *outs = kept
    stores = [pltpu.make_async_copy(a, b, sems.at[5 + i]) for i, (a, b) in enumerate(zip(kept, targets))]
    copies[0].wait()
    unit, _ = unit_rows(tokens[...].astype(HIGH))
    copies[1].wait()
    local, width = w_q.shape[1], tokens.shape[1]
    first = (unit * row(table, GAIN_ATTN, width) + row(table, SHIFT_ATTN, width)).astype(LOW)
    first_out[...] = first
    stores[0].start()
    for copy in copies[2:]:
        copy.wait()
    q_all = plain_dot(first, w_q[...]) + row(table, BIAS_Q, local)
    q_all = (q_all.astype(LOW) * 0.125).astype(LOW)
    k_all = plain_dot(first, w_k[...]).astype(LOW)
    v_all = (plain_dot(first, w_v[...]) + row(table, BIAS_V, local)).astype(LOW)
    q[...] = q_all
    k[...] = k_all
    v[...] = v_all
    for store in stores[1:4]:
        store.start()
    low_half, masks = half_masks()
    for s, o in enumerate(outs):
        rows = slice(s * length, (s + 1) * length)
        same = same_crop(table, crops + s, length)
        for t in range(local // PAIR):
            at = slice(t * PAIR, (t + 1) * PAIR)
            q_pair, k_pair, v_pair = q_all[rows, at], k_all[rows, at], v_all[rows, at]
            got = []
            for half in range(2):
                scores = jnp.where(same, right_trans(q_pair * masks[half], k_pair), NEGATIVE)
                top = jnp.max(scores, axis=-1, keepdims=True)
                expo = jnp.exp(scores - top)
                total = jnp.sum(expo, axis=-1, keepdims=True)
                probs = (expo * (1.0 / total)).astype(LOW)
                got.append(plain_dot(probs, v_pair))
                h = 2 * t + half
                lse[rows, h : h + 1] = top + jnp.log(total)
            o[:, at] = jnp.where(low_half, got[0], got[1])
        stores[5 + s].start()
    stores[4].start()
    for store in stores:
        store.wait()


def relative_rows(here, width, count, bits):
    size = width // count
    place = lax.broadcasted_iota(jnp.int32, (width, 1), 0)
    block = ((place.astype(HIGH) + 0.5) * (1.0 / size)).astype(jnp.int32)
    mask = jnp.zeros_like(block)
    for p, bit in enumerate(bits):
        mask = mask + (((block >> (len(bits) - 1 - p)) & 1) << bit)
    source = (mask ^ here) * size + (place - block * size)
    marks = lax.broadcasted_iota(jnp.int32, (width, width), 1) == source
    return marks.astype(HIGH).astype(LOW)


def turn_kernel(here, *refs, count, orders):
    sources, held = refs[:4], (refs[-2], *refs[4:7])
    order_b, sums, sems = refs[7], refs[8], refs[-1]
    seqs = (len(refs) - 11) // 3
    a1_a, a1_b, cot_a = (refs[9 + i * seqs : 9 + (i + 1) * seqs] for i in range(3))
    first = refs[-2]
    length = first.shape[0] // seqs
    copies = copies_of(sources, held, sems)
    width = first.shape[1]
    order_a = relative_rows(here[0], width, count, orders[0])
    order = relative_rows(here[0], width, count, orders[1])
    order_b[...] = order
    copies[0].wait()
    for s in range(seqs):
        part = first[s * length : (s + 1) * length, :]
        a1_a[s][...] = right_trans(order_a, part).astype(LOW)
        a1_b[s][...] = right_trans(order, part).astype(LOW)
    for copy in copies[1:]:
        copy.wait()
    cot = held[1][...]
    for s in range(seqs):
        part = cot[s * length : (s + 1) * length, :]
        cot_a[s][...] = right_trans(order_a, part).astype(LOW)
    sums[...] = col_sum(cot.astype(HIGH))


def low_kernel(values, out):
    out[...] = values[...].astype(LOW)


def gather_kernel(here, *refs):
    for b, piece in enumerate(refs[:-1]):
        size = piece.shape[0]
        start = pl.multiple_of(((here[0] & 3) ^ b) * size, size)
        refs[-1][pl.ds(start, size), :] = piece[...].astype(LOW)


def middle_kernel(*refs, blocks, seq, length):
    tokens, o_own, o_other, w_out, w_low, table, w_up, w_down, cotangent, order = refs[:10]
    hidden, a2_t, active, g_pre, g_second, g_bias = refs[-6:]
    rows = slice(seq * length, (seq + 1) * length)
    attn = plain_dot(o_own[...].astype(LOW), w_out[...])
    attn = attn + plain_dot(o_other[...].astype(LOW), w_low[...])
    width = tokens.shape[1]
    values = tokens[rows, :].astype(HIGH) + (attn + row(table, BIAS_OUT, width))
    hidden[...] = values
    unit, _ = unit_rows(values)
    second = (unit * row(table, GAIN_MLP, width) + row(table, SHIFT_MLP, width)).astype(LOW)
    cot = cotangent[rows, :]
    size = w_up.shape[1] // blocks
    total = None
    for b in range(blocks):
        at = slice(b * size, (b + 1) * size)
        low = b * size % width
        at_row = BIAS_UP + b * size // width
        bias_up = table[at_row : at_row + 1, low : low + size]
        pre = plain_dot(second, w_up[:, at]) + bias_up
        cdf = 0.5 * (1.0 + lax.erf(pre * 0.7071067811865476))
        active[:, at] = (pre * cdf).astype(LOW)
        slope = cdf + pre * (0.3989422804014327 * jnp.exp(-0.5 * (pre * pre)))
        grad = (right_trans(cot, w_down[at, :]) * slope).astype(LOW)
        g_pre[:, at] = grad
        bias = col_sum(grad.astype(HIGH))
        g_bias[:, at] = refs[10][:, at] + bias if seq else bias
        part = right_trans(grad, w_up[:, at])
        total = part if total is None else total + part
    g_second[...] = total
    a2_t[...] = right_trans(order[...], second).astype(LOW)


def back_kernel(*refs, seq, length, crops):
    tokens, table, cotangent, hidden, own, other, order = refs[:7]
    w_out, w_q, w_k, w_v, q, k, v, lse = refs[7:15]
    before = refs[15:17]
    g_hidden, gh_t, g_qk, g_val, sums, g_first = refs[17:]
    width, local = tokens.shape[1], q.shape[1]
    rows = slice(seq * length, (seq + 1) * length)
    full = slice(0, width)
    if seq:
        sums_before, first_before = before
        g_first[: seq * length, :] = first_before[...]
        sums[6:, :] = sums_before[6:, :]
    else:
        g_bias, cot_sum = before
        sums[6:7, :] = g_bias[:, :width]
        sums[7:8, :] = g_bias[:, width:]
        sums[8:9, :] = cot_sum[...]
        sums[9:, :] = jnp.zeros_like(sums[9:, :])

    def put(r, at, value):
        sums[r : r + 1, at] = sums_before[r : r + 1, at] + value if seq else value

    unit, scale = unit_rows(hidden[...])
    grad = own[...] + other[...]
    put(0, full, col_sum(grad * unit))
    put(1, full, col_sum(grad))
    values = norm_back(grad * row(table, GAIN_MLP, width), unit, scale)
    values = cotangent[rows, :].astype(HIGH) + values
    g_hidden[...] = values
    put(2, full, col_sum(values))
    low = values.astype(LOW)
    gh_t[...] = right_trans(order[...], low).astype(LOW)
    g_o = right_trans(low, w_out[...]).astype(LOW)
    same = same_crop(table, crops + seq, length)
    low_half, masks = half_masks()
    for t in range(local // PAIR):
        at = slice(t * PAIR, (t + 1) * PAIR)
        q_pair, k_pair, v_pair, o_pair = q[rows, at], k[rows, at], v[rows, at], g_o[:, at]
        got = []
        for half in range(2):
            h = 2 * t + half
            scores = right_trans(q_pair * masks[half], k_pair)
            probs = jnp.exp(jnp.where(same, scores, NEGATIVE) - lse[rows, h : h + 1])
            g_probs = right_trans(o_pair * masks[half], v_pair)
            inner = jnp.sum(g_probs * probs, axis=-1, keepdims=True)
            g_scores = (probs * (g_probs - inner)).astype(LOW)
            got.append(
                (
                    plain_dot(g_scores, k_pair),
                    left_trans(g_scores, q_pair),
                    left_trans(probs.astype(LOW), o_pair),
                )
            )
        g_q = (jnp.where(low_half, got[0][0], got[1][0]) * 0.125).astype(LOW)
        g_k = jnp.where(low_half, got[0][1], got[1][1]).astype(LOW)
        g_v = jnp.where(low_half, got[0][2], got[1][2]).astype(LOW)
        beside = slice(local + t * PAIR, local + (t + 1) * PAIR)
        g_qk[:, at] = g_q
        g_qk[:, beside] = g_k
        g_val[:, at] = g_v
        put(5, at, col_sum(g_q.astype(HIGH)))
        put(5, beside, col_sum(g_v.astype(HIGH)))
    part = right_trans(g_qk[:, :local], w_q[...])
    part = part + right_trans(g_qk[:, local:], w_k[...])
    part = part + right_trans(g_val[...], w_v[...])
    g_first[rows, :] = part
    unit_one, _ = unit_rows(tokens[rows, :].astype(HIGH))
    put(3, full, col_sum(part * unit_one))
    put(4, full, col_sum(part))


def base_kernel(table, tokens, own, *refs, length):
    g_hidden, (base, unit_out, scale_out) = refs[:-3], refs[-3:]
    gain = row(table, GAIN_ATTN, tokens.shape[1])
    for s in range(tokens.shape[0] // length):
        rows = slice(s * length, (s + 1) * length)
        part = own[rows, :]
        unit, scale = unit_rows(tokens[rows, :].astype(HIGH))
        base[rows, :] = g_hidden[s][...] + norm_back(part * gain, unit, scale)
        unit_out[rows, :] = unit
        scale_out[rows, :] = scale


def last_kernel(table, base, unit, scale, other, g_tokens, *, length):
    gain = row(table, GAIN_ATTN, base.shape[1])
    for s in range(base.shape[0] // length):
        rows = slice(s * length, (s + 1) * length)
        grad = norm_back(other[rows, :] * gain, unit[rows, :], scale[rows, :])
        g_tokens[rows, :] = base[rows, :] + grad


def out_kernel(*refs, seqs, length):
    table, own, other = refs[:3]
    for s in range(seqs):
        rows = slice(s * length, (s + 1) * length)
        total = refs[3 + s][...] + (own[rows, :] + other[rows, :])
        refs[3 + seqs][rows, :] = (total + row(table, BIAS_DOWN, total.shape[1])).astype(LOW)


def mlp_kernel(w_down, *refs):
    length = refs[0].shape[0]
    for s, active in enumerate(refs[:-1]):
        refs[-1][s * length : (s + 1) * length, :] = plain_dot(active[...], w_down[...])


def products(plan, refs, at):
    for lefts, rights, column in plan:
        wide = refs[rights[0]].shape[1]
        step = min(512, wide)
        for n in range(0, wide, step):
            value = None
            for left, right in zip(lefts, rights):
                part = plain_dot(refs[left][at, :], refs[right][:, n : n + step].astype(LOW))
                value = part if value is None else value + part
            yield slice(column + n, column + n + step), value


def far_kernel(*refs, plan, start, pieces, small):
    outs = refs[-pieces:]
    size = start // pieces
    for o, out in enumerate(outs):
        at = slice(start + o * size, start + (o + 1) * size)
        for columns, value in products(plan, refs, at):
            out[:size, columns] = value
    if small:
        outs[0][size:, :] = refs[-pieces - 1][...]


def part_kernel(*refs, plan, start, added):
    out = refs[-1]
    at = slice(start, start + out.shape[0])
    for columns, value in products(plan, refs, at):
        out[:, columns] = value + refs[-2][:, columns] if added else value


def near_kernel(*refs, plan, pieces, small):
    outs, got = refs[-2:], refs[-2 - pieces - small :]
    half = outs[0].shape[0]
    for o, out in enumerate(outs):
        at = slice(o * half, (o + 1) * half)
        size = 2 * half // pieces
        low = o * half % size
        for columns, value in products(plan, refs, at):
            out[:half, columns] = value + got[o * half // size][low : low + half, columns]
    if small:
        outs[1][half:, :] = got[pieces][...] + got[0][2 * half // pieces :, :]


def step_kernel(*refs, small, joined):
    count = 2 if joined else 1
    keeps, sents, gots = (refs[i * count : (i + 1) * count] for i in range(3))
    outs = refs[3 * count :]
    at = 0
    for i in range(count):
        half = outs[i].shape[0]
        got = gots[i]
        outs[i][...] = keeps[i][:half, :] + got[:half, :]
        outs[count][at : at + half, :] = keeps[i][half:, :] + got[half : 2 * half, :]
        at += half
        if small and not i:
            outs[count][at : at + SMALL, :] = sents[i][2 * half :, :] + got[2 * half :, :]
            at += SMALL


def end_kernel(*refs, wide):
    count = (len(refs) - 1) // (1 + wide)
    keeps, got, outs = refs[:count], refs[count], refs[count + 1 :]
    at = o = 0
    for keep in keeps:
        size, each = keep.shape[0], keep.shape[1] // wide
        for w in range(wide):
            columns = slice(w * each, (w + 1) * each)
            outs[o][...] = keep[:, columns] + got[at : at + size, columns]
            o += 1
        at += size


def vector_kernel(here, sent, got, *outs, size):
    total = sent[size : size + SMALL, :] + got[size : size + SMALL, :]
    bias_q, bias_v, bias_up, gain_mlp, shift_mlp, bias_out, bias_down, gains = outs
    width, each = total.shape[1], bias_q.shape[0]
    bias_q[...] = total[5, :each]
    bias_v[...] = total[5, each:]
    for i in range(bias_up.shape[0] // width):
        bias_up[i * width : (i + 1) * width] = total[6 + i, :]
    turned = pltpu.roll(total, lax.rem(width - here[0] * size, width), 1)
    for out, at in ((gain_mlp, 0), (shift_mlp, 1), (bias_out, 2), (bias_down, 8)):
        out[...] = turned[at, :size]
    gains[...] = turned[:8, : gains.shape[1]]


def gain_kernel(own, other, gain, shift):
    total = own[...] + other[...]
    gain[...] = total[3, : gain.shape[0]]
    shift[...] = total[4, : shift.shape[0]]


class Steps:
    def __init__(self):
        self.last = None

    def __call__(
        self, kernel, name, outs, args, scratch=(), limit=12, smem=0, whole=(), tie=0, alias=None, cost=0, out_whole=False
    ):
        args = list(args)
        if self.last is not None:
            args[tie], _ = lax.optimization_barrier((args[tie], self.last))
        result = pl.pallas_call(
            kernel,
            name=name,
            out_shape=[jax.ShapeDtypeStruct(s, d) for s, d in outs],
            in_specs=[pl.BlockSpec(memory_space=pltpu.SMEM)] * smem
            + [pl.BlockSpec(memory_space=pl.ANY) if i in whole else VMEM for i in range(smem, len(args))]
            if whole
            else [pl.BlockSpec(memory_space=pltpu.SMEM)] * smem + [VMEM] * (len(args) - smem),
            out_specs=[pl.BlockSpec(memory_space=pl.ANY) if out_whole else VMEM] * len(outs),
            scratch_shapes=list(scratch),
            input_output_aliases=alias or {},
            compiler_params=pltpu.CompilerParams(vmem_limit_bytes=limit << 20),
            cost_estimate=pl.CostEstimate(flops=1000 + cost, bytes_accessed=1000, transcendentals=0),
        )(*args)
        self.last = result[0]
        return result


def send(values, bit, count):
    return lax.ppermute(values, "dp", [(i, i ^ (1 << bit)) for i in range(count)])


def swap(values):
    return lax.ppermute(values, "mp", [(0, 1), (1, 0)])


class Scatter:
    def __init__(self, steps, count, bits, plan, pieces=2, wide=1, small=None):
        self.steps, self.count, self.bits = steps, count, bits
        self.pieces, self.wide, self.small = pieces, wide, small
        self.plan, self.arrays, self.columns = [], [], 0
        for lefts, rights in plan:
            at, each = len(self.arrays), len(lefts)
            self.arrays += lefts + rights
            places = list(range(at, at + each)), list(range(at + each, at + 2 * each))
            self.plan.append((*places, self.columns))
            self.columns += rights[0].shape[1]
        self.rows = plan[0][0][0].shape[0] // 2
        self.extra = SMALL if small is not None else 0
        self.at = 1

    def shapes(self, *sizes):
        return [((n, self.columns), HIGH) for n in sizes]

    def far(self):
        size = self.rows // self.pieces
        kernel = partial(
            far_kernel,
            plan=self.plan,
            start=self.rows,
            pieces=self.pieces,
            small=bool(self.extra),
        )
        held = self.arrays + ([self.small] if self.extra else [])
        outs = self.shapes(size + self.extra, *[size] * (self.pieces - 1))
        outs = self.steps(kernel, "far", outs, held)
        self.got = [send(o, self.bits[0], self.count) for o in outs]

    def near(self):
        kernel = partial(
            near_kernel,
            plan=self.plan,
            pieces=self.pieces,
            small=bool(self.extra),
        )
        held = self.arrays + self.got + ([self.small] if self.extra else [])
        self.rows //= 2
        outs = self.shapes(self.rows, self.rows + self.extra)
        self.keep, self.sent = self.steps(kernel, "near", outs, held)
        self.got = send(self.sent, self.bits[1], self.count)

    def part(self, start, added):
        kernel = partial(part_kernel, plan=self.plan, start=start * self.rows // 2, added=len(added))
        outs = self.shapes(self.rows // 2)
        return self.steps(kernel, "part", outs, self.arrays + added)[0]

    def far_parts(self):
        kernel = partial(far_kernel, plan=self.plan, start=self.rows, pieces=2, small=False)
        kept, sent = self.steps(kernel, "far", self.shapes(*[self.rows // 2] * 2), self.arrays)
        return [send(o, self.bits[0], self.count) for o in (sent, kept)]

    def near_sent(self, got):
        self.sent = self.part(1, [got])
        self.got = send(self.sent, self.bits[1], self.count)

    def near_keep(self, got):
        self.keep = self.part(0, [got])
        self.rows //= 2

    def rest(self):
        while self.at + 1 < len(self.bits):
            self.step()

    def step(self):
        self.at += 1
        self.rows //= 2
        outs = self.shapes(self.rows, self.rows + self.extra)
        kernel = partial(step_kernel, small=bool(self.extra), joined=False)
        self.keep, self.sent = self.steps(kernel, "sum", outs, [self.keep, self.sent, self.got])
        self.got = send(self.sent, self.bits[self.at], self.count)


def join(one, two):
    for part in (one, two):
        part.at += 1
        part.rows //= 2
    outs = one.shapes(one.rows) + two.shapes(two.rows) + one.shapes(one.rows + two.rows + one.extra)
    kernel = partial(step_kernel, small=bool(one.extra), joined=True)
    held = [one.keep, two.keep, one.sent, two.sent, one.got, two.got]
    one.keep, two.keep, sent = one.steps(kernel, "sums", outs, held)
    got = send(sent, one.bits[one.at], one.count)
    while one.at + 1 < len(one.bits):
        one.at += 1
        half = one.rows // 2
        starts = (0, one.rows + one.extra)
        keeps, sents = [], []
        for part, start in zip((one, two), starts):
            total = part.keep + got[start : start + part.rows]
            keeps.append(total[:half])
            sents.append(total[half:])
        if one.extra:
            at = slice(one.rows, one.rows + one.extra)
            sents.insert(1, sent[at] + got[at])
        one.keep, two.keep = keeps
        one.rows = two.rows = half
        sent = jnp.concatenate(sents)
        got = send(sent, one.bits[one.at], one.count)
    return sent, got


def finish(parts, got, cost=0):
    outs = []
    for part in parts:
        outs += [((part.rows, part.columns // part.wide), HIGH)] * part.wide
    kernel = partial(end_kernel, wide=parts[0].wide)
    held = [part.keep for part in parts] + [got]
    return parts[0].steps(kernel, "end", outs, held, cost=cost)


def body(
    tokens,
    crop_ids,
    w_query,
    w_key,
    w_value,
    bias_query,
    bias_value,
    w_out,
    bias_out,
    gain_attn,
    shift_attn,
    gain_mlp,
    shift_mlp,
    w_up,
    bias_up,
    w_down,
    bias_down,
    cotangent,
    count,
):
    width = tokens.shape[1]
    local = w_query.shape[1]
    hidden_units = w_up.shape[1]
    seqs, length = crop_ids.shape
    rows = seqs * length
    here = lax.axis_index("dp")
    scalar = here.reshape(1)
    bits = list(range(count.bit_length() - 1))
    orders = (bits, [0, 2, 1] + bits[3:])
    steps = Steps()
    piece = local // 4
    lines = [gain_attn, shift_attn, bias_query, bias_value, bias_out, gain_mlp, shift_mlp]
    lines += [bias_down, bias_up]
    crops = BIAS_UP + hidden_units // width
    held = [((piece, width), LOW), (crop_ids.shape, jnp.int32)] + [(v.shape, HIGH) for v in lines]
    mine, table = steps(
        load_kernel,
        "load",
        [((piece, width), HIGH), ((crops + seqs, width), HIGH)],
        [scalar, w_out, crop_ids] + lines,
        scratch=[pltpu.VMEM(*h) for h in held] + [pltpu.SemaphoreType.DMA((len(held),))],
        smem=1,
        whole=range(1, 3 + len(lines)),
        limit=63,
    )
    got = swap(mine)

    def like(*arrays):
        return [(a.shape, a.dtype) for a in arrays]

    loaded = [tokens, table, w_query, w_key, w_value]
    made = [((rows, width), LOW)] + [((rows, local), LOW)] * 3
    made += [((rows, 128), HIGH)] + [((length, local), HIGH)] * seqs
    first, query, key_rows, value_rows, log_total, *mixed = steps(
        partial(front_kernel, length=length, seqs=seqs, crops=crops),
        "front",
        made,
        loaded,
        scratch=[pltpu.VMEM(*v) for v in like(*loaded) + made]
        + [pltpu.SemaphoreType.DMA((len(loaded) + len(made),))],
        whole=range(5),
        out_whole=True,
        tie=1,
        limit=58,
    )
    mixed_other = [swap(o) for o in mixed]

    got, _ = lax.optimization_barrier((got, first))
    beside = send(got, 1, count)
    pieces = [got, send(got, 0, count), beside]
    turned = steps(
        partial(turn_kernel, count=count, orders=orders),
        "turn",
        like(cotangent, w_up, w_out)
        + [((width, width), LOW), ((1, width), HIGH)]
        + [((width, length), LOW)] * (3 * seqs),
        [scalar, first, cotangent, w_up, w_out],
        scratch=[pltpu.VMEM((rows, width), LOW), pltpu.SemaphoreType.DMA((4,))],
        whole=range(1, 5),
        smem=1,
        tie=1,
        limit=44,
    )

    cotangent, w_up, w_out, order_b, cot_sum = turned[:5]
    a1_a, a1_b, cot_a = (list(turned[5 + i * seqs : 5 + (i + 1) * seqs]) for i in range(3))
    beside, _ = lax.optimization_barrier((beside, order_b))
    pieces.append(send(beside, 0, count))
    mixed_other[0] = steps(low_kernel, "low", [((length, local), LOW)], [mixed_other[0]], cost=31 * 10**8)[0]
    w_low = steps(
        gather_kernel, "gather", [((local, width), LOW)], [scalar] + pieces, smem=1, tie=1
    )[0]
    hidden, a2_b, active, g_pre, second, carried = [], [], [], [], [], []
    for s in range(seqs):
        result = steps(
            partial(middle_kernel, blocks=2, seq=s, length=length),
            "middle",
            [
                ((length, width), HIGH),
                ((width, length), LOW),
                ((length, hidden_units), LOW),
                ((length, hidden_units), LOW),
                ((length, width), HIGH),
                ((1, hidden_units), HIGH),
            ],
            [
                tokens,
                mixed[s],
                mixed_other[s],
                w_out,
                w_low,
                table,
                w_up,
                w_down,
                cotangent,
                order_b,
            ]
            + carried,
            tie=1,
        )
        for held, value in zip((hidden, a2_b, active, g_pre, second), result):
            held.append(value)
        carried = list(result[5:])
    bias_sum = carried[0]
    second_other = [swap(g) for g in second]

    down = Scatter(steps, count, orders[0], [(cot_a, active)])
    up = Scatter(steps, count, orders[1], [(a2_b, g_pre)])
    (up_sent, up_kept), (down_sent, down_kept) = [one.far_parts() for one in (up, down)]
    up.near_sent(up_sent)
    down.near_sent(down_sent)
    mlp_part = steps(mlp_kernel, "mlp", [((rows, width), HIGH)], [w_down] + active, tie=1)[0]
    mlp_other = swap(mlp_part)
    down.near_keep(down_kept)
    up.near_keep(up_kept)
    g_hidden, gh_b, g_qk, g_val, carried = [], [], [], [], [bias_sum, cot_sum]
    for s in range(seqs):
        if s == seqs - 1:
            down.step()
            up.step()
        result = steps(
            partial(back_kernel, seq=s, length=length, crops=crops),
            "back",
            [
                ((length, width), HIGH),
                ((width, length), LOW),
                ((length, 2 * local), LOW),
                ((length, local), LOW),
                ((SMALL, width), HIGH),
                (((s + 1) * length, width), HIGH),
            ],
            [tokens, table, cotangent, hidden[s], second[s], second_other[s], order_b]
            + [w_out, w_query, w_key, w_value, query, key_rows, value_rows, log_total]
            + carried,
            tie=4,
            cost=0 if s else 6 * 10**9,
        )
        for held, value in zip((g_hidden, gh_b, g_qk, g_val), result):
            held.append(value)
        carried = list(result[4:])
    sums, g_first = carried
    first_other = swap(g_first)
    heads = Scatter(steps, count, orders[0], [(a1_a, g_qk)], wide=2, small=sums)
    others = Scatter(steps, count, orders[1], [(a1_b, g_val), (gh_b, mixed)], wide=2)
    heads.far()
    others.far()
    _, mlp_got = join(down, up)
    heads.near()
    others.near()
    heads.step()
    block_out = steps(
        partial(out_kernel, seqs=seqs, length=length),
        "out",
        [((rows, width), LOW)],
        [table, mlp_part, mlp_other] + hidden,
        tie=1,
        cost=3 * 10**9,
    )[0]
    others.step()
    w_down_t, done_w_up = finish([down, up], mlp_got, 15 * 10**8)
    heads.rest()
    others.rest()
    base, unit, scale = steps(
        partial(base_kernel, length=length),
        "base",
        [((rows, width), HIGH)] * 2 + [((rows, 1), HIGH)],
        [table, tokens, g_first] + g_hidden,
        tie=2,
    )
    size = width // count
    (
        done_bias_q,
        done_bias_v,
        done_bias_up,
        done_gain_mlp,
        done_shift_mlp,
        done_bias_out,
        done_bias_down,
        gains,
    ) = steps(
        partial(vector_kernel, size=size),
        "vectors",
        [((local,), HIGH)] * 2
        + [((hidden_units,), HIGH)]
        + [((size,), HIGH)] * 4
        + [((8, 128), HIGH)],
        [scalar, heads.sent, heads.got],
        smem=1,
        tie=1,
    )
    gains_other = swap(gains)
    grad_w_q, grad_w_k = finish([heads], heads.got)
    grad_w_v, w_out_t = finish([others], others.got)
    grad_tokens = steps(
        partial(last_kernel, length=length),
        "last",
        [((rows, width), HIGH)],
        [table, base, unit, scale, first_other],
        tie=1,
    )[0]
    done_gain_attn, done_shift_attn = steps(
        gain_kernel, "gains", [((size,), HIGH)] * 2, [gains, gains_other]
    )
    return (
        block_out,
        grad_tokens,
        grad_w_q,
        grad_w_k,
        grad_w_v,
        done_bias_q,
        done_bias_v,
        w_out_t.T,
        done_bias_out,
        done_gain_attn,
        done_shift_attn,
        done_gain_mlp,
        done_shift_mlp,
        done_w_up,
        done_bias_up,
        w_down_t.T,
        done_bias_down,
    )


def solution(mesh):
    placed = (
        P("dp", None),
        P("dp", None),
        P(None, "mp"),
        P(None, "mp"),
        P(None, "mp"),
        P("mp"),
        P("mp"),
        P("mp", None),
        P(),
        P(),
        P(),
        P(),
        P(),
        P(None, "mp"),
        P("mp"),
        P("mp", None),
        P(),
        P("dp", None),
    )
    return jax.shard_map(
        partial(body, count=mesh.shape["dp"]),
        mesh=mesh,
        in_specs=placed,
        out_specs=(
            P("dp", None),
            P("dp", None),
            P("dp", "mp"),
            P("dp", "mp"),
            P("dp", "mp"),
            P("mp"),
            P("mp"),
            P("mp", "dp"),
            P("dp"),
            P("dp"),
            P("dp"),
            P("dp"),
            P("dp"),
            P("dp", "mp"),
            P("mp"),
            P("mp", "dp"),
            P("dp"),
        ),
        check_vma=False,
    )
```
